32 devices in a mesh: dp: 2 (over x), tp: 4 (over z), sp: 4 (over y, core).
Axes of the slice: x: 2, y: 2, z: 4, core: 2. Of those that a mesh axis runs over, the one named last changes fastest.
Arguments:
- tokens: bfloat16 [16, 3072], P(('dp', 'sp')), parts along dimension 0
- states: float32 [4, 16, 24, 128, 128], P('sp', 'dp', 'tp'), parts along dimension 1
- k_cache: bfloat16 [16, 8, 8192, 128], P('dp', 'tp', 'sp'), parts along dimension 0
- v_cache: bfloat16 [16, 8, 8192, 128], P('dp', 'tp', 'sp'), parts along dimension 0
- slopes: float32 [24], P('tp')
- lin_gain: float32 [3072], replicated
- w_lin_qkv: bfloat16 [3072, 3, 3072], P(None, None, 'tp')
- w_lin_gate: bfloat16 [3072, 3072], P(None, 'tp')
- out_gain: float32 [3072], P('tp')
- w_lin_out: bfloat16 [3072, 3072], P('tp')
- attn_gain: float32 [3072], replicated
- w_attn_in: bfloat16 [3072, 8, 5, 128], P(None, 'tp')
- w_attn_out: bfloat16 [3072, 3072], P('tp')
Outputs:
- output 1: bfloat16 [16, 3072], P(('dp', 'sp')), parts along dimension 0
- output 2: float32 [16, 24, 128, 128], P(('dp', 'sp'), 'tp'), parts along dimension 0
- output 3: bfloat16 [16, 8, 8208, 128], P(('dp', 'sp'), 'tp'), parts along dimension 0
- output 4: bfloat16 [16, 8, 8208, 128], P(('dp', 'sp'), 'tp'), parts along dimension 0
There are 2 independent parts. The reference program is written for one: setup_inputs(seed, part) draws one part's arguments, and reference() takes and returns one part's arrays. A program takes and returns all parts, laid end to end along the dimension named above; an argument that names none is the same for every part.
All inputs are finite; a program needn't handle non-finite values.
Results may differ from the reference program's by a relative error of at most 0.0125481.
Values are sent between devices in bfloat16 or wider.
A program may use at most 1 GiB of HBM per device.

```python
import jax
import jax.numpy as jnp
from jax import lax

MODEL_DIM = 3072
NUM_HEADS = 24
KV_COUNT = 8
HEAD_DIM = 128
SEQ_SHARDS = 4
BATCH = 8
SHARD_LEN = 2048
CACHE_EXTRA = 16

PROMPT_LEN = SEQ_SHARDS * SHARD_LEN
HIDDEN = NUM_HEADS * HEAD_DIM
GROUP = NUM_HEADS // KV_COUNT
ROPE_DIM = HEAD_DIM // 2
NORM_EPS = 1e-6
ROPE_BASE = 10000000.0
RES_ALPHA = 1.0
RES_BETA = 1.0


def draw_weight(key, shape, fan_in):
    return (jax.random.normal(key, shape, jnp.float32) * fan_in ** -0.5).astype(jnp.bfloat16)


def draw_gain(key, width):
    return 1.0 + 0.3 * jax.random.normal(key, (width,), jnp.float32)


def draw_cache(key, wave_cos, wave_sin):
    sub_keys = jax.random.split(key, 3)
    amplitude = jax.random.normal(sub_keys[0], (BATCH, KV_COUNT, 3, HEAD_DIM), jnp.float32) * (2.0 / 3.0) ** 0.5
    phases = jax.random.uniform(sub_keys[1], (BATCH, KV_COUNT, 3, HEAD_DIM), jnp.float32, 0.0, 2.0 * jnp.pi)
    slow_part = jnp.einsum('bkjd,jt->bktd', amplitude * jnp.cos(phases), wave_cos) - jnp.einsum('bkjd,jt->bktd', amplitude * jnp.sin(phases), wave_sin)
    noise_vals = jax.random.normal(sub_keys[2], (BATCH, KV_COUNT, PROMPT_LEN, HEAD_DIM), jnp.float32)
    return (slow_part + 0.5 * noise_vals).astype(jnp.bfloat16)


def setup_inputs(seed: int = 0, part: int = 0) -> dict:
    base_key = jax.random.key(seed)
    shared = jax.random.split(base_key, 12)
    own_keys = jax.random.split(jax.random.fold_in(base_key, part), 4)
    positions = jnp.arange(PROMPT_LEN, dtype=jnp.float32) / PROMPT_LEN
    wave_arg = 2.0 * jnp.pi * jnp.arange(1, 4, dtype=jnp.float32)[:, None] * positions[None, :]
    wave_cos = jnp.cos(wave_arg)
    wave_sin = jnp.sin(wave_arg)
    return {
        'tokens': jax.random.normal(own_keys[0], (BATCH, MODEL_DIM), jnp.float32).astype(jnp.bfloat16),
        'states': jax.random.normal(own_keys[1], (SEQ_SHARDS, BATCH, NUM_HEADS, HEAD_DIM, HEAD_DIM), jnp.float32),
        'k_cache': draw_cache(own_keys[2], wave_cos, wave_sin),
        'v_cache': draw_cache(own_keys[3], wave_cos, wave_sin),
        'slopes': jax.random.uniform(shared[0], (NUM_HEADS,), jnp.float32, 0.2, 1.2) / PROMPT_LEN,
        'lin_gain': draw_gain(shared[1], MODEL_DIM),
        'w_lin_qkv': draw_weight(shared[2], (MODEL_DIM, 3, HIDDEN), MODEL_DIM),
        'w_lin_gate': draw_weight(shared[3], (MODEL_DIM, HIDDEN), MODEL_DIM),
        'out_gain': draw_gain(shared[4], HIDDEN),
        'w_lin_out': draw_weight(shared[5], (HIDDEN, MODEL_DIM), HIDDEN),
        'attn_gain': draw_gain(shared[6], MODEL_DIM),
        'w_attn_in': draw_weight(shared[7], (MODEL_DIM, KV_COUNT, GROUP + 2, HEAD_DIM), MODEL_DIM),
        'w_attn_out': draw_weight(shared[8], (HIDDEN, MODEL_DIM), HIDDEN),
    }


def rms_norm(vals_in, gain_vec):
    vals32 = vals_in.astype(jnp.float32)
    inv_rms = lax.rsqrt(jnp.mean(vals32 * vals32, axis=-1, keepdims=True) + NORM_EPS)
    return vals32 * inv_rms * gain_vec


def rotary(vals_in):
    half_dim = ROPE_DIM // 2
    inv_freq = ROPE_BASE ** (-jnp.arange(0, ROPE_DIM, 2, dtype=jnp.float32) / ROPE_DIM)
    angles = PROMPT_LEN * inv_freq
    cosine = jnp.cos(angles)
    sine_vals = jnp.sin(angles)
    vals32 = vals_in.astype(jnp.float32)
    first_half = vals32[..., :half_dim]
    second_half = vals32[..., half_dim:ROPE_DIM]
    return jnp.concatenate([first_half * cosine - second_half * sine_vals, second_half * cosine + first_half * sine_vals, vals32[..., ROPE_DIM:]], axis=-1).astype(jnp.bfloat16)


def attend_row(row_data):
    query_rot, keys_row, values_row, key_new, value_new = row_data
    score_scale = HEAD_DIM ** -0.5
    query_f32 = query_rot.astype(jnp.float32)
    scores = jnp.einsum('kgd,ktd->kgt', query_f32, keys_row.astype(jnp.float32)) * score_scale
    new_score = jnp.einsum('kgd,kd->kg', query_f32, key_new.astype(jnp.float32)) * score_scale
    row_max = jnp.maximum(jnp.max(scores, axis=-1), new_score)
    probs = jnp.exp(scores - row_max[..., None])
    new_prob = jnp.exp(new_score - row_max)
    prob_sum = jnp.sum(probs, axis=-1) + new_prob
    weighted_sum = jnp.einsum('kgt,ktd->kgd', probs.astype(jnp.bfloat16).astype(jnp.float32), values_row.astype(jnp.float32))
    weighted_sum = weighted_sum + new_prob.astype(jnp.bfloat16).astype(jnp.float32)[..., None] * value_new.astype(jnp.float32)[:, None, :]
    return weighted_sum / prob_sum[..., None]


def reference(tokens, states, k_cache, v_cache, slopes, lin_gain, w_lin_qkv, w_lin_gate, out_gain, w_lin_out, attn_gain, w_attn_in, w_attn_out):
    normed = rms_norm(tokens, lin_gain).astype(jnp.bfloat16)
    offsets = (SHARD_LEN * (SEQ_SHARDS - 1 - jnp.arange(SEQ_SHARDS))).astype(jnp.float32)
    shard_weight = jnp.exp(-slopes[None, :] * offsets[:, None])
    moved_state = jnp.einsum('ch,cbhde->bhde', shard_weight, states)
    lin_proj = jnp.dot(normed, w_lin_qkv.reshape(MODEL_DIM, 3 * HIDDEN), preferred_element_type=jnp.float32)
    act_vals = jax.nn.silu(lin_proj).astype(jnp.bfloat16).reshape(BATCH, 3, NUM_HEADS, HEAD_DIM).astype(jnp.float32)
    state_new = jnp.exp(-slopes)[None, :, None, None] * moved_state + jnp.einsum('bhd,bhe->bhde', act_vals[:, 1], act_vals[:, 2])
    lin_attn = jnp.einsum('bhd,bhde->bhe', act_vals[:, 0], state_new).reshape(BATCH, HIDDEN)
    gate_vals = jax.nn.sigmoid(jnp.dot(normed, w_lin_gate, preferred_element_type=jnp.float32))
    mixed_out = (rms_norm(lin_attn, out_gain) * gate_vals).astype(jnp.bfloat16)
    lin_out = jnp.dot(mixed_out, w_lin_out, preferred_element_type=jnp.float32)
    hidden = (RES_ALPHA * normed.astype(jnp.float32) + RES_BETA * lin_out).astype(jnp.bfloat16)

    normed_two = rms_norm(hidden, attn_gain).astype(jnp.bfloat16)
    attn_proj = jnp.dot(normed_two, w_attn_in.reshape(MODEL_DIM, KV_COUNT * (GROUP + 2) * HEAD_DIM), preferred_element_type=jnp.float32)
    attn_proj = attn_proj.astype(jnp.bfloat16).reshape(BATCH, KV_COUNT, GROUP + 2, HEAD_DIM)
    query_rot = rotary(attn_proj[:, :, :GROUP])
    key_new = rotary(attn_proj[:, :, GROUP])
    value_new = attn_proj[:, :, GROUP + 1]
    head_out = lax.map(attend_row, (query_rot, k_cache, v_cache, key_new, value_new))
    attn_out = jnp.dot(head_out.astype(jnp.bfloat16).reshape(BATCH, HIDDEN), w_attn_out, preferred_element_type=jnp.float32)
    hidden_out = (RES_ALPHA * normed_two.astype(jnp.float32) + RES_BETA * attn_out).astype(jnp.bfloat16)
    tail_zeros = jnp.zeros((BATCH, KV_COUNT, CACHE_EXTRA - 1, HEAD_DIM), jnp.bfloat16)
    k_out = jnp.concatenate([k_cache, key_new[:, :, None, :], tail_zeros], axis=2)
    v_out = jnp.concatenate([v_cache, value_new[:, :, None, :], tail_zeros], axis=2)
    return (hidden_out, state_new, k_out, v_out)
```

```python
import math

import jax
import jax.numpy as jnp
import numpy as np
from jax import lax
from jax.experimental import pallas as pl
from jax.experimental.pallas import tpu as pltpu
from jax.sharding import PartitionSpec as P

NORM_EPS = 1e-6
ROPE_BASE = 10000000.0
RES_ALPHA = 1.0
RES_BETA = 1.0
CACHE_EXTRA = 16

MESH = pl.DeviceIdType.MESH
F32 = jnp.float32
BF16 = jnp.bfloat16
MIB = 2**20

ST_OWN, ST_FWD, ST_SUM = 0, 1, 2
SQ, PO, PA = 3, 6, 9
QX, MX, OX = 12, 15, 18
KV_NEAR = 21
KV_FAR = 23
NUM_SEMS = KV_FAR + 16


def rope_table(head_dim, position):
    rope_dim = head_dim // 2
    half = rope_dim // 2
    inv_freq = ROPE_BASE ** (-np.arange(0, rope_dim, 2, dtype=np.float64) / rope_dim)
    cos, sin = np.cos(position * inv_freq), np.sin(position * inv_freq)
    table = np.zeros((8, head_dim), np.float32)
    table[0] = np.concatenate([cos, cos, np.ones(head_dim - rope_dim)])
    table[1, :rope_dim] = np.concatenate([-sin, sin])
    return table


def flip(index, mask):
    chip, core = index // 2, index % 2
    if mask & 2:
        chip = 1 - chip
    if mask & 1:
        core = 1 - core
    return chip * 2 + core


def silu(x):
    return x * (1.0 / (1.0 + jnp.exp(-x)))


def step_kernel(
    tokens, states, k_cache, v_cache, slopes, lin_gain, w_qkv, w_gate, out_gain, w_lin_out, attn_gain, w_in, w_attn_out, rope,
    k_buf, v_buf, s_out, hid,
    tok_v, lg_v, og_v, ag_v, rope_v, slope_s, qkv_v, gate_v, lout_v, in_v, aout_v,
    st_loc, st_rcv, st_sum, st_in, hb, rows_v, o_v, g_v, rep_v, acc_v, proj_v, qf_v, vf_v, q_all, sc_v, mrow_v, m_all, mcol_v,
    ns_v, ol_v, olr_v, ho_v, sq_all, po_all, pa_all, kst,
    send, recv, lsem, ksem,
):
    sp = lax.axis_index("sp")
    tp = lax.axis_index("tp")
    shard_len = k_cache.shape[2]
    kv_dev = k_cache.shape[1]
    head_dim = k_cache.shape[3]
    heads = slopes.shape[0]
    rows = tokens.shape[0]
    width = tokens.shape[1]
    group = heads // kv_dev
    prompt = 4 * shard_len
    local_w = heads * head_dim

    def to_sp(mask):
        return {"sp": flip(sp, mask)}

    def to_tp(off):
        return {"tp": lax.rem(tp + off, 4)}

    barrier = pltpu.get_barrier_semaphore()
    for i in (1, 2, 3):
        pl.semaphore_signal(barrier, inc=1, device_id=to_sp(i), device_id_type=MESH)
    for i in (1, 2, 3):
        pl.semaphore_signal(barrier, inc=1, device_id=to_tp(i), device_id_type=MESH)
    pl.semaphore_wait(barrier, 6)

    def remote(src, dst, i, dev):
        return pltpu.make_async_remote_copy(src, dst, send.at[i], recv.at[i], device_id=dev, device_id_type=MESH)

    def local(src, dst, i):
        return pltpu.make_async_copy(src, dst, lsem.at[i])

    my_rows = pl.ds(pl.multiple_of(sp * shard_len, shard_len), shard_len)
    far = []
    for t, (src, dst) in enumerate(((k_cache, k_buf), (v_cache, v_buf))):
        for b in range(rows):
            for j in range(kv_dev):
                for mask in (2, 3):
                    far.append(remote(src.at[flip(sp, mask) * rows + b, j], dst.at[b, j, my_rows], KV_FAR + len(far), to_sp(mask)))
    far_state = [0, 0]

    def start_far(n):
        for _ in range(n):
            if far_state[0] < len(far):
                far[far_state[0]].start()
                far_state[0] += 1

    def pump(n):
        for _ in range(n):
            far[far_state[1]].wait_send()
            far_state[1] += 1
            start_far(1)

    def st_rows(g):
        return pl.ds(g * rows, rows)

    st_own = remote(states.at[0, st_rows(flip(sp, 1))], st_rcv.at[0], ST_OWN, to_sp(1))
    st_fwd = remote(states.at[0, st_rows(flip(sp, 3))], st_rcv.at[1], ST_FWD, to_sp(1))
    st_fwd.start()
    start_far(1)
    ld_fwd = local(states.at[0, st_rows(flip(sp, 2))], st_loc.at[1], 0)
    ld_slope = local(slopes, slope_s, 1)
    ld_fwd.start()
    ld_slope.start()
    st_own.start()
    ld_own = local(states.at[0, st_rows(sp)], st_loc.at[0], 2)
    ld_tok = local(tokens, tok_v, 3)
    ld_lg = local(lin_gain, lg_v, 4)
    ld_og = local(out_gain, og_v, 5)
    ld_ag = local(attn_gain, ag_v, 6)
    ld_rope = local(rope, rope_v, 7)
    ld_qkv = [local(w_qkv.at[j], qkv_v.at[j], 8 + j) for j in range(3)]
    ld_gate = local(w_gate, gate_v, 11)
    ld_lout = local(w_lin_out, lout_v, 12)
    ld_in = local(w_in, in_v, 13)
    ld_aout = local(w_attn_out, aout_v, 14)
    own_kv = [local(src.at[st_rows(sp)], dst.at[:, :, my_rows], 15 + t) for t, (src, dst) in enumerate(((k_cache, k_buf), (v_cache, v_buf)))]
    near = [remote(src.at[st_rows(flip(sp, 1))], dst.at[:, :, my_rows], KV_NEAR + t, to_sp(1)) for t, (src, dst) in enumerate(((k_cache, k_buf), (v_cache, v_buf)))]
    for c in [ld_own, ld_tok, ld_lg, ld_og, ld_ag, ld_rope] + ld_qkv + [ld_gate, ld_lout, ld_in, ld_aout] + near + own_kv:
        c.start()

    def decay(h, shard):
        off = (shard_len * (3 - shard)).astype(F32)
        return jnp.exp(jnp.full((1, head_dim), -slope_s[h] * off, F32))

    ld_slope.wait()
    ld_fwd.wait()
    st_fwd.wait_recv()
    for h in range(heads):
        w_me, w_ot = decay(h, sp), decay(h, flip(sp, 1))
        for b in range(rows):
            st_sum[b, h] = w_me * st_loc[1, b, h] + w_ot * st_rcv[1, b, h]
    st_send = remote(st_sum, st_in, ST_SUM, to_sp(2))
    st_send.start()
    start_far(2)

    ld_tok.wait()
    ld_lg.wait()
    x = tok_v[...].astype(F32)
    inv = lax.rsqrt(jnp.mean(x * x, axis=-1, keepdims=True) + NORM_EPS)
    hb[...] = (x * inv * lg_v[...]).astype(BF16)

    def matvec(x_ref, w_ref, k_len, n_len, kb, out_dtype=F32):
        def body(k, acc):
            at = pl.ds(pl.multiple_of(k * kb, kb), kb)
            return acc + jnp.dot(x_ref[:, at], w_ref[at, :], preferred_element_type=F32)
        return lax.fori_loop(0, k_len // kb, body, jnp.zeros((rows, n_len), F32))

    acts = []
    for j in range(3):
        ld_qkv[j].wait()
        acts.append(silu(matvec(hb, qkv_v.at[j], width, local_w, 256)).astype(BF16).astype(F32))
    ld_gate.wait()
    gate = 1.0 / (1.0 + jnp.exp(-matvec(hb, gate_v, width, local_w, 256)))
    rows_v[...] = jnp.zeros_like(rows_v)
    for b in range(rows):
        for h in range(heads):
            cols = slice(h * head_dim, (h + 1) * head_dim)
            rows_v[pl.ds(b * 8 + h, 1), :] = acts[0][b:b + 1, cols]
            rows_v[pl.ds(16 + b * 8 + h, 1), :] = acts[1][b:b + 1, cols]
    cols_t = jnp.transpose(rows_v[...])

    ld_own.wait()
    st_own.wait_recv()
    st_send.wait_recv()
    for h in range(heads):
        w_me, w_ot = decay(h, sp), decay(h, flip(sp, 1))
        lam = jnp.exp(jnp.full((1, head_dim), -slope_s[h], F32))
        cols = slice(h * head_dim, (h + 1) * head_dim)
        for b in range(rows):
            moved = w_me * st_loc[0, b, h] + w_ot * st_rcv[0, b, h] + st_in[b, h]
            q_col = cols_t[:, b * 8 + h:b * 8 + h + 1]
            k_col = cols_t[:, 16 + b * 8 + h:16 + b * 8 + h + 1]
            new = lam * moved + k_col * acts[2][b:b + 1, cols]
            s_out[b, h] = new
            o_v[pl.ds(b, 1), cols] = jnp.sum(q_col * new, axis=0, keepdims=True)
    o = o_v[...]

    def gather_tp(ref, base):
        cs = [remote(ref.at[tp], ref.at[tp], base + i - 1, to_tp(i)) for i in (1, 2, 3)]
        for c in cs:
            c.start()
        return cs

    def settle(cs):
        for c in cs:
            c.wait_recv()
        for c in cs:
            c.wait_send()

    sq_all[tp] = jnp.broadcast_to(jnp.sum(o * o, axis=-1, keepdims=True), (rows, 128))
    cs = gather_tp(sq_all, SQ)
    pump(1)
    ld_og.wait()
    settle(cs)
    sq = ((sq_all[0] + sq_all[1]) + sq_all[2]) + sq_all[3]
    inv = lax.rsqrt(sq[:, :1] / (4 * local_w) + NORM_EPS)
    g_v[...] = (o * inv * og_v[...] * gate).astype(BF16)

    def project(x_ref, w_ref, dst):
        nb = 512

        def body(n, _):
            at = pl.ds(pl.multiple_of(n * nb, nb), nb)
            dst[tp, :, at] = jnp.dot(x_ref[...], w_ref[:, at], preferred_element_type=F32)
            return 0
        lax.fori_loop(0, width // nb, body, 0)

    ld_lout.wait()
    project(g_v, lout_v, po_all)
    cs = gather_tp(po_all, PO)
    reps = in_v.shape[0] // width
    d_id = lax.broadcasted_iota(jnp.int32, rep_v.shape, 0)
    l_id = lax.broadcasted_iota(jnp.int32, rep_v.shape, 1)
    rep_v[...] = jnp.where((l_id >= d_id * reps) & (l_id < d_id * reps + reps), 1.0, 0.0).astype(BF16)
    settle(cs)
    lin = ((po_all[0] + po_all[1]) + po_all[2]) + po_all[3]
    y = (RES_ALPHA * hb[...].astype(F32) + RES_BETA * lin).astype(BF16).astype(F32)

    ld_ag.wait()
    inv = lax.rsqrt(jnp.mean(y * y, axis=-1, keepdims=True) + NORM_EPS)
    hb[...] = (y * inv * ag_v[...]).astype(BF16)
    ld_in.wait()
    ld_rope.wait()
    lane = lax.broadcasted_iota(jnp.int32, (16, 128 * reps), 1)
    sub = lax.broadcasted_iota(jnp.int32, (16, 128 * reps), 0)
    pick = lax.rem(lane, reps) == sub

    def in_body(d, acc):
        xb = hb[:, pl.ds(pl.multiple_of(d * 128, 128), 128)]
        xr = jnp.dot(xb, rep_v[...], preferred_element_type=F32)
        lhs = jnp.concatenate([jnp.where(pick, xr[b:b + 1], 0.0) for b in range(rows)], axis=0).astype(BF16)
        w = in_v[pl.ds(pl.multiple_of(d * 128 * reps, 128), 128 * reps), :]
        return acc + jnp.dot(lhs, w, preferred_element_type=F32)

    proj = lax.fori_loop(0, width // 128, in_body, jnp.zeros((16 * rows, head_dim), F32)).astype(BF16).astype(F32)
    lane = lax.broadcasted_iota(jnp.int32, proj.shape, 1)
    quarter = head_dim // 4
    partner = jnp.where(lane < quarter, pltpu.roll(proj, head_dim - quarter, 1), pltpu.roll(proj, quarter, 1))
    proj_v[...] = proj
    acc_v[...] = (proj * rope_v[0:1] + partner * rope_v[1:2]).astype(BF16).astype(F32)
    qf_v[...] = jnp.zeros_like(qf_v)
    ns_v[...] = jnp.zeros_like(ns_v)
    tail_row = lax.broadcasted_iota(jnp.int32, (CACHE_EXTRA, head_dim), 0)
    for b in range(rows):
        for j in range(kv_dev):
            p = b * kv_dev + j
            for g in range(group):
                qf_v[pl.ds(p * 8 + g, 1), :] = acc_v[pl.ds(b * 16 + g * kv_dev + j, 1), :]
            k_new = acc_v[pl.ds(b * 16 + group * kv_dev + j, 1), :]
            v_new = proj_v[pl.ds(b * 16 + (group + 1) * kv_dev + j, 1), :]
            k_buf[b, j, pl.ds(prompt, CACHE_EXTRA), :] = jnp.where(tail_row == 0, k_new, 0.0).astype(BF16)
            v_buf[b, j, pl.ds(prompt, CACHE_EXTRA), :] = jnp.where(tail_row == 0, v_new, 0.0).astype(BF16)
            vf_v[pl.ds(p * 8, 8), :] = jnp.broadcast_to(v_new, (8, head_dim))
            ns_v[pl.ds(p * 8, 8), :] = jnp.broadcast_to(k_new, (8, head_dim))
    qf = qf_v[...]
    pairs = rows * kv_dev
    my_pairs = pl.ds(sp * pairs, pairs)
    q_all[my_pairs] = qf.astype(BF16).reshape(pairs, 8, head_dim)
    cs = [remote(q_all.at[my_pairs], q_all.at[my_pairs], QX + i - 1, to_sp(i)) for i in (1, 2, 3)]
    for c in cs:
        c.start()
    pump(2)
    scale = head_dim ** -0.5
    ns_v[...] = jnp.broadcast_to(jnp.sum(qf * ns_v[...], axis=-1, keepdims=True) * scale, ns_v.shape)

    n_pairs = 4 * pairs
    slots = kst.shape[0]

    def fetch(cache, i):
        slot = lax.rem(i, slots)
        return pltpu.make_async_copy(cache.at[i // kv_dev, lax.rem(i, kv_dev)], kst.at[slot], ksem.at[slot])

    def stream(cache, first, body):
        def step(i, _):
            fetch(cache, i).wait()
            body(i, kst[lax.rem(i, slots)])

            @pl.when(i + slots < n_pairs)
            def _():
                fetch(cache, i + slots).start()
            return 0
        lax.fori_loop(0, n_pairs, step, 0)

    for i in range(slots):
        fetch(k_cache, jnp.int32(i)).start()
    settle(cs)
    pump(1)

    def score_body(i, keys):
        s = lax.dot_general(q_all[i], keys, (((1,), (1,)), ((), ())), preferred_element_type=F32) * scale
        sc_v[i] = s
        mrow_v[pl.ds(pl.multiple_of(i * 8, 8), 8), :] = jnp.broadcast_to(jnp.max(s, axis=-1, keepdims=True), (8, 128))

    stream(k_cache, 0, score_body)
    for i in range(slots):
        fetch(v_cache, jnp.int32(i)).start()
    my_m = pl.ds(pl.multiple_of(sp * pairs * 8, 8), pairs * 8)
    mrow_v[my_m, :] = jnp.maximum(mrow_v[my_m, :], ns_v[...])
    m_all[sp] = jnp.transpose(mrow_v[...])[:8]
    cs = [remote(m_all.at[sp], m_all.at[sp], MX + i - 1, to_sp(i)) for i in (1, 2, 3)]
    for c in cs:
        c.start()
    pump(1)
    settle(cs)
    m = jnp.maximum(jnp.maximum(m_all[0], m_all[1]), jnp.maximum(m_all[2], m_all[3]))
    mcol_v[...] = jnp.transpose(jnp.broadcast_to(m[:1], (128, 128)))
    pump(1)
    sub = lax.broadcasted_iota(jnp.int32, (8, head_dim), 0)

    def out_body(i, values):
        p = jnp.exp(sc_v[i] - mcol_v[pl.ds(pl.multiple_of(i * 8, 8), 8), :][:, :1])
        total = jnp.broadcast_to(jnp.sum(p, axis=-1, keepdims=True), (8, head_dim))
        o = jnp.dot(p.astype(BF16), values, preferred_element_type=F32)
        ol_v[i] = jnp.where(sub < group, o, pltpu.roll(total, group, 0))

    stream(v_cache, 0, out_body)
    cs = [remote(ol_v.at[pl.ds(flip(sp, i) * pairs, pairs)], olr_v.at[sp], OX + i - 1, to_sp(i)) for i in (1, 2, 3)]
    for c in cs:
        c.start()
    olr_v[sp] = ol_v[my_pairs]
    pump(1)
    settle(cs)
    total = (((olr_v[0] + olr_v[1]) + olr_v[2]) + olr_v[3]).reshape(pairs * 8, head_dim)
    new_p = jnp.exp(ns_v[...] - mcol_v[my_m, :])
    denom = pltpu.roll(total, pairs * 8 - group, 0) + new_p
    numer = total + new_p.astype(BF16).astype(F32) * vf_v[...]
    qf_v[...] = numer / denom
    for b in range(rows):
        for j in range(kv_dev):
            for g in range(group):
                h = j * group + g
                ho_v[pl.ds(b, 1), h * head_dim:(h + 1) * head_dim] = qf_v[pl.ds((b * kv_dev + j) * 8 + g, 1), :]
    g_v[...] = ho_v[...].astype(BF16)
    ld_aout.wait()
    project(g_v, aout_v, pa_all)
    cs = gather_tp(pa_all, PA)
    start_far(len(far))
    settle(cs)
    att = ((pa_all[0] + pa_all[1]) + pa_all[2]) + pa_all[3]
    hid[...] = (RES_ALPHA * hb[...].astype(F32) + RES_BETA * att).astype(BF16)

    st_own.wait_send()
    st_fwd.wait_send()
    st_send.wait_send()
    for c in own_kv:
        c.wait()
    for c in near:
        c.wait()
    for c in far[far_state[1]:]:
        c.wait_send()
    for c in far:
        c.wait_recv()


def write_kernel(k_buf, v_buf, s_buf, hid_buf, hid, s_out, k_out, v_out, sem):
    cs = []
    for src, dst in ((k_buf, k_out), (v_buf, v_out)):
        for b in range(src.shape[0]):
            for j in range(src.shape[1]):
                cs.append(pltpu.make_async_copy(src.at[b, j], dst.at[b, j], sem.at[len(cs)]))
    cs.append(pltpu.make_async_copy(s_buf, s_out, sem.at[len(cs)]))
    cs.append(pltpu.make_async_copy(hid_buf, hid, sem.at[len(cs)]))
    for c in cs:
        c.start()
    for c in cs:
        c.wait()


def solution(mesh):
    def device_step(tokens, states, k_cache, v_cache, slopes, lin_gain, w_lin_qkv, w_lin_gate, out_gain, w_lin_out, attn_gain, w_attn_in, w_attn_out):
        rows, width = tokens.shape
        seqs, kv_dev, shard_len, head_dim = k_cache.shape
        heads = slopes.shape[0]
        local_w = heads * head_dim
        prompt = 4 * shard_len
        reps = w_attn_in.shape[1] * w_attn_in.shape[2]
        pairs = rows * kv_dev
        cache_shape = (rows, kv_dev, prompt + CACHE_EXTRA, head_dim)
        state_shape = (rows, heads, head_dim, head_dim)
        vm, any_ = pltpu.VMEM, pl.ANY
        w_qkv = jnp.transpose(w_lin_qkv, (1, 0, 2))
        w_in = jnp.transpose(w_attn_in, (0, 2, 1, 3)).reshape(width * reps, head_dim)
        rope = jnp.asarray(rope_table(head_dim, prompt))
        dma = pltpu.SemaphoreType.DMA
        k_buf, v_buf, s_buf, hid_buf = pl.pallas_call(
            step_kernel,
            name="step",
            out_shape=(vm(cache_shape, BF16), vm(cache_shape, BF16), vm(state_shape, F32), vm((rows, width), BF16)),
            in_specs=[pl.BlockSpec(memory_space=any_)] * 14,
            out_specs=[pl.BlockSpec(memory_space=vm)] * 4,
            scratch_shapes=[
                vm((rows, width), BF16), vm((1, width), F32), vm((1, local_w), F32), vm((1, width), F32), vm((8, head_dim), F32),
                pltpu.SMEM((heads,), F32), vm((3, width, local_w), BF16), vm((width, local_w), BF16), vm((local_w, width), BF16),
                vm((width * reps, head_dim), BF16), vm((local_w, width), BF16),
                vm((2,) + state_shape, F32), vm((2,) + state_shape, F32), vm(state_shape, F32), vm(state_shape, F32),
                vm((rows, width), BF16), vm((128, head_dim), F32), vm((rows, local_w), F32), vm((rows, local_w), BF16),
                vm((128, 128 * reps), BF16), vm((16 * rows, head_dim), F32), vm((16 * rows, head_dim), F32),
                vm((8 * pairs, head_dim), F32), vm((8 * pairs, head_dim), F32), vm((4 * pairs, 8, head_dim), BF16),
                vm((4 * pairs, 8, shard_len), F32), vm((128, 128), F32), vm((4, 8, 128), F32), vm((128, 128), F32),
                vm((8 * pairs, head_dim), F32), vm((4 * pairs, 8, head_dim), F32), vm((4, pairs, 8, head_dim), F32),
                vm((rows, local_w), F32), vm((4, rows, 128), F32), vm((4, rows, width), F32), vm((4, rows, width), F32),
                vm((4, shard_len, head_dim), BF16),
                dma((NUM_SEMS,)), dma((NUM_SEMS,)), dma((17,)), dma((4,)),
            ],
            compiler_params=pltpu.CompilerParams(collective_id=0, has_side_effects=True, vmem_limit_bytes=46 * MIB),
        )(tokens, states, k_cache, v_cache, slopes, lin_gain.reshape(1, -1), w_qkv, w_lin_gate, out_gain.reshape(1, -1), w_lin_out, attn_gain.reshape(1, -1), w_in, w_attn_out, rope)
        bufs = [pltpu.with_memory_space_constraint(a, vm) for a in (k_buf, v_buf, s_buf, hid_buf)]
        return pl.pallas_call(
            write_kernel,
            name="write",
            out_shape=(jax.ShapeDtypeStruct((rows, width), BF16), jax.ShapeDtypeStruct(state_shape, F32),
                       jax.ShapeDtypeStruct(cache_shape, BF16), jax.ShapeDtypeStruct(cache_shape, BF16)),
            in_specs=[pl.BlockSpec(memory_space=vm)] * 4,
            out_specs=[pl.BlockSpec(memory_space=any_)] * 4,
            scratch_shapes=[dma((10,))],
            compiler_params=pltpu.CompilerParams(vmem_limit_bytes=20 * MIB),
        )(*bufs)

    batch_spec = P(('dp', 'sp'), None)
    head_spec = P(('dp', 'sp'), 'tp', None, None)
    cache_spec = P('dp', 'tp', 'sp', None)
    in_specs = (batch_spec, P('sp', 'dp', 'tp', None, None), cache_spec, cache_spec, P('tp'), P(None), P(None, None, 'tp'), P(None, 'tp'), P('tp'), P('tp', None), P(None), P(None, 'tp', None, None), P('tp', None))
    out_specs = (batch_spec, head_spec, head_spec, head_spec)
    return jax.shard_map(device_step, mesh=mesh, in_specs=in_specs, out_specs=out_specs, check_vma=False)
```

```python
import math

import jax
import jax.numpy as jnp
import numpy as np
from jax import lax
from jax.experimental import pallas as pl
from jax.experimental.pallas import tpu as pltpu
from jax.sharding import PartitionSpec as P

NORM_EPS = 1e-6
ROPE_BASE = 10000000.0
RES_ALPHA = 1.0
RES_BETA = 1.0
CACHE_EXTRA = 16

MESH = pl.DeviceIdType.MESH
F32 = jnp.float32
BF16 = jnp.bfloat16
MIB = 2**20

ST_OWN, ST_FWD, ST_SUM = 0, 1, 2
SQ, PO, PA = 3, 6, 9
QX, MX, OX = 12, 15, 18
KV_NEAR = 21
KV_FAR = 23
NUM_SEMS = KV_FAR + 16
LATE = 2


def rope_table(head_dim, position):
    rope_dim = head_dim // 2
    half = rope_dim // 2
    inv_freq = ROPE_BASE ** (-np.arange(0, rope_dim, 2, dtype=np.float64) / rope_dim)
    cos, sin = np.cos(position * inv_freq), np.sin(position * inv_freq)
    table = np.zeros((8, head_dim), np.float32)
    table[0] = np.concatenate([cos, cos, np.ones(head_dim - rope_dim)])
    table[1, :rope_dim] = np.concatenate([-sin, sin])
    return table


def flip(index, mask):
    chip, core = index // 2, index % 2
    if mask & 2:
        chip = 1 - chip
    if mask & 1:
        core = 1 - core
    return chip * 2 + core


def silu(x):
    return x * (1.0 / (1.0 + jnp.exp(-x)))


def step_kernel(
    tokens, states, k_cache, v_cache, slopes, lin_gain, w_qkv, w_gate, out_gain, w_lin_out, attn_gain, w_in, w_attn_out, rope,
    k_buf, v_buf, s_out, hid,
    tok_v, lg_v, og_v, ag_v, rope_v, slope_s, qkv_v, gate_v, lout_v, in_v, aout_v,
    st_loc, st_rcv, st_sum, st_in, hb, rows_v, o_v, g_v, rep_v, acc_v, proj_v, qf_v, vf_v, qp_v, q_snd, q_all, sc_v, mrow_v, m_all, mcol_v,
    ns_v, ol_v, olr_v, ho_v, sq_all, po_all, pa_all, kst,
    send, recv, lsem, ksem, met,
):
    sp = lax.axis_index("sp")
    tp = lax.axis_index("tp")
    shard_len = k_cache.shape[2]
    kv_dev = k_cache.shape[1]
    head_dim = k_cache.shape[3]
    heads = slopes.shape[0]
    rows = tokens.shape[0]
    width = tokens.shape[1]
    group = heads // kv_dev
    prompt = 4 * shard_len
    local_w = heads * head_dim

    def to_sp(mask):
        return {"sp": flip(sp, mask)}

    def to_tp(off):
        return {"tp": lax.rem(tp + off, 4)}

    core = lax.rem(sp, 2)
    barrier = pltpu.get_barrier_semaphore()
    for i in (2, 3, 1):
        pl.semaphore_signal(barrier, inc=1, device_id=to_sp(i), device_id_type=MESH)

    @pl.when(core == 1)
    def _():
        pl.semaphore_wait(barrier, 3)
        pl.semaphore_signal(met.at[0], inc=1, device_id=to_sp(1), device_id_type=MESH)

    @pl.when(core == 0)
    def _():
        pl.semaphore_wait(met.at[0], 1)
        for i in (1, 2, 3):
            pl.semaphore_signal(barrier, inc=1, device_id=to_tp(i), device_id_type=MESH)

    def meet_tp():
        @pl.when(core == 0)
        def _():
            pl.semaphore_wait(barrier, 6)
            pl.semaphore_signal(met.at[1], inc=1, device_id=to_sp(1), device_id_type=MESH)

        @pl.when(core == 1)
        def _():
            pl.semaphore_wait(met.at[1], 1)

    def remote(src, dst, i, dev):
        return pltpu.make_async_remote_copy(src, dst, send.at[i], recv.at[i], device_id=dev, device_id_type=MESH)

    def local(src, dst, i):
        return pltpu.make_async_copy(src, dst, lsem.at[i])

    my_rows = pl.ds(pl.multiple_of(sp * shard_len, shard_len), shard_len)
    pieces = [(t, b, j, mask) for t in range(2) for b in range(rows) for j in range(kv_dev) for mask in (2, 3)]
    late = [(1, rows - 1, j, 2) for j in range(kv_dev)[-LATE:]]
    pieces = [p for p in pieces if p not in late] + late
    far = []
    for t, b, j, mask in pieces:
        src, dst = ((k_cache, k_buf), (v_cache, v_buf))[t]
        far.append(remote(src.at[flip(sp, mask) * rows + b, j], dst.at[b, j, my_rows], KV_FAR + len(far), to_sp(mask)))
    n_both = len(far) - len(late)
    far_state = [0, 0]

    def start_far(n):
        for _ in range(n):
            if far_state[0] < n_both:
                far[far_state[0]].start()
                far_state[0] += 1

    def pump(n):
        for _ in range(n):
            far[far_state[1]].wait_send()
            far_state[1] += 1
            start_far(1)

    def st_rows(g):
        return pl.ds(g * rows, rows)

    st_own = remote(states.at[0, st_rows(flip(sp, 1))], st_rcv.at[0], ST_OWN, to_sp(1))
    st_fwd = remote(states.at[0, st_rows(flip(sp, 3))], st_rcv.at[1], ST_FWD, to_sp(1))
    st_fwd.start()
    start_far(1)
    ld_fwd = local(states.at[0, st_rows(flip(sp, 2))], st_loc.at[1], 0)
    ld_slope = local(slopes, slope_s, 1)
    ld_fwd.start()
    ld_slope.start()
    st_own.start()
    ld_own = local(states.at[0, st_rows(sp)], st_loc.at[0], 2)
    ld_tok = local(tokens, tok_v, 3)
    ld_lg = local(lin_gain, lg_v, 4)
    ld_og = local(out_gain, og_v, 5)
    ld_ag = local(attn_gain, ag_v, 6)
    ld_rope = local(rope, rope_v, 7)
    ld_qkv = [local(w_qkv.at[j], qkv_v.at[j], 8 + j) for j in range(3)]
    ld_gate = local(w_gate, gate_v, 11)
    ld_lout = local(w_lin_out, lout_v, 12)
    ld_in = local(w_in, in_v, 13)
    ld_aout = local(w_attn_out, aout_v, 14)
    own_kv = [local(src.at[st_rows(sp)], dst.at[:, :, my_rows], 15 + t) for t, (src, dst) in enumerate(((k_cache, k_buf), (v_cache, v_buf)))]
    near = [remote(src.at[st_rows(flip(sp, 1))], dst.at[:, :, my_rows], KV_NEAR + t, to_sp(1)) for t, (src, dst) in enumerate(((k_cache, k_buf), (v_cache, v_buf)))]
    for c in [ld_own, ld_tok, ld_lg, ld_og, ld_ag, ld_rope] + ld_qkv + [ld_gate, ld_lout, ld_in, ld_aout] + near + own_kv:
        c.start()

    def decay(h, shard):
        off = (shard_len * (3 - shard)).astype(F32)
        return jnp.exp(jnp.full((1, head_dim), -slope_s[h] * off, F32))

    ld_slope.wait()
    ld_fwd.wait()
    st_fwd.wait_recv()
    for h in range(heads):
        w_me, w_ot = decay(h, sp), decay(h, flip(sp, 1))
        for b in range(rows):
            st_sum[b, h] = w_me * st_loc[1, b, h] + w_ot * st_rcv[1, b, h]
    st_send = remote(st_sum, st_in, ST_SUM, to_sp(2))
    st_send.start()
    start_far(2)

    ld_tok.wait()
    ld_lg.wait()
    x = tok_v[...].astype(F32)
    inv = lax.rsqrt(jnp.mean(x * x, axis=-1, keepdims=True) + NORM_EPS)
    hb[...] = (x * inv * lg_v[...]).astype(BF16)

    def matvec(x_ref, w_ref, k_len, n_len, kb, out_dtype=F32):
        def body(k, acc):
            at = pl.ds(pl.multiple_of(k * kb, kb), kb)
            return acc + jnp.dot(x_ref[:, at], w_ref[at, :], preferred_element_type=F32)
        return lax.fori_loop(0, k_len // kb, body, jnp.zeros((rows, n_len), F32))

    acts = []
    for j in range(3):
        ld_qkv[j].wait()
        acts.append(silu(matvec(hb, qkv_v.at[j], width, local_w, 256)).astype(BF16).astype(F32))
    ld_gate.wait()
    gate = 1.0 / (1.0 + jnp.exp(-matvec(hb, gate_v, width, local_w, 256)))
    rows_v[...] = jnp.zeros_like(rows_v)
    for b in range(rows):
        for h in range(heads):
            cols = slice(h * head_dim, (h + 1) * head_dim)
            rows_v[pl.ds(b * 8 + h, 1), :] = acts[0][b:b + 1, cols]
            rows_v[pl.ds(16 + b * 8 + h, 1), :] = acts[1][b:b + 1, cols]
    cols_t = jnp.transpose(rows_v[...])

    ld_own.wait()
    st_own.wait_recv()
    st_send.wait_recv()
    for h in range(heads):
        w_me, w_ot = decay(h, sp), decay(h, flip(sp, 1))
        lam = jnp.exp(jnp.full((1, head_dim), -slope_s[h], F32))
        cols = slice(h * head_dim, (h + 1) * head_dim)
        for b in range(rows):
            moved = w_me * st_loc[0, b, h] + w_ot * st_rcv[0, b, h] + st_in[b, h]
            q_col = cols_t[:, b * 8 + h:b * 8 + h + 1]
            k_col = cols_t[:, 16 + b * 8 + h:16 + b * 8 + h + 1]
            new = lam * moved + k_col * acts[2][b:b + 1, cols]
            s_out[b, h] = new
            o_v[pl.ds(b, 1), cols] = jnp.sum(q_col * new, axis=0, keepdims=True)
    o = o_v[...]

    def gather_tp(ref, base):
        cs = [remote(ref.at[tp], ref.at[tp], base + i - 1, to_tp(i)) for i in (1, 2, 3)]
        for c in cs:
            c.start()
        return cs

    def settle(cs):
        for c in cs:
            c.wait_recv()
        for c in cs:
            c.wait_send()

    sq_all[tp] = jnp.broadcast_to(jnp.sum(o * o, axis=-1, keepdims=True), (rows, 128))
    meet_tp()
    cs = gather_tp(sq_all, SQ)
    pump(1)
    ld_og.wait()
    settle(cs)
    sq = ((sq_all[0] + sq_all[1]) + sq_all[2]) + sq_all[3]
    inv = lax.rsqrt(sq[:, :1] / (4 * local_w) + NORM_EPS)
    out_g = jnp.concatenate([og_v[h:h + 1, :] for h in range(heads)], axis=1)
    g_v[...] = (o * inv * out_g * gate).astype(BF16)

    def project(x_ref, w_ref, dst):
        nb = 512

        def body(n, _):
            at = pl.ds(pl.multiple_of(n * nb, nb), nb)
            dst[tp, :, at] = jnp.dot(x_ref[...], w_ref[:, at], preferred_element_type=F32)
            return 0
        lax.fori_loop(0, width // nb, body, 0)

    ld_lout.wait()
    project(g_v, lout_v, po_all)
    cs = gather_tp(po_all, PO)
    reps = in_v.shape[0] // width
    d_id = lax.broadcasted_iota(jnp.int32, rep_v.shape, 0)
    l_id = lax.broadcasted_iota(jnp.int32, rep_v.shape, 1)
    rep_v[...] = jnp.where((l_id >= d_id * reps) & (l_id < d_id * reps + reps), 1.0, 0.0).astype(BF16)
    settle(cs)
    lin = ((po_all[0] + po_all[1]) + po_all[2]) + po_all[3]
    y = (RES_ALPHA * hb[...].astype(F32) + RES_BETA * lin).astype(BF16).astype(F32)

    ld_ag.wait()
    inv = lax.rsqrt(jnp.mean(y * y, axis=-1, keepdims=True) + NORM_EPS)
    hb[...] = (y * inv * ag_v[...]).astype(BF16)
    ld_in.wait()
    ld_rope.wait()
    lane = lax.broadcasted_iota(jnp.int32, (16, 128 * reps), 1)
    sub = lax.broadcasted_iota(jnp.int32, (16, 128 * reps), 0)
    pick = lax.rem(lane, reps) == sub

    def in_body(d, acc):
        xb = hb[:, pl.ds(pl.multiple_of(d * 128, 128), 128)]
        xr = jnp.dot(xb, rep_v[...], preferred_element_type=F32)
        lhs = jnp.concatenate([jnp.where(pick, xr[b:b + 1], 0.0) for b in range(rows)], axis=0).astype(BF16)
        w = in_v[pl.ds(pl.multiple_of(d * 128 * reps, 128), 128 * reps), :]
        return acc + jnp.dot(lhs, w, preferred_element_type=F32)

    proj = lax.fori_loop(0, width // 128, in_body, jnp.zeros((16 * rows, head_dim), F32)).astype(BF16).astype(F32)
    lane = lax.broadcasted_iota(jnp.int32, proj.shape, 1)
    quarter = head_dim // 4
    partner = jnp.where(lane < quarter, pltpu.roll(proj, head_dim - quarter, 1), pltpu.roll(proj, quarter, 1))
    proj_v[...] = proj
    acc_v[...] = (proj * rope_v[0:1] + partner * rope_v[1:2]).astype(BF16).astype(F32)
    qf_v[...] = jnp.zeros_like(qf_v)
    qp_v[...] = jnp.zeros_like(qp_v)
    ns_v[...] = jnp.zeros_like(ns_v)
    tail_row = lax.broadcasted_iota(jnp.int32, (CACHE_EXTRA, head_dim), 0)
    for b in range(rows):
        for j in range(kv_dev):
            p = b * kv_dev + j
            for g in range(group):
                q_row = acc_v[pl.ds(b * 16 + g * kv_dev + j, 1), :]
                qf_v[pl.ds(p * 8 + g, 1), :] = q_row
                qp_v[pl.ds(p * 4 + g, 1), :] = q_row
            k_new = acc_v[pl.ds(b * 16 + group * kv_dev + j, 1), :]
            v_new = proj_v[pl.ds(b * 16 + (group + 1) * kv_dev + j, 1), :]
            k_buf[b, j, pl.ds(prompt, CACHE_EXTRA), :] = jnp.where(tail_row == 0, k_new, 0.0).astype(BF16)
            v_buf[b, j, pl.ds(prompt, CACHE_EXTRA), :] = jnp.where(tail_row == 0, v_new, 0.0).astype(BF16)
            vf_v[pl.ds(p * 8, 8), :] = jnp.broadcast_to(v_new, (8, head_dim))
            ns_v[pl.ds(p * 8, 8), :] = jnp.broadcast_to(k_new, (8, head_dim))
    qf = qf_v[...]
    pairs = rows * kv_dev
    my_pairs = pl.ds(sp * pairs, pairs)
    q_snd[sp] = qp_v[...].astype(BF16)
    cs = [remote(q_snd.at[sp], q_snd.at[sp], QX + i - 1, to_sp(i)) for i in (1, 2, 3)]
    for c in cs:
        c.start()
    pump(2)
    scale = head_dim ** -0.5
    ns_v[...] = jnp.broadcast_to(jnp.sum(qf * ns_v[...], axis=-1, keepdims=True) * scale, ns_v.shape)

    n_pairs = 4 * pairs
    slots = kst.shape[0]

    def fetch(cache, i):
        slot = lax.rem(i, slots)
        return pltpu.make_async_copy(cache.at[i // kv_dev, lax.rem(i, kv_dev)], kst.at[slot], ksem.at[slot])

    def stream(cache, first, body):
        def step(i, _):
            fetch(cache, i).wait()
            body(i, kst[lax.rem(i, slots)])

            @pl.when(i + slots < n_pairs)
            def _():
                fetch(cache, i + slots).start()
            return 0
        lax.fori_loop(0, n_pairs, step, 0)

    for i in range(slots):
        fetch(k_cache, jnp.int32(i)).start()
    settle(cs)
    pump(1)
    for d in range(4):
        got = q_snd[d].astype(F32)
        for p in range(pairs):
            q_all[d * pairs + p] = jnp.concatenate([got[p * 4:p * 4 + 4], jnp.zeros((4, head_dim), F32)], axis=0).astype(BF16)

    def score_body(i, keys):
        s = lax.dot_general(q_all[i], keys, (((1,), (1,)), ((), ())), preferred_element_type=F32) * scale
        sc_v[i] = s
        mrow_v[pl.ds(pl.multiple_of(i * 8, 8), 8), :] = jnp.broadcast_to(jnp.max(s, axis=-1, keepdims=True), (8, 128))

    stream(k_cache, 0, score_body)
    for i in range(slots):
        fetch(v_cache, jnp.int32(i)).start()
    my_m = pl.ds(pl.multiple_of(sp * pairs * 8, 8), pairs * 8)
    mrow_v[my_m, :] = jnp.maximum(mrow_v[my_m, :], ns_v[...])
    m_all[sp] = jnp.transpose(mrow_v[...])[:1]
    cs = [remote(m_all.at[sp], m_all.at[sp], MX + i - 1, to_sp(i)) for i in (1, 2, 3)]
    for c in cs:
        c.start()
    pump(1)
    settle(cs)
    m = jnp.maximum(jnp.maximum(m_all[0], m_all[1]), jnp.maximum(m_all[2], m_all[3]))
    mcol_v[...] = jnp.transpose(jnp.broadcast_to(m, (128, 128)))
    pump(1)
    lane = lax.broadcasted_iota(jnp.int32, (1, head_dim), 1)

    def out_body(i, values):
        p = jnp.exp(sc_v[i] - mcol_v[pl.ds(pl.multiple_of(i * 8, 8), 8), :][:, :1])
        total = jnp.sum(p, axis=-1, keepdims=True)
        o = jnp.dot(p.astype(BF16), values, preferred_element_type=F32)
        sums = jnp.zeros((1, head_dim), F32)
        for g in range(group):
            sums = jnp.where(lane == g, total[g:g + 1], sums)
        ol_v[i] = jnp.concatenate([o[:group], sums], axis=0)

    stream(v_cache, 0, out_body)
    cs = [remote(ol_v.at[pl.ds(flip(sp, i) * pairs, pairs)], olr_v.at[sp], OX + i - 1, to_sp(i)) for i in (1, 2, 3)]
    for c in cs:
        c.start()
    olr_v[sp] = ol_v[my_pairs]
    pump(1)
    settle(cs)
    new_p = jnp.exp(ns_v[...] - mcol_v[my_m, :])
    new_o = new_p.astype(BF16).astype(F32) * vf_v[...]
    for b in range(rows):
        for j in range(kv_dev):
            p = b * kv_dev + j
            total = ((olr_v[0, p] + olr_v[1, p]) + olr_v[2, p]) + olr_v[3, p]
            for g in range(group):
                h, at = j * group + g, p * 8 + g
                denom = total[group:group + 1, g:g + 1] + new_p[at:at + 1]
                ho_v[pl.ds(b, 1), h * head_dim:(h + 1) * head_dim] = (total[g:g + 1] + new_o[at:at + 1]) / denom
    g_v[...] = ho_v[...].astype(BF16)
    ld_aout.wait()
    project(g_v, aout_v, pa_all)
    cs = gather_tp(pa_all, PA)
    start_far(len(far))

    @pl.when(core == 1)
    def _():
        for c in far[n_both:]:
            c.start()

    settle(cs)
    att = ((pa_all[0] + pa_all[1]) + pa_all[2]) + pa_all[3]
    hid[...] = (RES_ALPHA * hb[...].astype(F32) + RES_BETA * att).astype(BF16)

    st_own.wait_send()
    st_fwd.wait_send()
    st_send.wait_send()
    for c in own_kv:
        c.wait()
    for c in near:
        c.wait()
    for c in far[far_state[1]:n_both]:
        c.wait_send()
    for c in far[:n_both]:
        c.wait_recv()

    @pl.when(core == 1)
    def _():
        for c in far[n_both:]:
            c.wait()


def tail_kernel(v_cache, token, x_buf, send, recv):
    sp = lax.axis_index("sp")
    rows = v_cache.shape[0] // 4
    kv_dev = v_cache.shape[1]
    peer = flip(sp, 2)
    barrier = pltpu.get_barrier_semaphore()
    pl.semaphore_signal(barrier, inc=1, device_id={"sp": peer}, device_id_type=MESH)
    pl.semaphore_wait(barrier, 1)

    @pl.when(lax.rem(sp, 2) == 0)
    def _():
        cs = []
        for i in range(LATE):
            cs.append(pltpu.make_async_remote_copy(
                v_cache.at[peer * rows + rows - 1, kv_dev - LATE + i], x_buf.at[i], send.at[i], recv.at[i], device_id={"sp": peer}, device_id_type=MESH))
            cs[-1].start()
        for c in cs:
            c.wait()


def tail_write_kernel(v_in, x_buf, v_out, sem):
    sp = lax.axis_index("sp")
    rows, kv_dev = v_out.shape[:2]
    shard_len = x_buf.shape[1]

    @pl.when(lax.rem(sp, 2) == 0)
    def _():
        cs = []
        for i in range(LATE):
            at = pl.ds(pl.multiple_of(flip(sp, 2) * shard_len, shard_len), shard_len)
            cs.append(pltpu.make_async_copy(x_buf.at[i], v_out.at[rows - 1, kv_dev - LATE + i, at], sem.at[i]))
            cs[-1].start()
        for c in cs:
            c.wait()


def write_kernel(k_buf, v_buf, s_buf, hid_buf, hid, s_out, k_out, v_out, token, sem):
    token[...] = jnp.zeros_like(token)
    cs = []
    for src, dst in ((k_buf, k_out), (v_buf, v_out)):
        for b in range(src.shape[0]):
            for j in range(src.shape[1]):
                cs.append(pltpu.make_async_copy(src.at[b, j], dst.at[b, j], sem.at[len(cs)]))
    cs.append(pltpu.make_async_copy(s_buf, s_out, sem.at[len(cs)]))
    cs.append(pltpu.make_async_copy(hid_buf, hid, sem.at[len(cs)]))
    for c in cs:
        c.start()
    for c in cs:
        c.wait()


def solution(mesh):
    def device_step(tokens, states, k_cache, v_cache, slopes, lin_gain, w_lin_qkv, w_lin_gate, out_gain, w_lin_out, attn_gain, w_attn_in, w_attn_out):
        rows, width = tokens.shape
        seqs, kv_dev, shard_len, head_dim = k_cache.shape
        heads = slopes.shape[0]
        local_w = heads * head_dim
        prompt = 4 * shard_len
        reps = w_attn_in.shape[1] * w_attn_in.shape[2]
        pairs = rows * kv_dev
        group = heads // kv_dev
        cache_shape = (rows, kv_dev, prompt + CACHE_EXTRA, head_dim)
        state_shape = (rows, heads, head_dim, head_dim)
        vm, any_ = pltpu.VMEM, pl.ANY
        w_qkv = jnp.transpose(w_lin_qkv, (1, 0, 2))
        w_in = jnp.transpose(w_attn_in, (0, 2, 1, 3)).reshape(width * reps, head_dim)
        rope = jnp.asarray(rope_table(head_dim, prompt))
        dma = pltpu.SemaphoreType.DMA
        k_buf, v_buf, s_buf, hid_buf = pl.pallas_call(
            step_kernel,
            name="step",
            out_shape=(vm(cache_shape, BF16), vm(cache_shape, BF16), vm(state_shape, F32), vm((rows, width), BF16)),
            in_specs=[pl.BlockSpec(memory_space=any_)] * 14,
            out_specs=[pl.BlockSpec(memory_space=vm)] * 4,
            scratch_shapes=[
                vm((rows, width), BF16), vm((1, width), F32), vm((heads, head_dim), F32), vm((1, width), F32), vm((8, head_dim), F32),
                pltpu.SMEM((heads,), F32), vm((3, width, local_w), BF16), vm((width, local_w), BF16), vm((local_w, width), BF16),
                vm((width * reps, head_dim), BF16), vm((local_w, width), BF16),
                vm((2,) + state_shape, F32), vm((2,) + state_shape, F32), vm(state_shape, F32), vm(state_shape, F32),
                vm((rows, width), BF16), vm((128, head_dim), F32), vm((rows, local_w), F32), vm((rows, local_w), BF16),
                vm((128, 128 * reps), BF16), vm((16 * rows, head_dim), F32), vm((16 * rows, head_dim), F32),
                vm((8 * pairs, head_dim), F32), vm((8 * pairs, head_dim), F32), vm((4 * pairs, head_dim), F32), vm((4, 4 * pairs, head_dim), BF16), vm((4 * pairs, 8, head_dim), BF16),
                vm((4 * pairs, 8, shard_len), F32), vm((128, 128), F32), vm((4, 1, 128), F32), vm((128, 128), F32),
                vm((8 * pairs, head_dim), F32), vm((4 * pairs, group + 1, head_dim), F32), vm((4, pairs, group + 1, head_dim), F32),
                vm((rows, local_w), F32), vm((4, rows, 128), F32), vm((4, rows, width), F32), vm((4, rows, width), F32),
                vm((4, shard_len, head_dim), BF16),
                dma((NUM_SEMS,)), dma((NUM_SEMS,)), dma((17,)), dma((4,)), pltpu.SemaphoreType.REGULAR((2,)),
            ],
            compiler_params=pltpu.CompilerParams(collective_id=0, has_side_effects=True, vmem_limit_bytes=46 * MIB),
        )(tokens, states, k_cache, v_cache, slopes, lin_gain.reshape(1, -1), w_qkv, w_lin_gate, out_gain.reshape(heads, head_dim), w_lin_out, attn_gain.reshape(1, -1), w_in, w_attn_out, rope)
        bufs = [pltpu.with_memory_space_constraint(a, vm) for a in (k_buf, v_buf, s_buf, hid_buf)]
        hid, s_out, k_out, v_out, token = pl.pallas_call(
            write_kernel,
            name="write",
            out_shape=(jax.ShapeDtypeStruct((rows, width), BF16), jax.ShapeDtypeStruct(state_shape, F32),
                       jax.ShapeDtypeStruct(cache_shape, BF16), jax.ShapeDtypeStruct(cache_shape, BF16), vm((8, 128), F32)),
            in_specs=[pl.BlockSpec(memory_space=vm)] * 4,
            out_specs=[pl.BlockSpec(memory_space=any_)] * 4 + [pl.BlockSpec(memory_space=vm)],
            scratch_shapes=[dma((10,))],
            compiler_params=pltpu.CompilerParams(vmem_limit_bytes=20 * MIB),
        )(*bufs)
        x_buf = pl.pallas_call(
            tail_kernel,
            name="tail",
            out_shape=vm((LATE, shard_len, head_dim), BF16),
            in_specs=[pl.BlockSpec(memory_space=any_), pl.BlockSpec(memory_space=vm)],
            out_specs=pl.BlockSpec(memory_space=vm),
            scratch_shapes=[dma((LATE,)), dma((LATE,))],
            compiler_params=pltpu.CompilerParams(collective_id=1, has_side_effects=True, vmem_limit_bytes=4 * MIB),
        )(pltpu.with_memory_space_constraint(v_cache, pltpu.HBM), pltpu.with_memory_space_constraint(token, vm))
        v_out = pl.pallas_call(
            tail_write_kernel,
            name="tail_write",
            out_shape=jax.ShapeDtypeStruct(cache_shape, BF16),
            in_specs=[pl.BlockSpec(memory_space=any_), pl.BlockSpec(memory_space=vm)],
            out_specs=pl.BlockSpec(memory_space=any_),
            scratch_shapes=[dma((LATE,))],
            input_output_aliases={0: 0},
            compiler_params=pltpu.CompilerParams(vmem_limit_bytes=4 * MIB),
        )(v_out, pltpu.with_memory_space_constraint(x_buf, vm))
        return hid, s_out, k_out, v_out

    batch_spec = P(('dp', 'sp'), None)
    head_spec = P(('dp', 'sp'), 'tp', None, None)
    cache_spec = P('dp', 'tp', 'sp', None)
    in_specs = (batch_spec, P('sp', 'dp', 'tp', None, None), cache_spec, cache_spec, P('tp'), P(None), P(None, None, 'tp'), P(None, 'tp'), P('tp'), P('tp', None), P(None), P(None, 'tp', None, None), P('tp', None))
    out_specs = (batch_spec, head_spec, head_spec, head_spec)
    return jax.shard_map(device_step, mesh=mesh, in_specs=in_specs, out_specs=out_specs, check_vma=False)
```

```python
import math

import jax
import jax.numpy as jnp
import numpy as np
from jax import lax
from jax.experimental import pallas as pl
from jax.experimental.pallas import tpu as pltpu
from jax.sharding import PartitionSpec as P

NORM_EPS = 1e-6
ROPE_BASE = 10000000.0
RES_ALPHA = 1.0
RES_BETA = 1.0
CACHE_EXTRA = 16

MESH = pl.DeviceIdType.MESH
F32 = jnp.float32
BF16 = jnp.bfloat16
MIB = 2**20

ST_OWN, ST_FWD, ST_SUM = 0, 1, 2
SQ, PO, PA = 3, 6, 9
QX, MX, OX = 12, 15, 18
KV_NEAR = 21
KV_FAR = 23
NUM_SEMS = KV_FAR + 16
LATE = 2


def rope_table(head_dim, position):
    rope_dim = head_dim // 2
    half = rope_dim // 2
    inv_freq = ROPE_BASE ** (-np.arange(0, rope_dim, 2, dtype=np.float64) / rope_dim)
    cos, sin = np.cos(position * inv_freq), np.sin(position * inv_freq)
    table = np.zeros((8, head_dim), np.float32)
    table[0] = np.concatenate([cos, cos, np.ones(head_dim - rope_dim)])
    table[1, :rope_dim] = np.concatenate([-sin, sin])
    return table


def flip(index, mask):
    chip, core = index // 2, index % 2
    if mask & 2:
        chip = 1 - chip
    if mask & 1:
        core = 1 - core
    return chip * 2 + core


def silu(x):
    return x * (1.0 / (1.0 + jnp.exp(-x)))


def step_kernel(
    tokens, states, k_cache, v_cache, slopes, lin_gain, w_qkv, w_gate, out_gain, w_lin_out, attn_gain, w_in, w_attn_out, rope,
    k_buf, v_buf, s_out, hid,
    tok_v, lg_v, og_v, ag_v, rope_v, slope_s, qkv_v, gate_v, lout_v, in_v, aout_v,
    st_loc, st_rcv, st_sum, st_in, hb, rows_v, o_v, g_v, rep_v, acc_v, proj_v, qf_v, vf_v, qp_v, q_snd, q_all, sc_v, mrow_v, m_all, mcol_v,
    ns_v, ol_v, olr_v, ho_v, sq_all, po_all, pa_all, kst,
    send, recv, lsem, ksem, met,
):
    sp = lax.axis_index("sp")
    tp = lax.axis_index("tp")
    shard_len = k_cache.shape[2]
    kv_dev = k_cache.shape[1]
    head_dim = k_cache.shape[3]
    heads = slopes.shape[0]
    rows = tokens.shape[0]
    width = tokens.shape[1]
    group = heads // kv_dev
    prompt = 4 * shard_len
    local_w = heads * head_dim

    def to_sp(mask):
        return {"sp": flip(sp, mask)}

    def to_tp(off):
        return {"tp": lax.rem(tp + off, 4)}

    core = lax.rem(sp, 2)
    barrier = pltpu.get_barrier_semaphore()
    for i in (2, 3, 1):
        pl.semaphore_signal(barrier, inc=1, device_id=to_sp(i), device_id_type=MESH)

    @pl.when(core == 0)
    def _():
        pl.semaphore_wait(barrier, 3)
        pl.semaphore_signal(met.at[0], inc=1, device_id=to_sp(1), device_id_type=MESH)

    @pl.when(core == 1)
    def _():
        pl.semaphore_wait(met.at[0], 1)
        for i in (1, 2, 3):
            pl.semaphore_signal(barrier, inc=1, device_id=to_tp(i), device_id_type=MESH)

    def meet_tp():
        @pl.when(core == 1)
        def _():
            pl.semaphore_wait(barrier, 6)
            pl.semaphore_signal(met.at[1], inc=1, device_id=to_sp(1), device_id_type=MESH)

        @pl.when(core == 0)
        def _():
            pl.semaphore_wait(met.at[1], 1)

    def remote(src, dst, i, dev):
        return pltpu.make_async_remote_copy(src, dst, send.at[i], recv.at[i], device_id=dev, device_id_type=MESH)

    def local(src, dst, i):
        return pltpu.make_async_copy(src, dst, lsem.at[i])

    my_rows = pl.ds(pl.multiple_of(sp * shard_len, shard_len), shard_len)
    pieces = [(t, b, j, mask) for t in range(2) for b in range(rows) for j in range(kv_dev) for mask in (2, 3)]
    late = [(1, rows - 1, j, 2) for j in range(kv_dev)[-LATE:]]
    pieces = [p for p in pieces if p not in late] + late
    far = []
    for t, b, j, mask in pieces:
        src, dst = ((k_cache, k_buf), (v_cache, v_buf))[t]
        far.append(remote(src.at[flip(sp, mask) * rows + b, j], dst.at[b, j, my_rows], KV_FAR + len(far), to_sp(mask)))
    n_both = len(far) - len(late)
    far_state = [0, 0]

    def start_far(n):
        for _ in range(n):
            if far_state[0] < n_both:
                far[far_state[0]].start()
                far_state[0] += 1

    def pump(n):
        for _ in range(n):
            far[far_state[1]].wait_send()
            far_state[1] += 1
            start_far(1)

    def st_rows(g):
        return pl.ds(g * rows, rows)

    st_own = remote(states.at[0, st_rows(flip(sp, 1))], st_rcv.at[0], ST_OWN, to_sp(1))
    st_fwd = remote(states.at[0, st_rows(flip(sp, 3))], st_rcv.at[1], ST_FWD, to_sp(1))
    st_fwd.start()
    start_far(1)
    ld_fwd = local(states.at[0, st_rows(flip(sp, 2))], st_loc.at[1], 0)
    ld_slope = local(slopes, slope_s, 1)
    ld_fwd.start()
    ld_slope.start()
    st_own.start()
    ld_own = local(states.at[0, st_rows(sp)], st_loc.at[0], 2)
    ld_tok = local(tokens, tok_v, 3)
    ld_lg = local(lin_gain, lg_v, 4)
    ld_og = local(out_gain, og_v, 5)
    ld_ag = local(attn_gain, ag_v, 6)
    ld_rope = local(rope, rope_v, 7)
    ld_qkv = [local(w_qkv.at[j], qkv_v.at[j], 8 + j) for j in range(3)]
    ld_gate = local(w_gate, gate_v, 11)
    ld_lout = local(w_lin_out, lout_v, 12)
    ld_in = local(w_in, in_v, 13)
    ld_aout = local(w_attn_out, aout_v, 14)
    own_kv = [local(src.at[st_rows(sp)], dst.at[:, :, my_rows], 15 + t) for t, (src, dst) in enumerate(((k_cache, k_buf), (v_cache, v_buf)))]
    near = [remote(src.at[st_rows(flip(sp, 1))], dst.at[:, :, my_rows], KV_NEAR + t, to_sp(1)) for t, (src, dst) in enumerate(((k_cache, k_buf), (v_cache, v_buf)))]
    for c in [ld_own, ld_tok, ld_lg, ld_og, ld_ag, ld_rope] + ld_qkv + [ld_gate, ld_lout, ld_in, ld_aout] + near + own_kv:
        c.start()

    def decay(h, shard):
        off = (shard_len * (3 - shard)).astype(F32)
        return jnp.exp(jnp.full((1, head_dim), -slope_s[h] * off, F32))

    ld_slope.wait()
    ld_fwd.wait()
    st_fwd.wait_recv()
    for h in range(heads):
        w_me, w_ot = decay(h, sp), decay(h, flip(sp, 1))
        for b in range(rows):
            st_sum[b, h] = w_me * st_loc[1, b, h] + w_ot * st_rcv[1, b, h]
    st_send = remote(st_sum, st_in, ST_SUM, to_sp(2))
    st_send.start()
    start_far(2)

    ld_tok.wait()
    ld_lg.wait()
    x = tok_v[...].astype(F32)
    inv = lax.rsqrt(jnp.mean(x * x, axis=-1, keepdims=True) + NORM_EPS)
    hb[...] = (x * inv * lg_v[...]).astype(BF16)

    def matvec(x_ref, w_ref, k_len, n_len, kb, out_dtype=F32):
        def body(k, acc):
            at = pl.ds(pl.multiple_of(k * kb, kb), kb)
            return acc + jnp.dot(x_ref[:, at], w_ref[at, :], preferred_element_type=F32)
        return lax.fori_loop(0, k_len // kb, body, jnp.zeros((rows, n_len), F32))

    acts = []
    for j in range(3):
        ld_qkv[j].wait()
        acts.append(silu(matvec(hb, qkv_v.at[j], width, local_w, 256)).astype(BF16).astype(F32))
    ld_gate.wait()
    gate = 1.0 / (1.0 + jnp.exp(-matvec(hb, gate_v, width, local_w, 256)))
    rows_v[...] = jnp.zeros_like(rows_v)
    for b in range(rows):
        for h in range(heads):
            cols = slice(h * head_dim, (h + 1) * head_dim)
            rows_v[pl.ds(b * 8 + h, 1), :] = acts[0][b:b + 1, cols]
            rows_v[pl.ds(16 + b * 8 + h, 1), :] = acts[1][b:b + 1, cols]
    cols_t = jnp.transpose(rows_v[...])

    ld_own.wait()
    st_own.wait_recv()
    st_send.wait_recv()
    for h in range(heads):
        w_me, w_ot = decay(h, sp), decay(h, flip(sp, 1))
        lam = jnp.exp(jnp.full((1, head_dim), -slope_s[h], F32))
        cols = slice(h * head_dim, (h + 1) * head_dim)
        for b in range(rows):
            moved = w_me * st_loc[0, b, h] + w_ot * st_rcv[0, b, h] + st_in[b, h]
            q_col = cols_t[:, b * 8 + h:b * 8 + h + 1]
            k_col = cols_t[:, 16 + b * 8 + h:16 + b * 8 + h + 1]
            new = lam * moved + k_col * acts[2][b:b + 1, cols]
            s_out[b, h] = new
            o_v[pl.ds(b, 1), cols] = jnp.sum(q_col * new, axis=0, keepdims=True)
    o = o_v[...]

    def gather_tp(ref, base):
        cs = [remote(ref.at[tp], ref.at[tp], base + i - 1, to_tp(i)) for i in (1, 2, 3)]
        for c in cs:
            c.start()
        return cs

    def settle(cs):
        for c in cs:
            c.wait_recv()
        for c in cs:
            c.wait_send()

    sq_all[tp] = jnp.broadcast_to(jnp.sum(o * o, axis=-1, keepdims=True), (rows, 128))
    meet_tp()
    cs = gather_tp(sq_all, SQ)
    pump(1)
    ld_og.wait()
    settle(cs)
    sq = ((sq_all[0] + sq_all[1]) + sq_all[2]) + sq_all[3]
    inv = lax.rsqrt(sq[:, :1] / (4 * local_w) + NORM_EPS)
    out_g = jnp.concatenate([og_v[h:h + 1, :] for h in range(heads)], axis=1)
    g_v[...] = (o * inv * out_g * gate).astype(BF16)

    def project(x_ref, w_ref, dst):
        nb = 512

        def body(n, _):
            at = pl.ds(pl.multiple_of(n * nb, nb), nb)
            dst[tp, :, at] = jnp.dot(x_ref[...], w_ref[:, at], preferred_element_type=F32)
            return 0
        lax.fori_loop(0, width // nb, body, 0)

    ld_lout.wait()
    project(g_v, lout_v, po_all)
    cs = gather_tp(po_all, PO)
    reps = in_v.shape[0] // width
    d_id = lax.broadcasted_iota(jnp.int32, rep_v.shape, 0)
    l_id = lax.broadcasted_iota(jnp.int32, rep_v.shape, 1)
    rep_v[...] = jnp.where((l_id >= d_id * reps) & (l_id < d_id * reps + reps), 1.0, 0.0).astype(BF16)
    settle(cs)
    lin = ((po_all[0] + po_all[1]) + po_all[2]) + po_all[3]
    y = (RES_ALPHA * hb[...].astype(F32) + RES_BETA * lin).astype(BF16).astype(F32)

    ld_ag.wait()
    inv = lax.rsqrt(jnp.mean(y * y, axis=-1, keepdims=True) + NORM_EPS)
    hb[...] = (y * inv * ag_v[...]).astype(BF16)
    ld_in.wait()
    ld_rope.wait()
    lane = lax.broadcasted_iota(jnp.int32, (16, 128 * reps), 1)
    sub = lax.broadcasted_iota(jnp.int32, (16, 128 * reps), 0)
    pick = lax.rem(lane, reps) == sub

    def in_body(d, acc):
        xb = hb[:, pl.ds(pl.multiple_of(d * 128, 128), 128)]
        xr = jnp.dot(xb, rep_v[...], preferred_element_type=F32)
        lhs = jnp.concatenate([jnp.where(pick, xr[b:b + 1], 0.0) for b in range(rows)], axis=0).astype(BF16)
        w = in_v[pl.ds(pl.multiple_of(d * 128 * reps, 128), 128 * reps), :]
        return acc + jnp.dot(lhs, w, preferred_element_type=F32)

    proj = lax.fori_loop(0, width // 128, in_body, jnp.zeros((16 * rows, head_dim), F32)).astype(BF16).astype(F32)
    lane = lax.broadcasted_iota(jnp.int32, proj.shape, 1)
    quarter = head_dim // 4
    partner = jnp.where(lane < quarter, pltpu.roll(proj, head_dim - quarter, 1), pltpu.roll(proj, quarter, 1))
    proj_v[...] = proj
    acc_v[...] = (proj * rope_v[0:1] + partner * rope_v[1:2]).astype(BF16).astype(F32)
    qf_v[...] = jnp.zeros_like(qf_v)
    qp_v[...] = jnp.zeros_like(qp_v)
    ns_v[...] = jnp.zeros_like(ns_v)
    tail_row = lax.broadcasted_iota(jnp.int32, (CACHE_EXTRA, head_dim), 0)
    for b in range(rows):
        for j in range(kv_dev):
            p = b * kv_dev + j
            for g in range(group):
                q_row = acc_v[pl.ds(b * 16 + g * kv_dev + j, 1), :]
                qf_v[pl.ds(p * 8 + g, 1), :] = q_row
                qp_v[pl.ds(p * 4 + g, 1), :] = q_row
            k_new = acc_v[pl.ds(b * 16 + group * kv_dev + j, 1), :]
            v_new = proj_v[pl.ds(b * 16 + (group + 1) * kv_dev + j, 1), :]
            k_buf[b, j, pl.ds(prompt, CACHE_EXTRA), :] = jnp.where(tail_row == 0, k_new, 0.0).astype(BF16)
            v_buf[b, j, pl.ds(prompt, CACHE_EXTRA), :] = jnp.where(tail_row == 0, v_new, 0.0).astype(BF16)
            vf_v[pl.ds(p * 8, 8), :] = jnp.broadcast_to(v_new, (8, head_dim))
            ns_v[pl.ds(p * 8, 8), :] = jnp.broadcast_to(k_new, (8, head_dim))
    qf = qf_v[...]
    pairs = rows * kv_dev
    my_pairs = pl.ds(sp * pairs, pairs)
    q_snd[sp] = qp_v[...].astype(BF16)
    cs = [remote(q_snd.at[sp], q_snd.at[sp], QX + i - 1, to_sp(i)) for i in (1, 2, 3)]
    for c in cs:
        c.start()
    pump(2)
    scale = head_dim ** -0.5
    ns_v[...] = jnp.broadcast_to(jnp.sum(qf * ns_v[...], axis=-1, keepdims=True) * scale, ns_v.shape)

    n_pairs = 4 * pairs
    slots = kst.shape[0]

    def fetch(cache, i):
        slot = lax.rem(i, slots)
        return pltpu.make_async_copy(cache.at[i // kv_dev, lax.rem(i, kv_dev)], kst.at[slot], ksem.at[slot])

    def stream(cache, first, body):
        def step(i, _):
            fetch(cache, i).wait()
            body(i, kst[lax.rem(i, slots)])

            @pl.when(i + slots < n_pairs)
            def _():
                fetch(cache, i + slots).start()
            return 0
        lax.fori_loop(0, n_pairs, step, 0)

    for i in range(slots):
        fetch(k_cache, jnp.int32(i)).start()
    settle(cs)
    pump(1)
    for d in range(4):
        got = q_snd[d].astype(F32)
        for p in range(pairs):
            q_all[d * pairs + p] = jnp.concatenate([got[p * 4:p * 4 + 4], jnp.zeros((4, head_dim), F32)], axis=0).astype(BF16)

    def score_body(i, keys):
        s = lax.dot_general(q_all[i], keys, (((1,), (1,)), ((), ())), preferred_element_type=F32) * scale
        sc_v[i] = s
        mrow_v[pl.ds(pl.multiple_of(i * 8, 8), 8), :] = jnp.broadcast_to(jnp.max(s, axis=-1, keepdims=True), (8, 128))

    stream(k_cache, 0, score_body)
    for i in range(slots):
        fetch(v_cache, jnp.int32(i)).start()
    my_m = pl.ds(pl.multiple_of(sp * pairs * 8, 8), pairs * 8)
    mrow_v[my_m, :] = jnp.maximum(mrow_v[my_m, :], ns_v[...])
    m_all[sp] = jnp.transpose(mrow_v[...])[:1]
    cs = [remote(m_all.at[sp], m_all.at[sp], MX + i - 1, to_sp(i)) for i in (1, 2, 3)]
    for c in cs:
        c.start()
    pump(1)
    settle(cs)
    m = jnp.maximum(jnp.maximum(m_all[0], m_all[1]), jnp.maximum(m_all[2], m_all[3]))
    mcol_v[...] = jnp.transpose(jnp.broadcast_to(m, (128, 128)))
    pump(1)
    lane = lax.broadcasted_iota(jnp.int32, (1, head_dim), 1)

    def out_body(i, values):
        p = jnp.exp(sc_v[i] - mcol_v[pl.ds(pl.multiple_of(i * 8, 8), 8), :][:, :1])
        total = jnp.sum(p, axis=-1, keepdims=True)
        o = jnp.dot(p.astype(BF16), values, preferred_element_type=F32)
        sums = jnp.zeros((1, head_dim), F32)
        for g in range(group):
            sums = jnp.where(lane == g, total[g:g + 1], sums)
        ol_v[i] = jnp.concatenate([o[:group], sums], axis=0)

    stream(v_cache, 0, out_body)
    cs = [remote(ol_v.at[pl.ds(flip(sp, i) * pairs, pairs)], olr_v.at[sp], OX + i - 1, to_sp(i)) for i in (1, 2, 3)]
    for c in cs:
        c.start()
    olr_v[sp] = ol_v[my_pairs]
    pump(1)
    settle(cs)
    new_p = jnp.exp(ns_v[...] - mcol_v[my_m, :])
    new_o = new_p.astype(BF16).astype(F32) * vf_v[...]
    for b in range(rows):
        for j in range(kv_dev):
            p = b * kv_dev + j
            total = ((olr_v[0, p] + olr_v[1, p]) + olr_v[2, p]) + olr_v[3, p]
            for g in range(group):
                h, at = j * group + g, p * 8 + g
                denom = total[group:group + 1, g:g + 1] + new_p[at:at + 1]
                ho_v[pl.ds(b, 1), h * head_dim:(h + 1) * head_dim] = (total[g:g + 1] + new_o[at:at + 1]) / denom
    g_v[...] = ho_v[...].astype(BF16)
    ld_aout.wait()
    project(g_v, aout_v, pa_all)
    cs = gather_tp(pa_all, PA)
    start_far(len(far))

    @pl.when(core == 0)
    def _():
        for c in far[n_both:]:
            c.start()

    settle(cs)
    att = ((pa_all[0] + pa_all[1]) + pa_all[2]) + pa_all[3]
    hid[...] = (RES_ALPHA * hb[...].astype(F32) + RES_BETA * att).astype(BF16)

    st_own.wait_send()
    st_fwd.wait_send()
    st_send.wait_send()
    for c in own_kv:
        c.wait()
    for c in near:
        c.wait()
    for c in far[far_state[1]:n_both]:
        c.wait_send()
    for c in far[:n_both]:
        c.wait_recv()

    @pl.when(core == 0)
    def _():
        for c in far[n_both:]:
            c.wait()


def tail_kernel(v_cache, token, x_buf, send, recv):
    sp = lax.axis_index("sp")
    rows = v_cache.shape[0] // 4
    kv_dev = v_cache.shape[1]
    peer = flip(sp, 2)
    barrier = pltpu.get_barrier_semaphore()
    pl.semaphore_signal(barrier, inc=1, device_id={"sp": peer}, device_id_type=MESH)
    pl.semaphore_wait(barrier, 1)

    @pl.when(lax.rem(sp, 2) == 1)
    def _():
        cs = []
        for i in range(LATE):
            cs.append(pltpu.make_async_remote_copy(
                v_cache.at[peer * rows + rows - 1, kv_dev - LATE + i], x_buf.at[i], send.at[i], recv.at[i], device_id={"sp": peer}, device_id_type=MESH))
            cs[-1].start()
        for c in cs:
            c.wait()


def tail_write_kernel(v_in, x_buf, v_out, sem):
    sp = lax.axis_index("sp")
    rows, kv_dev = v_out.shape[:2]
    shard_len = x_buf.shape[1]

    @pl.when(lax.rem(sp, 2) == 1)
    def _():
        cs = []
        for i in range(LATE):
            at = pl.ds(pl.multiple_of(flip(sp, 2) * shard_len, shard_len), shard_len)
            cs.append(pltpu.make_async_copy(x_buf.at[i], v_out.at[rows - 1, kv_dev - LATE + i, at], sem.at[i]))
            cs[-1].start()
        for c in cs:
            c.wait()


def write_kernel(k_buf, v_buf, s_buf, hid_buf, hid, s_out, k_out, v_out, token, sem):
    token[...] = jnp.zeros_like(token)
    cs = []
    for src, dst in ((k_buf, k_out), (v_buf, v_out)):
        for b in range(src.shape[0]):
            for j in range(src.shape[1]):
                cs.append(pltpu.make_async_copy(src.at[b, j], dst.at[b, j], sem.at[len(cs)]))
    cs.append(pltpu.make_async_copy(s_buf, s_out, sem.at[len(cs)]))
    cs.append(pltpu.make_async_copy(hid_buf, hid, sem.at[len(cs)]))
    for c in cs:
        c.start()
    for c in cs:
        c.wait()


def solution(mesh):
    def device_step(tokens, states, k_cache, v_cache, slopes, lin_gain, w_lin_qkv, w_lin_gate, out_gain, w_lin_out, attn_gain, w_attn_in, w_attn_out):
        rows, width = tokens.shape
        seqs, kv_dev, shard_len, head_dim = k_cache.shape
        heads = slopes.shape[0]
        local_w = heads * head_dim
        prompt = 4 * shard_len
        reps = w_attn_in.shape[1] * w_attn_in.shape[2]
        pairs = rows * kv_dev
        group = heads // kv_dev
        cache_shape = (rows, kv_dev, prompt + CACHE_EXTRA, head_dim)
        state_shape = (rows, heads, head_dim, head_dim)
        vm, any_ = pltpu.VMEM, pl.ANY
        w_qkv = jnp.transpose(w_lin_qkv, (1, 0, 2))
        w_in = jnp.transpose(w_attn_in, (0, 2, 1, 3)).reshape(width * reps, head_dim)
        rope = jnp.asarray(rope_table(head_dim, prompt))
        dma = pltpu.SemaphoreType.DMA
        k_buf, v_buf, s_buf, hid_buf = pl.pallas_call(
            step_kernel,
            name="step",
            out_shape=(vm(cache_shape, BF16), vm(cache_shape, BF16), vm(state_shape, F32), vm((rows, width), BF16)),
            in_specs=[pl.BlockSpec(memory_space=any_)] * 14,
            out_specs=[pl.BlockSpec(memory_space=vm)] * 4,
            scratch_shapes=[
                vm((rows, width), BF16), vm((1, width), F32), vm((heads, head_dim), F32), vm((1, width), F32), vm((8, head_dim), F32),
                pltpu.SMEM((heads,), F32), vm((3, width, local_w), BF16), vm((width, local_w), BF16), vm((local_w, width), BF16),
                vm((width * reps, head_dim), BF16), vm((local_w, width), BF16),
                vm((2,) + state_shape, F32), vm((2,) + state_shape, F32), vm(state_shape, F32), vm(state_shape, F32),
                vm((rows, width), BF16), vm((128, head_dim), F32), vm((rows, local_w), F32), vm((rows, local_w), BF16),
                vm((128, 128 * reps), BF16), vm((16 * rows, head_dim), F32), vm((16 * rows, head_dim), F32),
                vm((8 * pairs, head_dim), F32), vm((8 * pairs, head_dim), F32), vm((4 * pairs, head_dim), F32), vm((4, 4 * pairs, head_dim), BF16), vm((4 * pairs, 8, head_dim), BF16),
                vm((4 * pairs, 8, shard_len), F32), vm((128, 128), F32), vm((4, 1, 128), F32), vm((128, 128), F32),
                vm((8 * pairs, head_dim), F32), vm((4 * pairs, group + 1, head_dim), F32), vm((4, pairs, group + 1, head_dim), F32),
                vm((rows, local_w), F32), vm((4, rows, 128), F32), vm((4, rows, width), F32), vm((4, rows, width), F32),
                vm((4, shard_len, head_dim), BF16),
                dma((NUM_SEMS,)), dma((NUM_SEMS,)), dma((17,)), dma((4,)), pltpu.SemaphoreType.REGULAR((2,)),
            ],
            compiler_params=pltpu.CompilerParams(collective_id=0, has_side_effects=True, vmem_limit_bytes=46 * MIB),
        )(tokens, states, k_cache, v_cache, slopes, lin_gain.reshape(1, -1), w_qkv, w_lin_gate, out_gain.reshape(heads, head_dim), w_lin_out, attn_gain.reshape(1, -1), w_in, w_attn_out, rope)
        bufs = [pltpu.with_memory_space_constraint(a, vm) for a in (k_buf, v_buf, s_buf, hid_buf)]
        hid, s_out, k_out, v_out, token = pl.pallas_call(
            write_kernel,
            name="write",
            out_shape=(jax.ShapeDtypeStruct((rows, width), BF16), jax.ShapeDtypeStruct(state_shape, F32),
                       jax.ShapeDtypeStruct(cache_shape, BF16), jax.ShapeDtypeStruct(cache_shape, BF16), vm((8, 128), F32)),
            in_specs=[pl.BlockSpec(memory_space=vm)] * 4,
            out_specs=[pl.BlockSpec(memory_space=any_)] * 4 + [pl.BlockSpec(memory_space=vm)],
            scratch_shapes=[dma((10,))],
            compiler_params=pltpu.CompilerParams(vmem_limit_bytes=20 * MIB),
        )(*bufs)
        x_buf = pl.pallas_call(
            tail_kernel,
            name="tail",
            out_shape=vm((LATE, shard_len, head_dim), BF16),
            in_specs=[pl.BlockSpec(memory_space=any_), pl.BlockSpec(memory_space=vm)],
            out_specs=pl.BlockSpec(memory_space=vm),
            scratch_shapes=[dma((LATE,)), dma((LATE,))],
            compiler_params=pltpu.CompilerParams(collective_id=1, has_side_effects=True, vmem_limit_bytes=4 * MIB),
        )(pltpu.with_memory_space_constraint(v_cache, pltpu.HBM), pltpu.with_memory_space_constraint(token, vm))
        v_out = pl.pallas_call(
            tail_write_kernel,
            name="tail_write",
            out_shape=jax.ShapeDtypeStruct(cache_shape, BF16),
            in_specs=[pl.BlockSpec(memory_space=any_), pl.BlockSpec(memory_space=vm)],
            out_specs=pl.BlockSpec(memory_space=any_),
            scratch_shapes=[dma((LATE,))],
            input_output_aliases={0: 0},
            compiler_params=pltpu.CompilerParams(vmem_limit_bytes=4 * MIB),
        )(v_out, pltpu.with_memory_space_constraint(x_buf, vm))
        return hid, s_out, k_out, v_out

    batch_spec = P(('dp', 'sp'), None)
    head_spec = P(('dp', 'sp'), 'tp', None, None)
    cache_spec = P('dp', 'tp', 'sp', None)
    in_specs = (batch_spec, P('sp', 'dp', 'tp', None, None), cache_spec, cache_spec, P('tp'), P(None), P(None, None, 'tp'), P(None, 'tp'), P('tp'), P('tp', None), P(None), P(None, 'tp', None, None), P('tp', None))
    out_specs = (batch_spec, head_spec, head_spec, head_spec)
    return jax.shard_map(device_step, mesh=mesh, in_specs=in_specs, out_specs=out_specs, check_vma=False)
```

```python
import math

import jax
import jax.numpy as jnp
import numpy as np
from jax import lax
from jax.experimental import pallas as pl
from jax.experimental.pallas import tpu as pltpu
from jax.sharding import PartitionSpec as P

NORM_EPS = 1e-6
ROPE_BASE = 10000000.0
RES_ALPHA = 1.0
RES_BETA = 1.0
CACHE_EXTRA = 16

MESH = pl.DeviceIdType.MESH
F32 = jnp.float32
BF16 = jnp.bfloat16
MIB = 2**20

ST_OWN, ST_FWD, ST_SUM = 0, 1, 2
SQ, PO, PA = 3, 6, 9
QX, MX, OX = 12, 15, 18
KV_NEAR = 21
KV_FAR = 23
NUM_SEMS = KV_FAR + 16
LATE = 2


def rope_table(head_dim, position):
    rope_dim = head_dim // 2
    half = rope_dim // 2
    inv_freq = ROPE_BASE ** (-np.arange(0, rope_dim, 2, dtype=np.float64) / rope_dim)
    cos, sin = np.cos(position * inv_freq), np.sin(position * inv_freq)
    table = np.zeros((8, head_dim), np.float32)
    table[0] = np.concatenate([cos, cos, np.ones(head_dim - rope_dim)])
    table[1, :rope_dim] = np.concatenate([-sin, sin])
    return table


def flip(index, mask):
    chip, core = index // 2, index % 2
    if mask & 2:
        chip = 1 - chip
    if mask & 1:
        core = 1 - core
    return chip * 2 + core


def silu(x):
    return x * (1.0 / (1.0 + jnp.exp(-x)))


def step_kernel(
    tokens, states, k_cache, v_cache, slopes, lin_gain, w_qkv, w_gate, out_gain, w_lin_out, attn_gain, w_in, w_attn_out, rope,
    k_buf, v_buf, s_out, hid,
    tok_v, lg_v, og_v, ag_v, rope_v, slope_s, qkv_v, gate_v, lout_v, in_v, aout_v,
    st_loc, st_rcv, st_sum, st_in, hb, rows_v, o_v, g_v, rep_v, acc_v, proj_v, qf_v, vf_v, qp_v, q_snd, q_all, sc_v, mrow_v, m_all, mcol_v,
    ns_v, ol_v, ol_sum, olr_v, ho_v, sq_all, po_all, pa_all, kst,
    send, recv, lsem, ksem, met,
):
    sp = lax.axis_index("sp")
    tp = lax.axis_index("tp")
    shard_len = k_cache.shape[2]
    kv_dev = k_cache.shape[1]
    head_dim = k_cache.shape[3]
    heads = slopes.shape[0]
    rows = tokens.shape[0]
    width = tokens.shape[1]
    group = heads // kv_dev
    prompt = 4 * shard_len
    local_w = heads * head_dim

    def to_sp(mask):
        return {"sp": flip(sp, mask)}

    def to_tp(off):
        return {"tp": lax.rem(tp + off, 4)}

    core = lax.rem(sp, 2)
    barrier = pltpu.get_barrier_semaphore()
    pl.semaphore_signal(barrier, inc=1, device_id=to_sp(2), device_id_type=MESH)

    @pl.when(core == 0)
    def _():
        for i in (1, 2, 3):
            pl.semaphore_signal(barrier, inc=1, device_id=to_tp(i), device_id_type=MESH)

    def remote(src, dst, i, dev):
        return pltpu.make_async_remote_copy(src, dst, send.at[i], recv.at[i], device_id=dev, device_id_type=MESH)

    def local(src, dst, i):
        return pltpu.make_async_copy(src, dst, lsem.at[i])

    my_rows = pl.ds(pl.multiple_of(sp * shard_len, shard_len), shard_len)
    pieces = [(t, b, j, mask) for t in range(2) for b in range(rows) for j in range(kv_dev) for mask in (2, 3)]
    late = [(1, rows - 1, j, 2) for j in range(kv_dev)[-LATE:]]
    pieces = sorted([p for p in pieces if p not in late], key=lambda p: p[0] > 0 or p[1] > 0) + late
    pieces[1], pieces[2] = pieces[2], pieces[1]
    far = []
    for t, b, j, mask in pieces:
        src, dst = ((k_cache, k_buf), (v_cache, v_buf))[t]
        far.append(remote(src.at[flip(sp, mask) * rows + b, j], dst.at[b, j, my_rows], KV_FAR + len(far), to_sp(mask)))
    n_both = len(far) - len(late)
    far_state = [0, 0]

    def start_far(n):
        for _ in range(n):
            if far_state[0] < n_both:
                far[far_state[0]].start()
                far_state[0] += 1

    def pump(n):
        for _ in range(n):
            far[far_state[1]].wait_send()
            far_state[1] += 1
            start_far(1)

    @pl.when(core == 1)
    def _():
        pl.semaphore_wait(barrier, 1)
        far[0].start()
        far[1].start()
        pl.semaphore_signal(barrier, inc=1, device_id=to_sp(1), device_id_type=MESH)
        pl.semaphore_wait(met.at[0], 1)

    @pl.when(core == 0)
    def _():
        pl.semaphore_wait(barrier, 5)
        pl.semaphore_signal(met.at[0], inc=1, device_id=to_sp(1), device_id_type=MESH)
        far[0].start()
        for i in (1, 2, 3):
            pl.semaphore_signal(met.at[2], inc=1, device_id=to_tp(i), device_id_type=MESH)

    def meet_tp():
        @pl.when(core == 0)
        def _():
            pl.semaphore_wait(met.at[2], 3)
            pl.semaphore_signal(met.at[1], inc=1, device_id=to_sp(1), device_id_type=MESH)

        @pl.when(core == 1)
        def _():
            pl.semaphore_wait(met.at[1], 1)

    def st_rows(g):
        return pl.ds(g * rows, rows)

    st_own = remote(states.at[0, st_rows(flip(sp, 1))], st_rcv.at[0], ST_OWN, to_sp(1))
    st_fwd = remote(states.at[0, st_rows(flip(sp, 3))], st_rcv.at[1], ST_FWD, to_sp(1))
    st_fwd.start()
    ld_fwd = local(states.at[0, st_rows(flip(sp, 2))], st_loc.at[1], 0)
    ld_slope = local(slopes, slope_s, 1)
    ld_fwd.start()
    ld_slope.start()
    st_own.start()
    ld_own = local(states.at[0, st_rows(sp)], st_loc.at[0], 2)
    ld_tok = local(tokens, tok_v, 3)
    ld_lg = local(lin_gain, lg_v, 4)
    ld_og = local(out_gain, og_v, 5)
    ld_ag = local(attn_gain, ag_v, 6)
    ld_rope = local(rope, rope_v, 7)
    ld_qkv = [local(w_qkv.at[j], qkv_v.at[j], 8 + j) for j in range(3)]
    ld_gate = local(w_gate, gate_v, 11)
    ld_lout = local(w_lin_out, lout_v, 12)
    ld_in = local(w_in, in_v, 13)
    ld_aout = local(w_attn_out, aout_v, 14)
    own_kv = [local(src.at[st_rows(sp)], dst.at[:, :, my_rows], 15 + t) for t, (src, dst) in enumerate(((k_cache, k_buf), (v_cache, v_buf)))]
    near = [remote(src.at[st_rows(flip(sp, 1))], dst.at[:, :, my_rows], KV_NEAR + t, to_sp(1)) for t, (src, dst) in enumerate(((k_cache, k_buf), (v_cache, v_buf)))]
    for c in [ld_own, ld_tok, ld_lg, ld_og, ld_ag, ld_rope] + ld_qkv + [ld_gate, ld_lout, ld_in, ld_aout] + near + own_kv:
        c.start()

    def decay(h, shard):
        off = (shard_len * (3 - shard)).astype(F32)
        return jnp.exp(jnp.full((1, head_dim), -slope_s[h] * off, F32))

    ld_slope.wait()
    ld_fwd.wait()
    st_fwd.wait_recv()
    for h in range(heads):
        w_me, w_ot = decay(h, sp), decay(h, flip(sp, 1))
        for b in range(rows):
            st_sum[b, h] = w_me * st_loc[1, b, h] + w_ot * st_rcv[1, b, h]
    st_send = remote(st_sum, st_in, ST_SUM, to_sp(2))
    st_send.start()

    @pl.when(core == 0)
    def _():
        far[1].start()

    far_state[0] = 2
    start_far(1)

    ld_tok.wait()
    ld_lg.wait()
    x = tok_v[...].astype(F32)
    inv = lax.rsqrt(jnp.mean(x * x, axis=-1, keepdims=True) + NORM_EPS)
    hb[...] = (x * inv * lg_v[...]).astype(BF16)

    def matvec(x_ref, w_ref, k_len, n_len, kb, out_dtype=F32):
        def body(k, acc):
            at = pl.ds(pl.multiple_of(k * kb, kb), kb)
            return acc + jnp.dot(x_ref[:, at], w_ref[at, :], preferred_element_type=F32)
        return lax.fori_loop(0, k_len // kb, body, jnp.zeros((rows, n_len), F32))

    acts = []
    for j in range(3):
        ld_qkv[j].wait()
        acts.append(silu(matvec(hb, qkv_v.at[j], width, local_w, 256)).astype(BF16).astype(F32))
    ld_gate.wait()
    gate = 1.0 / (1.0 + jnp.exp(-matvec(hb, gate_v, width, local_w, 256)))
    rows_v[...] = jnp.zeros_like(rows_v)
    for b in range(rows):
        for h in range(heads):
            cols = slice(h * head_dim, (h + 1) * head_dim)
            rows_v[pl.ds(b * 8 + h, 1), :] = acts[0][b:b + 1, cols]
            rows_v[pl.ds(16 + b * 8 + h, 1), :] = acts[1][b:b + 1, cols]
    cols_t = jnp.transpose(rows_v[...])

    ld_own.wait()
    st_own.wait_recv()
    st_send.wait_recv()
    for h in range(heads):
        w_me, w_ot = decay(h, sp), decay(h, flip(sp, 1))
        lam = jnp.exp(jnp.full((1, head_dim), -slope_s[h], F32))
        cols = slice(h * head_dim, (h + 1) * head_dim)
        for b in range(rows):
            moved = w_me * st_loc[0, b, h] + w_ot * st_rcv[0, b, h] + st_in[b, h]
            q_col = cols_t[:, b * 8 + h:b * 8 + h + 1]
            k_col = cols_t[:, 16 + b * 8 + h:16 + b * 8 + h + 1]
            new = lam * moved + k_col * acts[2][b:b + 1, cols]
            s_out[b, h] = new
            o_v[pl.ds(b, 1), cols] = jnp.sum(q_col * new, axis=0, keepdims=True)
    o = o_v[...]

    def gather_tp(ref, base):
        cs = [remote(ref.at[tp], ref.at[tp], base + i - 1, to_tp(i)) for i in (1, 2, 3)]
        for c in cs:
            c.start()
        return cs

    def settle(cs):
        for c in cs:
            c.wait_recv()
        for c in cs:
            c.wait_send()

    sq_all[tp] = jnp.broadcast_to(jnp.sum(o * o, axis=-1, keepdims=True), (rows, 128))
    meet_tp()
    cs = gather_tp(sq_all, SQ)
    pump(1)
    ld_og.wait()
    settle(cs)
    sq = ((sq_all[0] + sq_all[1]) + sq_all[2]) + sq_all[3]
    inv = lax.rsqrt(sq[:, :1] / (4 * local_w) + NORM_EPS)
    out_g = jnp.concatenate([og_v[h:h + 1, :] for h in range(heads)], axis=1)
    g_v[...] = (o * inv * out_g * gate).astype(BF16)

    def project(x_ref, w_ref, dst):
        nb = 512

        def body(n, _):
            at = pl.ds(pl.multiple_of(n * nb, nb), nb)
            dst[tp, :, at] = jnp.dot(x_ref[...], w_ref[:, at], preferred_element_type=F32)
            return 0
        lax.fori_loop(0, width // nb, body, 0)

    ld_lout.wait()
    project(g_v, lout_v, po_all)
    cs = gather_tp(po_all, PO)
    reps = in_v.shape[0] // width
    d_id = lax.broadcasted_iota(jnp.int32, rep_v.shape, 0)
    l_id = lax.broadcasted_iota(jnp.int32, rep_v.shape, 1)
    rep_v[...] = jnp.where((l_id >= d_id * reps) & (l_id < d_id * reps + reps), 1.0, 0.0).astype(BF16)
    settle(cs)
    lin = ((po_all[0] + po_all[1]) + po_all[2]) + po_all[3]
    y = (RES_ALPHA * hb[...].astype(F32) + RES_BETA * lin).astype(BF16).astype(F32)

    ld_ag.wait()
    inv = lax.rsqrt(jnp.mean(y * y, axis=-1, keepdims=True) + NORM_EPS)
    hb[...] = (y * inv * ag_v[...]).astype(BF16)
    ld_in.wait()
    ld_rope.wait()
    lane = lax.broadcasted_iota(jnp.int32, (16, 128 * reps), 1)
    sub = lax.broadcasted_iota(jnp.int32, (16, 128 * reps), 0)
    pick = lax.rem(lane, reps) == sub

    def in_body(d, acc):
        xb = hb[:, pl.ds(pl.multiple_of(d * 128, 128), 128)]
        xr = jnp.dot(xb, rep_v[...], preferred_element_type=F32)
        lhs = jnp.concatenate([jnp.where(pick, xr[b:b + 1], 0.0) for b in range(rows)], axis=0).astype(BF16)
        w = in_v[pl.ds(pl.multiple_of(d * 128 * reps, 128), 128 * reps), :]
        return acc + jnp.dot(lhs, w, preferred_element_type=F32)

    proj = lax.fori_loop(0, width // 128, in_body, jnp.zeros((16 * rows, head_dim), F32)).astype(BF16).astype(F32)
    lane = lax.broadcasted_iota(jnp.int32, proj.shape, 1)
    quarter = head_dim // 4
    partner = jnp.where(lane < quarter, pltpu.roll(proj, head_dim - quarter, 1), pltpu.roll(proj, quarter, 1))
    proj_v[...] = proj
    acc_v[...] = (proj * rope_v[0:1] + partner * rope_v[1:2]).astype(BF16).astype(F32)
    qf_v[...] = jnp.zeros_like(qf_v)
    qp_v[...] = jnp.zeros_like(qp_v)
    ns_v[...] = jnp.zeros_like(ns_v)
    tail_row = lax.broadcasted_iota(jnp.int32, (CACHE_EXTRA, head_dim), 0)
    for b in range(rows):
        for j in range(kv_dev):
            p = b * kv_dev + j
            for g in range(group):
                q_row = acc_v[pl.ds(b * 16 + g * kv_dev + j, 1), :]
                qf_v[pl.ds(p * 8 + g, 1), :] = q_row
                qp_v[pl.ds(p * 4 + g, 1), :] = q_row
            k_new = acc_v[pl.ds(b * 16 + group * kv_dev + j, 1), :]
            v_new = proj_v[pl.ds(b * 16 + (group + 1) * kv_dev + j, 1), :]
            k_buf[b, j, pl.ds(prompt, CACHE_EXTRA), :] = jnp.where(tail_row == 0, k_new, 0.0).astype(BF16)
            v_buf[b, j, pl.ds(prompt, CACHE_EXTRA), :] = jnp.where(tail_row == 0, v_new, 0.0).astype(BF16)
            vf_v[pl.ds(p * 8, 8), :] = jnp.broadcast_to(v_new, (8, head_dim))
            ns_v[pl.ds(p * 8, 8), :] = jnp.broadcast_to(k_new, (8, head_dim))
    qf = qf_v[...]
    pairs = rows * kv_dev
    my_pairs = pl.ds(sp * pairs, pairs)
    q_snd[sp] = qp_v[...].astype(BF16)
    cs = [remote(q_snd.at[sp], q_snd.at[sp], QX + i - 1, to_sp(i)) for i in (1, 2)]
    for c in cs:
        c.start()
    pump(2)
    scale = head_dim ** -0.5
    ns_v[...] = jnp.broadcast_to(jnp.sum(qf * ns_v[...], axis=-1, keepdims=True) * scale, ns_v.shape)

    n_pairs = 4 * pairs
    slots = kst.shape[0]

    def fetch(cache, i):
        slot = lax.rem(i, slots)
        return pltpu.make_async_copy(cache.at[i // kv_dev, lax.rem(i, kv_dev)], kst.at[slot], ksem.at[slot])

    def stream(cache, first, body):
        def step(i, _):
            fetch(cache, i).wait()
            body(i, kst[lax.rem(i, slots)])

            @pl.when(i + slots < n_pairs)
            def _():
                fetch(cache, i + slots).start()
            return 0
        lax.fori_loop(0, n_pairs, step, 0)

    for i in range(slots):
        fetch(k_cache, jnp.int32(i)).start()
    cs[1].wait_recv()
    hand_on = remote(q_snd.at[flip(sp, 2)], q_snd.at[flip(sp, 2)], QX + 2, to_sp(1))
    hand_on.start()
    cs[0].wait_recv()
    hand_on.wait_recv()
    for c in cs + [hand_on]:
        c.wait_send()
    pump(1)
    for d in range(4):
        got = q_snd[d].astype(F32)
        for p in range(pairs):
            q_all[d * pairs + p] = jnp.concatenate([got[p * 4:p * 4 + 4], jnp.zeros((4, head_dim), F32)], axis=0).astype(BF16)

    def score_body(i, keys):
        s = lax.dot_general(q_all[i], keys, (((1,), (1,)), ((), ())), preferred_element_type=F32) * scale
        sc_v[i] = s
        mrow_v[pl.ds(pl.multiple_of(i * 8, 8), 8), :] = jnp.broadcast_to(jnp.max(s, axis=-1, keepdims=True), (8, 128))

    stream(k_cache, 0, score_body)
    for i in range(slots):
        fetch(v_cache, jnp.int32(i)).start()
    my_m = pl.ds(pl.multiple_of(sp * pairs * 8, 8), pairs * 8)
    mrow_v[my_m, :] = jnp.maximum(mrow_v[my_m, :], ns_v[...])
    m_all[sp] = jnp.transpose(mrow_v[...])[:1]
    cs = [remote(m_all.at[sp], m_all.at[sp], MX + i - 1, to_sp(i)) for i in (1, 2, 3)]
    for c in cs:
        c.start()
    pump(1)
    settle(cs)
    m = jnp.maximum(jnp.maximum(m_all[0], m_all[1]), jnp.maximum(m_all[2], m_all[3]))
    mcol_v[...] = jnp.transpose(jnp.broadcast_to(m, (128, 128)))
    pump(1)
    lane = lax.broadcasted_iota(jnp.int32, (1, head_dim), 1)

    def out_body(i, values):
        p = jnp.exp(sc_v[i] - mcol_v[pl.ds(pl.multiple_of(i * 8, 8), 8), :][:, :1])
        total = jnp.sum(p, axis=-1, keepdims=True)
        o = jnp.dot(p.astype(BF16), values, preferred_element_type=F32)
        sums = jnp.zeros((1, head_dim), F32)
        for g in range(group):
            sums = jnp.where(lane == g, total[g:g + 1], sums)
        ol_v[i] = jnp.concatenate([o[:group], sums], axis=0)

    stream(v_cache, 0, out_body)
    o_fwd = remote(ol_v.at[pl.ds(flip(sp, 3) * pairs, pairs)], olr_v.at[1], OX, to_sp(1))
    o_own = remote(ol_v.at[pl.ds(flip(sp, 1) * pairs, pairs)], olr_v.at[0], OX + 1, to_sp(1))
    o_fwd.start()
    o_own.start()
    o_fwd.wait_recv()
    ol_sum[...] = ol_v[pl.ds(flip(sp, 2) * pairs, pairs)] + olr_v[1]
    o_sum = remote(ol_sum, olr_v.at[2], OX + 2, to_sp(2))
    o_sum.start()
    pump(1)
    o_own.wait_recv()
    o_sum.wait_recv()
    for c in (o_fwd, o_own, o_sum):
        c.wait_send()
    mine = ol_v[my_pairs]
    new_p = jnp.exp(ns_v[...] - mcol_v[my_m, :])
    new_o = new_p.astype(BF16).astype(F32) * vf_v[...]
    for b in range(rows):
        for j in range(kv_dev):
            p = b * kv_dev + j
            total = (mine[p] + olr_v[0, p]) + olr_v[2, p]
            for g in range(group):
                h, at = j * group + g, p * 8 + g
                denom = total[group:group + 1, g:g + 1] + new_p[at:at + 1]
                ho_v[pl.ds(b, 1), h * head_dim:(h + 1) * head_dim] = (total[g:g + 1] + new_o[at:at + 1]) / denom
    g_v[...] = ho_v[...].astype(BF16)
    ld_aout.wait()
    project(g_v, aout_v, pa_all)
    cs = gather_tp(pa_all, PA)
    start_far(len(far))

    @pl.when(core == 0)
    def _():
        for c in far[n_both:]:
            c.start()

    settle(cs)
    att = ((pa_all[0] + pa_all[1]) + pa_all[2]) + pa_all[3]
    hid[...] = (RES_ALPHA * hb[...].astype(F32) + RES_BETA * att).astype(BF16)

    st_own.wait_send()
    st_fwd.wait_send()
    st_send.wait_send()
    for c in own_kv:
        c.wait()
    for c in near:
        c.wait()
    for c in far[far_state[1]:n_both]:
        c.wait_send()
    for c in far[:n_both]:
        c.wait_recv()

    @pl.when(core == 0)
    def _():
        for c in far[n_both:]:
            c.wait()


def tail_kernel(v_cache, token, x_buf, send, recv):
    sp = lax.axis_index("sp")
    rows = v_cache.shape[0] // 4
    kv_dev = v_cache.shape[1]
    peer = flip(sp, 2)
    barrier = pltpu.get_barrier_semaphore()
    pl.semaphore_signal(barrier, inc=1, device_id={"sp": peer}, device_id_type=MESH)
    pl.semaphore_wait(barrier, 1)

    @pl.when(lax.rem(sp, 2) == 1)
    def _():
        cs = []
        for i in range(LATE):
            cs.append(pltpu.make_async_remote_copy(
                v_cache.at[peer * rows + rows - 1, kv_dev - LATE + i], x_buf.at[i], send.at[i], recv.at[i], device_id={"sp": peer}, device_id_type=MESH))
            cs[-1].start()
        for c in cs:
            c.wait()


def tail_write_kernel(v_in, x_buf, v_out, sem):
    sp = lax.axis_index("sp")
    rows, kv_dev = v_out.shape[:2]
    shard_len = x_buf.shape[1]

    @pl.when(lax.rem(sp, 2) == 1)
    def _():
        cs = []
        for i in range(LATE):
            at = pl.ds(pl.multiple_of(flip(sp, 2) * shard_len, shard_len), shard_len)
            cs.append(pltpu.make_async_copy(x_buf.at[i], v_out.at[rows - 1, kv_dev - LATE + i, at], sem.at[i]))
            cs[-1].start()
        for c in cs:
            c.wait()


def write_kernel(k_buf, v_buf, s_buf, hid_buf, hid, s_out, k_out, v_out, token, sem):
    token[...] = jnp.zeros_like(token)
    cs = []
    for src, dst in ((k_buf, k_out), (v_buf, v_out)):
        for b in range(src.shape[0]):
            for j in range(src.shape[1]):
                cs.append(pltpu.make_async_copy(src.at[b, j], dst.at[b, j], sem.at[len(cs)]))
    cs.append(pltpu.make_async_copy(s_buf, s_out, sem.at[len(cs)]))
    cs.append(pltpu.make_async_copy(hid_buf, hid, sem.at[len(cs)]))
    for c in cs:
        c.start()
    for c in cs:
        c.wait()


def solution(mesh):
    def device_step(tokens, states, k_cache, v_cache, slopes, lin_gain, w_lin_qkv, w_lin_gate, out_gain, w_lin_out, attn_gain, w_attn_in, w_attn_out):
        rows, width = tokens.shape
        seqs, kv_dev, shard_len, head_dim = k_cache.shape
        heads = slopes.shape[0]
        local_w = heads * head_dim
        prompt = 4 * shard_len
        reps = w_attn_in.shape[1] * w_attn_in.shape[2]
        pairs = rows * kv_dev
        group = heads // kv_dev
        cache_shape = (rows, kv_dev, prompt + CACHE_EXTRA, head_dim)
        state_shape = (rows, heads, head_dim, head_dim)
        vm, any_ = pltpu.VMEM, pl.ANY
        w_qkv = jnp.transpose(w_lin_qkv, (1, 0, 2))
        w_in = jnp.transpose(w_attn_in, (0, 2, 1, 3)).reshape(width * reps, head_dim)
        rope = jnp.asarray(rope_table(head_dim, prompt))
        dma = pltpu.SemaphoreType.DMA
        k_buf, v_buf, s_buf, hid_buf = pl.pallas_call(
            step_kernel,
            name="step",
            out_shape=(vm(cache_shape, BF16), vm(cache_shape, BF16), vm(state_shape, F32), vm((rows, width), BF16)),
            in_specs=[pl.BlockSpec(memory_space=any_)] * 14,
            out_specs=[pl.BlockSpec(memory_space=vm)] * 4,
            scratch_shapes=[
                vm((rows, width), BF16), vm((1, width), F32), vm((heads, head_dim), F32), vm((1, width), F32), vm((8, head_dim), F32),
                pltpu.SMEM((heads,), F32), vm((3, width, local_w), BF16), vm((width, local_w), BF16), vm((local_w, width), BF16),
                vm((width * reps, head_dim), BF16), vm((local_w, width), BF16),
                vm((2,) + state_shape, F32), vm((2,) + state_shape, F32), vm(state_shape, F32), vm(state_shape, F32),
                vm((rows, width), BF16), vm((128, head_dim), F32), vm((rows, local_w), F32), vm((rows, local_w), BF16),
                vm((128, 128 * reps), BF16), vm((16 * rows, head_dim), F32), vm((16 * rows, head_dim), F32),
                vm((8 * pairs, head_dim), F32), vm((8 * pairs, head_dim), F32), vm((4 * pairs, head_dim), F32), vm((4, 4 * pairs, head_dim), BF16), vm((4 * pairs, 8, head_dim), BF16),
                vm((4 * pairs, 8, shard_len), F32), vm((128, 128), F32), vm((4, 1, 128), F32), vm((128, 128), F32),
                vm((8 * pairs, head_dim), F32), vm((4 * pairs, group + 1, head_dim), F32), vm((pairs, group + 1, head_dim), F32), vm((3, pairs, group + 1, head_dim), F32),
                vm((rows, local_w), F32), vm((4, rows, 128), F32), vm((4, rows, width), F32), vm((4, rows, width), F32),
                vm((4, shard_len, head_dim), BF16),
                dma((NUM_SEMS,)), dma((NUM_SEMS,)), dma((17,)), dma((4,)), pltpu.SemaphoreType.REGULAR((3,)),
            ],
            compiler_params=pltpu.CompilerParams(collective_id=0, has_side_effects=True, vmem_limit_bytes=46 * MIB),
        )(tokens, states, k_cache, v_cache, slopes, lin_gain.reshape(1, -1), w_qkv, w_lin_gate, out_gain.reshape(heads, head_dim), w_lin_out, attn_gain.reshape(1, -1), w_in, w_attn_out, rope)
        bufs = [pltpu.with_memory_space_constraint(a, vm) for a in (k_buf, v_buf, s_buf, hid_buf)]
        hid, s_out, k_out, v_out, token = pl.pallas_call(
            write_kernel,
            name="write",
            out_shape=(jax.ShapeDtypeStruct((rows, width), BF16), jax.ShapeDtypeStruct(state_shape, F32),
                       jax.ShapeDtypeStruct(cache_shape, BF16), jax.ShapeDtypeStruct(cache_shape, BF16), vm((8, 128), F32)),
            in_specs=[pl.BlockSpec(memory_space=vm)] * 4,
            out_specs=[pl.BlockSpec(memory_space=any_)] * 4 + [pl.BlockSpec(memory_space=vm)],
            scratch_shapes=[dma((10,))],
            compiler_params=pltpu.CompilerParams(vmem_limit_bytes=20 * MIB),
        )(*bufs)
        x_buf = pl.pallas_call(
            tail_kernel,
            name="tail",
            out_shape=vm((LATE, shard_len, head_dim), BF16),
            in_specs=[pl.BlockSpec(memory_space=any_), pl.BlockSpec(memory_space=vm)],
            out_specs=pl.BlockSpec(memory_space=vm),
            scratch_shapes=[dma((LATE,)), dma((LATE,))],
            compiler_params=pltpu.CompilerParams(collective_id=1, has_side_effects=True, vmem_limit_bytes=4 * MIB),
        )(pltpu.with_memory_space_constraint(v_cache, pltpu.HBM), pltpu.with_memory_space_constraint(token, vm))
        v_out = pl.pallas_call(
            tail_write_kernel,
            name="tail_write",
            out_shape=jax.ShapeDtypeStruct(cache_shape, BF16),
            in_specs=[pl.BlockSpec(memory_space=any_), pl.BlockSpec(memory_space=vm)],
            out_specs=pl.BlockSpec(memory_space=any_),
            scratch_shapes=[dma((LATE,))],
            input_output_aliases={0: 0},
            compiler_params=pltpu.CompilerParams(vmem_limit_bytes=4 * MIB),
        )(v_out, pltpu.with_memory_space_constraint(x_buf, vm))
        return hid, s_out, k_out, v_out

    batch_spec = P(('dp', 'sp'), None)
    head_spec = P(('dp', 'sp'), 'tp', None, None)
    cache_spec = P('dp', 'tp', 'sp', None)
    in_specs = (batch_spec, P('sp', 'dp', 'tp', None, None), cache_spec, cache_spec, P('tp'), P(None), P(None, None, 'tp'), P(None, 'tp'), P('tp'), P('tp', None), P(None), P(None, 'tp', None, None), P('tp', None))
    out_specs = (batch_spec, head_spec, head_spec, head_spec)
    return jax.shard_map(device_step, mesh=mesh, in_specs=in_specs, out_specs=out_specs, check_vma=False)
```

```python
import math

import jax
import jax.numpy as jnp
import numpy as np
from jax import lax
from jax.experimental import pallas as pl
from jax.experimental.pallas import tpu as pltpu
from jax.sharding import PartitionSpec as P

NORM_EPS = 1e-6
ROPE_BASE = 10000000.0
RES_ALPHA = 1.0
RES_BETA = 1.0
CACHE_EXTRA = 16

MESH = pl.DeviceIdType.MESH
F32 = jnp.float32
BF16 = jnp.bfloat16
MIB = 2**20

ST_OWN, ST_FWD, ST_SUM = 0, 1, 2
SQ, PO, PA = 3, 6, 9
QX, MX, OX = 12, 15, 18
KV_NEAR = 21
KV_FAR = 23
NUM_SEMS = KV_FAR + 16
LATE = 2


def rope_table(head_dim, position):
    rope_dim = head_dim // 2
    half = rope_dim // 2
    inv_freq = ROPE_BASE ** (-np.arange(0, rope_dim, 2, dtype=np.float64) / rope_dim)
    cos, sin = np.cos(position * inv_freq), np.sin(position * inv_freq)
    table = np.zeros((8, head_dim), np.float32)
    table[0] = np.concatenate([cos, cos, np.ones(head_dim - rope_dim)])
    table[1, :rope_dim] = np.concatenate([-sin, sin])
    return table


def flip(index, mask):
    chip, core = index // 2, index % 2
    if mask & 2:
        chip = 1 - chip
    if mask & 1:
        core = 1 - core
    return chip * 2 + core


def silu(x):
    return x * (1.0 / (1.0 + jnp.exp(-x)))


def step_kernel(
    tokens, states, k_cache, v_cache, slopes, lin_gain, w_qkv, w_gate, out_gain, w_lin_out, attn_gain, w_in, w_attn_out, rope,
    k_buf, v_buf, s_out, hid, x_src,
    tok_v, lg_v, og_v, ag_v, rope_v, slope_s, qkv_v, gate_v, lout_v, in_v, aout_v,
    st_loc, st_rcv, st_sum, st_in, hb, rows_v, o_v, g_v, rep_v, acc_v, proj_v, qf_v, vf_v, qp_v, q_snd, q_all, sc_v, mrow_v, m_all, mcol_v,
    ns_v, ol_v, ol_sum, olr_v, ho_v, sq_all, po_all, pa_all, kst,
    send, recv, lsem, ksem, met,
):
    sp = lax.axis_index("sp")
    tp = lax.axis_index("tp")
    shard_len = k_cache.shape[2]
    kv_dev = k_cache.shape[1]
    head_dim = k_cache.shape[3]
    heads = slopes.shape[0]
    rows = tokens.shape[0]
    width = tokens.shape[1]
    group = heads // kv_dev
    prompt = 4 * shard_len
    local_w = heads * head_dim

    def to_sp(mask):
        return {"sp": flip(sp, mask)}

    def to_tp(off):
        return {"tp": lax.rem(tp + off, 4)}

    core = lax.rem(sp, 2)
    barrier = pltpu.get_barrier_semaphore()
    pl.semaphore_signal(barrier, inc=1, device_id=to_sp(2), device_id_type=MESH)

    @pl.when(core == 0)
    def _():
        for i in (1, 2, 3):
            pl.semaphore_signal(barrier, inc=1, device_id=to_tp(i), device_id_type=MESH)

    def remote(src, dst, i, dev):
        return pltpu.make_async_remote_copy(src, dst, send.at[i], recv.at[i], device_id=dev, device_id_type=MESH)

    def local(src, dst, i):
        return pltpu.make_async_copy(src, dst, lsem.at[i])

    my_rows = pl.ds(pl.multiple_of(sp * shard_len, shard_len), shard_len)
    pieces = [(t, b, j, mask) for t in range(2) for b in range(rows) for j in range(kv_dev) for mask in (2, 3)]
    late = [(1, rows - 1, j, 2) for j in range(kv_dev)[-LATE:]]
    pieces = sorted([p for p in pieces if p not in late], key=lambda p: p[0] > 0 or p[1] > 0) + late
    pieces[1], pieces[2] = pieces[2], pieces[1]
    far = []
    for t, b, j, mask in pieces:
        src, dst = ((k_cache, k_buf), (v_cache, v_buf))[t]
        far.append(remote(src.at[flip(sp, mask) * rows + b, j], dst.at[b, j, my_rows], KV_FAR + len(far), to_sp(mask)))
    n_both = len(far) - len(late)
    far_state = [0, 0]

    def start_far(n):
        for _ in range(n):
            if far_state[0] < n_both:
                far[far_state[0]].start()
                far_state[0] += 1

    def pump(n):
        for _ in range(n):
            far[far_state[1]].wait_send()
            far_state[1] += 1
            start_far(1)

    @pl.when(core == 1)
    def _():
        pl.semaphore_wait(barrier, 1)
        far[0].start()
        far[1].start()
        pl.semaphore_signal(barrier, inc=1, device_id=to_sp(1), device_id_type=MESH)
        pl.semaphore_wait(met.at[0], 1)

    @pl.when(core == 0)
    def _():
        pl.semaphore_wait(barrier, 5)
        pl.semaphore_signal(met.at[0], inc=1, device_id=to_sp(1), device_id_type=MESH)
        far[0].start()
        for i in (1, 2, 3):
            pl.semaphore_signal(met.at[2], inc=1, device_id=to_tp(i), device_id_type=MESH)

    def meet_tp():
        @pl.when(core == 0)
        def _():
            pl.semaphore_wait(met.at[2], 3)
            pl.semaphore_signal(met.at[1], inc=1, device_id=to_sp(1), device_id_type=MESH)

        @pl.when(core == 1)
        def _():
            pl.semaphore_wait(met.at[1], 1)

    def st_rows(g):
        return pl.ds(g * rows, rows)

    st_own = remote(states.at[0, st_rows(flip(sp, 1))], st_rcv.at[0], ST_OWN, to_sp(1))
    st_fwd = remote(states.at[0, st_rows(flip(sp, 3))], st_rcv.at[1], ST_FWD, to_sp(1))
    st_fwd.start()
    ld_fwd = local(states.at[0, st_rows(flip(sp, 2))], st_loc.at[1], 0)
    ld_slope = local(slopes, slope_s, 1)
    ld_fwd.start()
    ld_slope.start()
    st_own.start()
    ld_own = local(states.at[0, st_rows(sp)], st_loc.at[0], 2)
    ld_tok = local(tokens, tok_v, 3)
    ld_lg = local(lin_gain, lg_v, 4)
    ld_og = local(out_gain, og_v, 5)
    ld_ag = local(attn_gain, ag_v, 6)
    ld_rope = local(rope, rope_v, 7)
    ld_qkv = [local(w_qkv.at[j], qkv_v.at[j], 8 + j) for j in range(3)]
    ld_gate = local(w_gate, gate_v, 11)
    ld_lout = local(w_lin_out, lout_v, 12)
    ld_in = local(w_in, in_v, 13)
    ld_aout = local(w_attn_out, aout_v, 14)
    own_kv = [local(src.at[st_rows(sp)], dst.at[:, :, my_rows], 15 + t) for t, (src, dst) in enumerate(((k_cache, k_buf), (v_cache, v_buf)))]
    near = [remote(src.at[st_rows(flip(sp, 1))], dst.at[:, :, my_rows], KV_NEAR + t, to_sp(1)) for t, (src, dst) in enumerate(((k_cache, k_buf), (v_cache, v_buf)))]
    ld_x = local(v_cache.at[flip(sp, 2) * rows + rows - 1, pl.ds(kv_dev - LATE, LATE)], x_src, 17)
    for c in [ld_own, ld_tok, ld_lg, ld_og, ld_ag, ld_rope] + ld_qkv + [ld_gate, ld_lout, ld_in, ld_aout] + near + own_kv + [ld_x]:
        c.start()

    def decay(h, shard):
        off = (shard_len * (3 - shard)).astype(F32)
        return jnp.exp(jnp.full((1, head_dim), -slope_s[h] * off, F32))

    st_fwd.wait_recv()
    ld_slope.wait()
    ld_fwd.wait()
    for h in range(heads):
        w_me, w_ot = decay(h, sp), decay(h, flip(sp, 1))
        for b in range(rows):
            st_sum[b, h] = w_me * st_loc[1, b, h] + w_ot * st_rcv[1, b, h]
    st_send = remote(st_sum, st_in, ST_SUM, to_sp(2))
    st_send.start()

    @pl.when(core == 0)
    def _():
        far[1].start()

    far_state[0] = 2
    start_far(1)

    st_own.wait_recv()
    st_send.wait_recv()
    start_far(1)
    ld_own.wait()
    ld_tok.wait()
    ld_lg.wait()
    x = tok_v[...].astype(F32)
    inv = lax.rsqrt(jnp.mean(x * x, axis=-1, keepdims=True) + NORM_EPS)
    hb[...] = (x * inv * lg_v[...]).astype(BF16)

    def matvec(x_ref, w_ref, k_len, n_len, kb, out_dtype=F32):
        def body(k, acc):
            at = pl.ds(pl.multiple_of(k * kb, kb), kb)
            return acc + jnp.dot(x_ref[:, at], w_ref[at, :], preferred_element_type=F32)
        return lax.fori_loop(0, k_len // kb, body, jnp.zeros((rows, n_len), F32))

    acts = []
    for j in range(3):
        ld_qkv[j].wait()
        acts.append(silu(matvec(hb, qkv_v.at[j], width, local_w, 256)).astype(BF16).astype(F32))
    ld_gate.wait()
    gate = 1.0 / (1.0 + jnp.exp(-matvec(hb, gate_v, width, local_w, 256)))
    rows_v[...] = jnp.zeros_like(rows_v)
    for b in range(rows):
        for h in range(heads):
            cols = slice(h * head_dim, (h + 1) * head_dim)
            rows_v[pl.ds(b * 8 + h, 1), :] = acts[0][b:b + 1, cols]
            rows_v[pl.ds(16 + b * 8 + h, 1), :] = acts[1][b:b + 1, cols]
    cols_t = jnp.transpose(rows_v[...])

    for h in range(heads):
        w_me, w_ot = decay(h, sp), decay(h, flip(sp, 1))
        lam = jnp.exp(jnp.full((1, head_dim), -slope_s[h], F32))
        cols = slice(h * head_dim, (h + 1) * head_dim)
        for b in range(rows):
            moved = w_me * st_loc[0, b, h] + w_ot * st_rcv[0, b, h] + st_in[b, h]
            q_col = cols_t[:, b * 8 + h:b * 8 + h + 1]
            k_col = cols_t[:, 16 + b * 8 + h:16 + b * 8 + h + 1]
            new = lam * moved + k_col * acts[2][b:b + 1, cols]
            s_out[b, h] = new
            o_v[pl.ds(b, 1), cols] = jnp.sum(q_col * new, axis=0, keepdims=True)
    o = o_v[...]

    def gather_tp(ref, base):
        cs = [remote(ref.at[tp], ref.at[tp], base + i - 1, to_tp(i)) for i in (1, 2, 3)]
        for c in cs:
            c.start()
        return cs

    def settle(cs):
        for c in cs:
            c.wait_recv()
        for c in cs:
            c.wait_send()

    sq_all[tp] = jnp.broadcast_to(jnp.sum(o * o, axis=-1, keepdims=True), (rows, 128))
    meet_tp()
    cs = gather_tp(sq_all, SQ)
    pump(1)
    ld_og.wait()
    settle(cs)
    sq = ((sq_all[0] + sq_all[1]) + sq_all[2]) + sq_all[3]
    inv = lax.rsqrt(sq[:, :1] / (4 * local_w) + NORM_EPS)
    out_g = jnp.concatenate([og_v[h:h + 1, :] for h in range(heads)], axis=1)
    g_v[...] = (o * inv * out_g * gate).astype(BF16)

    def project(x_ref, w_ref, dst):
        nb = 512

        def body(n, _):
            at = pl.ds(pl.multiple_of(n * nb, nb), nb)
            dst[tp, :, at] = jnp.dot(x_ref[...], w_ref[:, at], preferred_element_type=F32)
            return 0
        lax.fori_loop(0, width // nb, body, 0)

    ld_lout.wait()
    project(g_v, lout_v, po_all)
    cs = gather_tp(po_all, PO)
    reps = in_v.shape[0] // width
    d_id = lax.broadcasted_iota(jnp.int32, rep_v.shape, 0)
    l_id = lax.broadcasted_iota(jnp.int32, rep_v.shape, 1)
    rep_v[...] = jnp.where((l_id >= d_id * reps) & (l_id < d_id * reps + reps), 1.0, 0.0).astype(BF16)
    settle(cs)
    lin = ((po_all[0] + po_all[1]) + po_all[2]) + po_all[3]
    y = (RES_ALPHA * hb[...].astype(F32) + RES_BETA * lin).astype(BF16).astype(F32)

    ld_ag.wait()
    inv = lax.rsqrt(jnp.mean(y * y, axis=-1, keepdims=True) + NORM_EPS)
    hb[...] = (y * inv * ag_v[...]).astype(BF16)
    ld_in.wait()
    ld_rope.wait()
    lane = lax.broadcasted_iota(jnp.int32, (16, 128 * reps), 1)
    sub = lax.broadcasted_iota(jnp.int32, (16, 128 * reps), 0)
    pick = lax.rem(lane, reps) == sub

    def in_body(d, acc):
        xb = hb[:, pl.ds(pl.multiple_of(d * 128, 128), 128)]
        xr = jnp.dot(xb, rep_v[...], preferred_element_type=F32)
        lhs = jnp.concatenate([jnp.where(pick, xr[b:b + 1], 0.0) for b in range(rows)], axis=0).astype(BF16)
        w = in_v[pl.ds(pl.multiple_of(d * 128 * reps, 128), 128 * reps), :]
        return acc + jnp.dot(lhs, w, preferred_element_type=F32)

    proj = lax.fori_loop(0, width // 128, in_body, jnp.zeros((16 * rows, head_dim), F32)).astype(BF16).astype(F32)
    lane = lax.broadcasted_iota(jnp.int32, proj.shape, 1)
    quarter = head_dim // 4
    partner = jnp.where(lane < quarter, pltpu.roll(proj, head_dim - quarter, 1), pltpu.roll(proj, quarter, 1))
    proj_v[...] = proj
    acc_v[...] = (proj * rope_v[0:1] + partner * rope_v[1:2]).astype(BF16).astype(F32)
    qf_v[...] = jnp.zeros_like(qf_v)
    qp_v[...] = jnp.zeros_like(qp_v)
    ns_v[...] = jnp.zeros_like(ns_v)
    tail_row = lax.broadcasted_iota(jnp.int32, (CACHE_EXTRA, head_dim), 0)
    for b in range(rows):
        for j in range(kv_dev):
            p = b * kv_dev + j
            for g in range(group):
                q_row = acc_v[pl.ds(b * 16 + g * kv_dev + j, 1), :]
                qf_v[pl.ds(p * 8 + g, 1), :] = q_row
                qp_v[pl.ds(p * 4 + g, 1), :] = q_row
            k_new = acc_v[pl.ds(b * 16 + group * kv_dev + j, 1), :]
            v_new = proj_v[pl.ds(b * 16 + (group + 1) * kv_dev + j, 1), :]
            k_buf[b, j, pl.ds(prompt, CACHE_EXTRA), :] = jnp.where(tail_row == 0, k_new, 0.0).astype(BF16)
            v_buf[b, j, pl.ds(prompt, CACHE_EXTRA), :] = jnp.where(tail_row == 0, v_new, 0.0).astype(BF16)
            vf_v[pl.ds(p * 8, 8), :] = jnp.broadcast_to(v_new, (8, head_dim))
            ns_v[pl.ds(p * 8, 8), :] = jnp.broadcast_to(k_new, (8, head_dim))
    qf = qf_v[...]
    pairs = rows * kv_dev
    my_pairs = pl.ds(sp * pairs, pairs)
    q_snd[sp] = qp_v[...].astype(BF16)
    cs = [remote(q_snd.at[sp], q_snd.at[sp], QX + i - 1, to_sp(i)) for i in (1, 2)]
    for c in cs:
        c.start()
    pump(2)
    scale = head_dim ** -0.5
    ns_v[...] = jnp.broadcast_to(jnp.sum(qf * ns_v[...], axis=-1, keepdims=True) * scale, ns_v.shape)

    n_pairs = 4 * pairs
    slots = kst.shape[0]

    def fetch(cache, i):
        slot = lax.rem(i, slots)
        return pltpu.make_async_copy(cache.at[i // kv_dev, lax.rem(i, kv_dev)], kst.at[slot], ksem.at[slot])

    def stream(cache, first, body):
        def step(i, _):
            fetch(cache, i).wait()
            body(i, kst[lax.rem(i, slots)])

            @pl.when(i + slots < n_pairs)
            def _():
                fetch(cache, i + slots).start()
            return 0
        lax.fori_loop(0, n_pairs, step, 0)

    for i in range(slots):
        fetch(k_cache, jnp.int32(i)).start()
    cs[1].wait_recv()
    hand_on = remote(q_snd.at[flip(sp, 2)], q_snd.at[flip(sp, 2)], QX + 2, to_sp(1))
    hand_on.start()
    cs[0].wait_recv()
    hand_on.wait_recv()
    for c in cs + [hand_on]:
        c.wait_send()
    pump(1)
    for d in range(4):
        got = q_snd[d].astype(F32)
        for p in range(pairs):
            q_all[d * pairs + p] = jnp.concatenate([got[p * 4:p * 4 + 4], jnp.zeros((4, head_dim), F32)], axis=0).astype(BF16)

    def score_body(i, keys):
        s = lax.dot_general(q_all[i], keys, (((1,), (1,)), ((), ())), preferred_element_type=F32) * scale
        sc_v[i] = s
        mrow_v[pl.ds(pl.multiple_of(i * 8, 8), 8), :] = jnp.broadcast_to(jnp.max(s, axis=-1, keepdims=True), (8, 128))

    stream(k_cache, 0, score_body)
    for i in range(slots):
        fetch(v_cache, jnp.int32(i)).start()
    my_m = pl.ds(pl.multiple_of(sp * pairs * 8, 8), pairs * 8)
    mrow_v[my_m, :] = jnp.maximum(mrow_v[my_m, :], ns_v[...])
    m_all[sp] = jnp.transpose(mrow_v[...])[:1]
    cs = [remote(m_all.at[sp], m_all.at[sp], MX + i - 1, to_sp(i)) for i in (1, 2, 3)]
    for c in cs:
        c.start()
    pump(1)
    settle(cs)
    m = jnp.maximum(jnp.maximum(m_all[0], m_all[1]), jnp.maximum(m_all[2], m_all[3]))
    mcol_v[...] = jnp.transpose(jnp.broadcast_to(m, (128, 128)))
    pump(1)
    lane = lax.broadcasted_iota(jnp.int32, (1, head_dim), 1)

    def out_body(i, values):
        p = jnp.exp(sc_v[i] - mcol_v[pl.ds(pl.multiple_of(i * 8, 8), 8), :][:, :1])
        total = jnp.sum(p, axis=-1, keepdims=True)
        o = jnp.dot(p.astype(BF16), values, preferred_element_type=F32)
        sums = jnp.zeros((1, head_dim), F32)
        for g in range(group):
            sums = jnp.where(lane == g, total[g:g + 1], sums)
        ol_v[i] = jnp.concatenate([o[:group], sums], axis=0)

    stream(v_cache, 0, out_body)
    o_fwd = remote(ol_v.at[pl.ds(flip(sp, 3) * pairs, pairs)], olr_v.at[1], OX, to_sp(1))
    o_own = remote(ol_v.at[pl.ds(flip(sp, 1) * pairs, pairs)], olr_v.at[0], OX + 1, to_sp(1))
    o_fwd.start()
    o_own.start()
    o_fwd.wait_recv()
    ol_sum[...] = ol_v[pl.ds(flip(sp, 2) * pairs, pairs)] + olr_v[1]
    o_sum = remote(ol_sum, olr_v.at[2], OX + 2, to_sp(2))
    o_sum.start()
    pump(1)
    o_own.wait_recv()
    o_sum.wait_recv()
    for c in (o_fwd, o_own, o_sum):
        c.wait_send()
    mine = ol_v[my_pairs]
    new_p = jnp.exp(ns_v[...] - mcol_v[my_m, :])
    new_o = new_p.astype(BF16).astype(F32) * vf_v[...]
    for b in range(rows):
        for j in range(kv_dev):
            p = b * kv_dev + j
            total = (mine[p] + olr_v[0, p]) + olr_v[2, p]
            for g in range(group):
                h, at = j * group + g, p * 8 + g
                denom = total[group:group + 1, g:g + 1] + new_p[at:at + 1]
                ho_v[pl.ds(b, 1), h * head_dim:(h + 1) * head_dim] = (total[g:g + 1] + new_o[at:at + 1]) / denom
    g_v[...] = ho_v[...].astype(BF16)
    ld_aout.wait()
    project(g_v, aout_v, pa_all)
    cs = gather_tp(pa_all, PA)
    start_far(len(far))

    @pl.when(core == 0)
    def _():
        for c in far[n_both:]:
            c.start()

    settle(cs)
    att = ((pa_all[0] + pa_all[1]) + pa_all[2]) + pa_all[3]
    hid[...] = (RES_ALPHA * hb[...].astype(F32) + RES_BETA * att).astype(BF16)

    st_own.wait_send()
    st_fwd.wait_send()
    st_send.wait_send()
    for c in own_kv + [ld_x]:
        c.wait()
    for c in near:
        c.wait()
    for c in far[far_state[1]:n_both]:
        c.wait_send()
    for c in far[:n_both]:
        c.wait_recv()

    @pl.when(core == 0)
    def _():
        for c in far[n_both:]:
            c.wait()


def tail_kernel(x_src, token, x_buf, send, recv):
    sp = lax.axis_index("sp")
    peer = flip(sp, 2)
    barrier = pltpu.get_barrier_semaphore()
    pl.semaphore_signal(barrier, inc=1, device_id={"sp": peer}, device_id_type=MESH)
    pl.semaphore_wait(barrier, 1)

    @pl.when(lax.rem(sp, 2) == 1)
    def _():
        cs = []
        for i in range(LATE):
            cs.append(pltpu.make_async_remote_copy(
                x_src.at[i], x_buf.at[i], send.at[i], recv.at[i], device_id={"sp": peer}, device_id_type=MESH))
            cs[-1].start()
        for c in cs:
            c.wait()


def tail_write_kernel(v_in, x_buf, v_out, sem):
    sp = lax.axis_index("sp")
    rows, kv_dev = v_out.shape[:2]
    shard_len = x_buf.shape[1]

    @pl.when(lax.rem(sp, 2) == 1)
    def _():
        cs = []
        for i in range(LATE):
            at = pl.ds(pl.multiple_of(flip(sp, 2) * shard_len, shard_len), shard_len)
            cs.append(pltpu.make_async_copy(x_buf.at[i], v_out.at[rows - 1, kv_dev - LATE + i, at], sem.at[i]))
            cs[-1].start()
        for c in cs:
            c.wait()


def write_kernel(k_buf, v_buf, s_buf, hid_buf, hid, s_out, k_out, v_out, token, sem):
    token[...] = jnp.zeros_like(token)
    cs = []
    for src, dst in ((k_buf, k_out), (v_buf, v_out)):
        for b in range(src.shape[0]):
            for j in range(src.shape[1]):
                cs.append(pltpu.make_async_copy(src.at[b, j], dst.at[b, j], sem.at[len(cs)]))
    cs.append(pltpu.make_async_copy(s_buf, s_out, sem.at[len(cs)]))
    cs.append(pltpu.make_async_copy(hid_buf, hid, sem.at[len(cs)]))
    for c in cs:
        c.start()
    for c in cs:
        c.wait()


def solution(mesh):
    def device_step(tokens, states, k_cache, v_cache, slopes, lin_gain, w_lin_qkv, w_lin_gate, out_gain, w_lin_out, attn_gain, w_attn_in, w_attn_out):
        rows, width = tokens.shape
        seqs, kv_dev, shard_len, head_dim = k_cache.shape
        heads = slopes.shape[0]
        local_w = heads * head_dim
        prompt = 4 * shard_len
        reps = w_attn_in.shape[1] * w_attn_in.shape[2]
        pairs = rows * kv_dev
        group = heads // kv_dev
        cache_shape = (rows, kv_dev, prompt + CACHE_EXTRA, head_dim)
        state_shape = (rows, heads, head_dim, head_dim)
        vm, any_ = pltpu.VMEM, pl.ANY
        w_qkv = jnp.transpose(w_lin_qkv, (1, 0, 2))
        w_in = jnp.transpose(w_attn_in, (0, 2, 1, 3)).reshape(width * reps, head_dim)
        rope = jnp.asarray(rope_table(head_dim, prompt))
        dma = pltpu.SemaphoreType.DMA
        x_shape = (LATE, shard_len, head_dim)
        k_buf, v_buf, s_buf, hid_buf, x_src = pl.pallas_call(
            step_kernel,
            name="step",
            out_shape=(vm(cache_shape, BF16), vm(cache_shape, BF16), vm(state_shape, F32), vm((rows, width), BF16), vm(x_shape, BF16)),
            in_specs=[pl.BlockSpec(memory_space=any_)] * 14,
            out_specs=[pl.BlockSpec(memory_space=vm)] * 5,
            scratch_shapes=[
                vm((rows, width), BF16), vm((1, width), F32), vm((heads, head_dim), F32), vm((1, width), F32), vm((8, head_dim), F32),
                pltpu.SMEM((heads,), F32), vm((3, width, local_w), BF16), vm((width, local_w), BF16), vm((local_w, width), BF16),
                vm((width * reps, head_dim), BF16), vm((local_w, width), BF16),
                vm((2,) + state_shape, F32), vm((2,) + state_shape, F32), vm(state_shape, F32), vm(state_shape, F32),
                vm((rows, width), BF16), vm((128, head_dim), F32), vm((rows, local_w), F32), vm((rows, local_w), BF16),
                vm((128, 128 * reps), BF16), vm((16 * rows, head_dim), F32), vm((16 * rows, head_dim), F32),
                vm((8 * pairs, head_dim), F32), vm((8 * pairs, head_dim), F32), vm((4 * pairs, head_dim), F32), vm((4, 4 * pairs, head_dim), BF16), vm((4 * pairs, 8, head_dim), BF16),
                vm((4 * pairs, 8, shard_len), F32), vm((128, 128), F32), vm((4, 1, 128), F32), vm((128, 128), F32),
                vm((8 * pairs, head_dim), F32), vm((4 * pairs, group + 1, head_dim), F32), vm((pairs, group + 1, head_dim), F32), vm((3, pairs, group + 1, head_dim), F32),
                vm((rows, local_w), F32), vm((4, rows, 128), F32), vm((4, rows, width), F32), vm((4, rows, width), F32),
                vm((4, shard_len, head_dim), BF16),
                dma((NUM_SEMS,)), dma((NUM_SEMS,)), dma((18,)), dma((4,)), pltpu.SemaphoreType.REGULAR((3,)),
            ],
            compiler_params=pltpu.CompilerParams(collective_id=0, has_side_effects=True, vmem_limit_bytes=45 * MIB),
        )(tokens, states, k_cache, v_cache, slopes, lin_gain.reshape(1, -1), w_qkv, w_lin_gate, out_gain.reshape(heads, head_dim), w_lin_out, attn_gain.reshape(1, -1), w_in, w_attn_out, rope)
        bufs = [pltpu.with_memory_space_constraint(a, vm) for a in (k_buf, v_buf, s_buf, hid_buf)]
        hid, s_out, k_out, v_out, token = pl.pallas_call(
            write_kernel,
            name="write",
            out_shape=(jax.ShapeDtypeStruct((rows, width), BF16), jax.ShapeDtypeStruct(state_shape, F32),
                       jax.ShapeDtypeStruct(cache_shape, BF16), jax.ShapeDtypeStruct(cache_shape, BF16), vm((8, 128), F32)),
            in_specs=[pl.BlockSpec(memory_space=vm)] * 4,
            out_specs=[pl.BlockSpec(memory_space=any_)] * 4 + [pl.BlockSpec(memory_space=vm)],
            scratch_shapes=[dma((10,))],
            compiler_params=pltpu.CompilerParams(vmem_limit_bytes=20 * MIB),
        )(*bufs)
        x_buf = pl.pallas_call(
            tail_kernel,
            name="tail",
            out_shape=vm(x_shape, BF16),
            in_specs=[pl.BlockSpec(memory_space=vm), pl.BlockSpec(memory_space=vm)],
            out_specs=pl.BlockSpec(memory_space=vm),
            scratch_shapes=[dma((LATE,)), dma((LATE,))],
            compiler_params=pltpu.CompilerParams(collective_id=1, has_side_effects=True, vmem_limit_bytes=4 * MIB),
        )(pltpu.with_memory_space_constraint(x_src, vm), pltpu.with_memory_space_constraint(token, vm))
        v_out = pl.pallas_call(
            tail_write_kernel,
            name="tail_write",
            out_shape=jax.ShapeDtypeStruct(cache_shape, BF16),
            in_specs=[pl.BlockSpec(memory_space=any_), pl.BlockSpec(memory_space=vm)],
            out_specs=pl.BlockSpec(memory_space=any_),
            scratch_shapes=[dma((LATE,))],
            input_output_aliases={0: 0},
            compiler_params=pltpu.CompilerParams(vmem_limit_bytes=4 * MIB),
        )(v_out, pltpu.with_memory_space_constraint(x_buf, vm))
        return hid, s_out, k_out, v_out

    batch_spec = P(('dp', 'sp'), None)
    head_spec = P(('dp', 'sp'), 'tp', None, None)
    cache_spec = P('dp', 'tp', 'sp', None)
    in_specs = (batch_spec, P('sp', 'dp', 'tp', None, None), cache_spec, cache_spec, P('tp'), P(None), P(None, None, 'tp'), P(None, 'tp'), P('tp'), P('tp', None), P(None), P(None, 'tp', None, None), P('tp', None))
    out_specs = (batch_spec, head_spec, head_spec, head_spec)
    return jax.shard_map(device_step, mesh=mesh, in_specs=in_specs, out_specs=out_specs, check_vma=False)
```

```python
import math

import jax
import jax.numpy as jnp
import numpy as np
from jax import lax
from jax.experimental import pallas as pl
from jax.experimental.pallas import tpu as pltpu
from jax.sharding import PartitionSpec as P

NORM_EPS = 1e-6
ROPE_BASE = 10000000.0
RES_ALPHA = 1.0
RES_BETA = 1.0
CACHE_EXTRA = 16

MESH = pl.DeviceIdType.MESH
F32 = jnp.float32
BF16 = jnp.bfloat16
MIB = 2**20

ST_OWN, ST_FWD, ST_SUM = 0, 1, 2
SQ, PO, PA = 3, 6, 9
QX, MX, OX = 12, 15, 18
KV_NEAR = 21
KV_FAR = 23
NUM_SEMS = KV_FAR + 16
LATE = 2


def rope_table(head_dim, position):
    rope_dim = head_dim // 2
    half = rope_dim // 2
    inv_freq = ROPE_BASE ** (-np.arange(0, rope_dim, 2, dtype=np.float64) / rope_dim)
    cos, sin = np.cos(position * inv_freq), np.sin(position * inv_freq)
    table = np.zeros((8, head_dim), np.float32)
    table[0] = np.concatenate([cos, cos, np.ones(head_dim - rope_dim)])
    table[1, :rope_dim] = np.concatenate([-sin, sin])
    return table


def flip(index, mask):
    chip, core = index // 2, index % 2
    if mask & 2:
        chip = 1 - chip
    if mask & 1:
        core = 1 - core
    return chip * 2 + core


def silu(x):
    return x * (1.0 / (1.0 + jnp.exp(-x)))


def step_kernel(
    tokens, states, k_cache, v_cache, slopes, lin_gain, w_qkv, w_gate, out_gain, w_lin_out, attn_gain, w_in, w_attn_out, rope,
    k_buf, v_buf, s_out, hid, x_src,
    tok_v, lg_v, og_v, ag_v, rope_v, slope_s, qkv_v, gate_v, lout_v, in_v, aout_v,
    st_loc, st_rcv, st_sum, st_in, hb, rows_v, o_v, g_v, rep_v, acc_v, proj_v, qf_v, vf_v, qp_v, q_snd, q_all, sc_v, mrow_v, m_all, mcol_v,
    ns_v, ol_v, ol_sum, olr_v, ho_v, sq_all, po_all, pa_all, kst,
    send, recv, lsem, ksem, met,
):
    sp = lax.axis_index("sp")
    tp = lax.axis_index("tp")
    shard_len = k_cache.shape[2]
    kv_dev = k_cache.shape[1]
    head_dim = k_cache.shape[3]
    heads = slopes.shape[0]
    rows = tokens.shape[0]
    width = tokens.shape[1]
    group = heads // kv_dev
    prompt = 4 * shard_len
    local_w = heads * head_dim

    def to_sp(mask):
        return {"sp": flip(sp, mask)}

    def to_tp(off):
        return {"tp": lax.rem(tp + off, 4)}

    core = lax.rem(sp, 2)
    barrier = pltpu.get_barrier_semaphore()
    pl.semaphore_signal(barrier, inc=1, device_id=to_sp(2), device_id_type=MESH)

    @pl.when(core == 0)
    def _():
        for i in (1, 2, 3):
            pl.semaphore_signal(barrier, inc=1, device_id=to_tp(i), device_id_type=MESH)

    def remote(src, dst, i, dev):
        return pltpu.make_async_remote_copy(src, dst, send.at[i], recv.at[i], device_id=dev, device_id_type=MESH)

    def local(src, dst, i):
        return pltpu.make_async_copy(src, dst, lsem.at[i])

    my_rows = pl.ds(pl.multiple_of(sp * shard_len, shard_len), shard_len)
    pieces = [(t, b, j, mask) for t in range(2) for b in range(rows) for j in range(kv_dev) for mask in (2, 3)]
    late = [(1, rows - 1, j, 2) for j in range(kv_dev)[-LATE:]]
    pieces = sorted([p for p in pieces if p not in late], key=lambda p: p[0] > 0 or p[1] > 0) + late
    pieces[1], pieces[2] = pieces[2], pieces[1]
    far = []
    for t, b, j, mask in pieces:
        src, dst = ((k_cache, k_buf), (v_cache, v_buf))[t]
        far.append(remote(src.at[flip(sp, mask) * rows + b, j], dst.at[b, j, my_rows], KV_FAR + len(far), to_sp(mask)))
    n_both = len(far) - len(late)
    far_state = [0, 0]

    def start_far(n):
        for _ in range(n):
            if far_state[0] < n_both:
                far[far_state[0]].start()
                far_state[0] += 1

    def pump(n):
        for _ in range(n):
            far[far_state[1]].wait_send()
            far_state[1] += 1
            start_far(1)

    @pl.when(core == 1)
    def _():
        pl.semaphore_wait(barrier, 1)
        far[0].start()
        far[1].start()
        pl.semaphore_signal(barrier, inc=1, device_id=to_sp(1), device_id_type=MESH)
        pl.semaphore_wait(met.at[0], 1)

    @pl.when(core == 0)
    def _():
        pl.semaphore_wait(barrier, 5)
        pl.semaphore_signal(met.at[0], inc=1, device_id=to_sp(1), device_id_type=MESH)
        far[0].start()
        for i in (1, 2, 3):
            pl.semaphore_signal(met.at[2], inc=1, device_id=to_tp(i), device_id_type=MESH)

    def meet_tp():
        @pl.when(core == 0)
        def _():
            pl.semaphore_wait(met.at[2], 3)
            pl.semaphore_signal(met.at[1], inc=1, device_id=to_sp(1), device_id_type=MESH)

        @pl.when(core == 1)
        def _():
            pl.semaphore_wait(met.at[1], 1)

    def st_rows(g):
        return pl.ds(g * rows, rows)

    st_own = remote(states.at[0, st_rows(flip(sp, 1))], st_rcv.at[0], ST_OWN, to_sp(1))
    st_fwd = remote(states.at[0, st_rows(flip(sp, 3))], st_rcv.at[1], ST_FWD, to_sp(1))
    st_fwd.start()
    ld_fwd = local(states.at[0, st_rows(flip(sp, 2))], st_loc.at[1], 0)
    ld_slope = local(slopes, slope_s, 1)
    ld_fwd.start()
    ld_slope.start()
    st_own.start()
    ld_own = local(states.at[0, st_rows(sp)], st_loc.at[0], 2)
    ld_tok = local(tokens, tok_v, 3)
    ld_lg = local(lin_gain, lg_v, 4)
    ld_og = local(out_gain, og_v, 5)
    ld_ag = local(attn_gain, ag_v, 6)
    ld_rope = local(rope, rope_v, 7)
    ld_qkv = [local(w_qkv.at[j], qkv_v.at[j], 8 + j) for j in range(3)]
    ld_gate = local(w_gate, gate_v, 11)
    ld_lout = local(w_lin_out, lout_v, 12)
    ld_in = local(w_in, in_v, 13)
    ld_aout = local(w_attn_out, aout_v, 14)
    own_kv = [local(src.at[st_rows(sp)], dst.at[:, :, my_rows], 15 + t) for t, (src, dst) in enumerate(((k_cache, k_buf), (v_cache, v_buf)))]
    near = [remote(src.at[st_rows(flip(sp, 1))], dst.at[:, :, my_rows], KV_NEAR + t, to_sp(1)) for t, (src, dst) in enumerate(((k_cache, k_buf), (v_cache, v_buf)))]
    ld_x = local(v_cache.at[flip(sp, 2) * rows + rows - 1, pl.ds(kv_dev - LATE, LATE)], x_src, 17)
    for c in [ld_own, ld_tok, ld_lg, ld_og, ld_ag, ld_rope] + ld_qkv + [ld_gate, ld_lout, ld_in, ld_aout] + near + own_kv + [ld_x]:
        c.start()

    def decay(h, shard):
        off = (shard_len * (3 - shard)).astype(F32)
        return jnp.exp(jnp.full((1, head_dim), -slope_s[h] * off, F32))

    st_fwd.wait_recv()
    ld_slope.wait()
    ld_fwd.wait()
    for h in range(heads):
        w_me, w_ot = decay(h, sp), decay(h, flip(sp, 1))
        for b in range(rows):
            st_sum[b, h] = w_me * st_loc[1, b, h] + w_ot * st_rcv[1, b, h]
    st_send = remote(st_sum, st_in, ST_SUM, to_sp(2))
    st_send.start()

    @pl.when(core == 0)
    def _():
        far[1].start()

    far_state[0] = 2
    start_far(1)

    st_own.wait_recv()
    st_send.wait_recv()
    start_far(1)
    ld_own.wait()
    ld_tok.wait()
    ld_lg.wait()
    x = tok_v[...].astype(F32)
    inv = lax.rsqrt(jnp.mean(x * x, axis=-1, keepdims=True) + NORM_EPS)
    hb[...] = (x * inv * lg_v[...]).astype(BF16)

    def matvec(x_ref, w_ref, k_len, n_len, kb, out_dtype=F32):
        def body(k, acc):
            at = pl.ds(pl.multiple_of(k * kb, kb), kb)
            return acc + jnp.dot(x_ref[:, at], w_ref[at, :], preferred_element_type=F32)
        return lax.fori_loop(0, k_len // kb, body, jnp.zeros((rows, n_len), F32))

    acts = []
    for j in range(3):
        ld_qkv[j].wait()
        acts.append(silu(matvec(hb, qkv_v.at[j], width, local_w, 256)).astype(BF16).astype(F32))
    ld_gate.wait()
    gate = 1.0 / (1.0 + jnp.exp(-matvec(hb, gate_v, width, local_w, 256)))
    rows_v[...] = jnp.zeros_like(rows_v)
    for b in range(rows):
        for h in range(heads):
            cols = slice(h * head_dim, (h + 1) * head_dim)
            rows_v[pl.ds(b * 8 + h, 1), :] = acts[0][b:b + 1, cols]
            rows_v[pl.ds(16 + b * 8 + h, 1), :] = acts[1][b:b + 1, cols]
    cols_t = jnp.transpose(rows_v[...])

    for h in range(heads):
        w_me, w_ot = decay(h, sp), decay(h, flip(sp, 1))
        lam = jnp.exp(jnp.full((1, head_dim), -slope_s[h], F32))
        cols = slice(h * head_dim, (h + 1) * head_dim)
        for b in range(rows):
            moved = w_me * st_loc[0, b, h] + w_ot * st_rcv[0, b, h] + st_in[b, h]
            q_col = cols_t[:, b * 8 + h:b * 8 + h + 1]
            k_col = cols_t[:, 16 + b * 8 + h:16 + b * 8 + h + 1]
            new = lam * moved + k_col * acts[2][b:b + 1, cols]
            s_out[b, h] = new
            o_v[pl.ds(b, 1), cols] = jnp.sum(q_col * new, axis=0, keepdims=True)
    o = o_v[...]

    def gather_tp(ref, base):
        cs = [remote(ref.at[tp], ref.at[tp], base + i - 1, to_tp(i)) for i in (1, 2, 3)]
        for c in cs:
            c.start()
        return cs

    def settle(cs):
        for c in cs:
            c.wait_recv()
        for c in cs:
            c.wait_send()

    sq_all[tp] = jnp.broadcast_to(jnp.sum(o * o, axis=-1, keepdims=True), (rows, 128))
    meet_tp()
    cs = gather_tp(sq_all, SQ)
    pump(1)
    ld_og.wait()
    settle(cs)
    sq = ((sq_all[0] + sq_all[1]) + sq_all[2]) + sq_all[3]
    inv = lax.rsqrt(sq[:, :1] / (4 * local_w) + NORM_EPS)
    out_g = jnp.concatenate([og_v[h:h + 1, :] for h in range(heads)], axis=1)
    g_v[...] = (o * inv * out_g * gate).astype(BF16)

    def project(x_ref, w_ref, dst):
        nb = 512

        def body(n, _):
            at = pl.ds(pl.multiple_of(n * nb, nb), nb)
            dst[tp, :, at] = jnp.dot(x_ref[...], w_ref[:, at], preferred_element_type=F32)
            return 0
        lax.fori_loop(0, width // nb, body, 0)

    ld_lout.wait()
    project(g_v, lout_v, po_all)
    cs = gather_tp(po_all, PO)
    reps = in_v.shape[0] // width
    d_id = lax.broadcasted_iota(jnp.int32, rep_v.shape, 0)
    l_id = lax.broadcasted_iota(jnp.int32, rep_v.shape, 1)
    rep_v[...] = jnp.where((l_id >= d_id * reps) & (l_id < d_id * reps + reps), 1.0, 0.0).astype(BF16)
    settle(cs)
    lin = ((po_all[0] + po_all[1]) + po_all[2]) + po_all[3]
    y = (RES_ALPHA * hb[...].astype(F32) + RES_BETA * lin).astype(BF16).astype(F32)

    ld_ag.wait()
    inv = lax.rsqrt(jnp.mean(y * y, axis=-1, keepdims=True) + NORM_EPS)
    hb[...] = (y * inv * ag_v[...]).astype(BF16)
    ld_in.wait()
    ld_rope.wait()
    lane = lax.broadcasted_iota(jnp.int32, (16, 128 * reps), 1)
    sub = lax.broadcasted_iota(jnp.int32, (16, 128 * reps), 0)
    pick = lax.rem(lane, reps) == sub

    def in_body(d, acc):
        xb = hb[:, pl.ds(pl.multiple_of(d * 128, 128), 128)]
        xr = jnp.dot(xb, rep_v[...], preferred_element_type=F32)
        lhs = jnp.concatenate([jnp.where(pick, xr[b:b + 1], 0.0) for b in range(rows)], axis=0).astype(BF16)
        w = in_v[pl.ds(pl.multiple_of(d * 128 * reps, 128), 128 * reps), :]
        return acc + jnp.dot(lhs, w, preferred_element_type=F32)

    proj = lax.fori_loop(0, width // 128, in_body, jnp.zeros((16 * rows, head_dim), F32)).astype(BF16).astype(F32)
    lane = lax.broadcasted_iota(jnp.int32, proj.shape, 1)
    quarter = head_dim // 4
    partner = jnp.where(lane < quarter, pltpu.roll(proj, head_dim - quarter, 1), pltpu.roll(proj, quarter, 1))
    proj_v[...] = proj
    acc_v[...] = (proj * rope_v[0:1] + partner * rope_v[1:2]).astype(BF16).astype(F32)
    qf_v[...] = jnp.zeros_like(qf_v)
    qp_v[...] = jnp.zeros_like(qp_v)
    ns_v[...] = jnp.zeros_like(ns_v)
    tail_row = lax.broadcasted_iota(jnp.int32, (CACHE_EXTRA, head_dim), 0)
    for b in range(rows):
        for j in range(kv_dev):
            p = b * kv_dev + j
            for g in range(group):
                q_row = acc_v[pl.ds(b * 16 + g * kv_dev + j, 1), :]
                qf_v[pl.ds(p * 8 + g, 1), :] = q_row
                qp_v[pl.ds(p * 4 + g, 1), :] = q_row
            k_new = acc_v[pl.ds(b * 16 + group * kv_dev + j, 1), :]
            v_new = proj_v[pl.ds(b * 16 + (group + 1) * kv_dev + j, 1), :]
            k_buf[b, j, pl.ds(prompt, CACHE_EXTRA), :] = jnp.where(tail_row == 0, k_new, 0.0).astype(BF16)
            v_buf[b, j, pl.ds(prompt, CACHE_EXTRA), :] = jnp.where(tail_row == 0, v_new, 0.0).astype(BF16)
            vf_v[pl.ds(p * 8, 8), :] = jnp.broadcast_to(v_new, (8, head_dim))
            ns_v[pl.ds(p * 8, 8), :] = jnp.broadcast_to(k_new, (8, head_dim))
    qf = qf_v[...]
    pairs = rows * kv_dev
    my_pairs = pl.ds(sp * pairs, pairs)
    q_snd[sp] = qp_v[...].astype(BF16)
    cs = [remote(q_snd.at[sp], q_snd.at[sp], QX + i - 1, to_sp(i)) for i in (1, 2)]
    for c in cs:
        c.start()
    pump(2)
    scale = head_dim ** -0.5
    ns_v[...] = jnp.broadcast_to(jnp.sum(qf * ns_v[...], axis=-1, keepdims=True) * scale, ns_v.shape)

    n_pairs = 4 * pairs
    slots = kst.shape[0]

    def fetch(cache, i):
        slot = lax.rem(i, slots)
        return pltpu.make_async_copy(cache.at[i // kv_dev, lax.rem(i, kv_dev)], kst.at[slot], ksem.at[slot])

    def stream(cache, first, body):
        def step(i, _):
            fetch(cache, i).wait()
            body(i, kst[lax.rem(i, slots)])

            @pl.when(i + slots < n_pairs)
            def _():
                fetch(cache, i + slots).start()
            return 0
        lax.fori_loop(0, n_pairs, step, 0)

    for i in range(slots):
        fetch(k_cache, jnp.int32(i)).start()
    cs[1].wait_recv()
    hand_on = remote(q_snd.at[flip(sp, 2)], q_snd.at[flip(sp, 2)], QX + 2, to_sp(1))
    hand_on.start()
    cs[0].wait_recv()
    hand_on.wait_recv()
    for c in cs + [hand_on]:
        c.wait_send()
    pump(1)
    for d in range(4):
        got = q_snd[d].astype(F32)
        for p in range(pairs):
            q_all[d * pairs + p] = jnp.concatenate([got[p * 4:p * 4 + 4], jnp.zeros((4, head_dim), F32)], axis=0).astype(BF16)

    def score_body(i, keys):
        s = lax.dot_general(q_all[i], keys, (((1,), (1,)), ((), ())), preferred_element_type=F32) * scale
        sc_v[i] = s
        mrow_v[pl.ds(pl.multiple_of(i * 8, 8), 8), :] = jnp.broadcast_to(jnp.max(s, axis=-1, keepdims=True), (8, 128))

    stream(k_cache, 0, score_body)
    for i in range(slots):
        fetch(v_cache, jnp.int32(i)).start()
    my_m = pl.ds(pl.multiple_of(sp * pairs * 8, 8), pairs * 8)
    mrow_v[my_m, :] = jnp.maximum(mrow_v[my_m, :], ns_v[...])
    m_all[sp] = jnp.transpose(mrow_v[...])[:1]
    cs = [remote(m_all.at[sp], m_all.at[sp], MX + i - 1, to_sp(i)) for i in (1, 2, 3)]
    for c in cs:
        c.start()
    pump(1)
    settle(cs)
    m = jnp.maximum(jnp.maximum(m_all[0], m_all[1]), jnp.maximum(m_all[2], m_all[3]))
    mcol_v[...] = jnp.transpose(jnp.broadcast_to(m, (128, 128)))
    pump(1)
    lane = lax.broadcasted_iota(jnp.int32, (1, head_dim), 1)

    def out_body(i, values):
        p = jnp.exp(sc_v[i] - mcol_v[pl.ds(pl.multiple_of(i * 8, 8), 8), :][:, :1])
        total = jnp.sum(p, axis=-1, keepdims=True)
        o = jnp.dot(p.astype(BF16), values, preferred_element_type=F32)
        sums = jnp.zeros((1, head_dim), F32)
        for g in range(group):
            sums = jnp.where(lane == g, total[g:g + 1], sums)
        ol_v[i] = jnp.concatenate([o[:group], sums], axis=0)

    stream(v_cache, 0, out_body)
    o_fwd = remote(ol_v.at[pl.ds(flip(sp, 3) * pairs, pairs)], olr_v.at[1], OX, to_sp(1))
    o_own = remote(ol_v.at[pl.ds(flip(sp, 1) * pairs, pairs)], olr_v.at[0], OX + 1, to_sp(1))
    o_fwd.start()
    o_own.start()
    o_fwd.wait_recv()
    ol_sum[...] = ol_v[pl.ds(flip(sp, 2) * pairs, pairs)] + olr_v[1]
    o_sum = remote(ol_sum, olr_v.at[2], OX + 2, to_sp(2))
    o_sum.start()
    start_far(len(far))

    @pl.when(core == 0)
    def _():
        for c in far[n_both:]:
            c.start()

    o_own.wait_recv()
    o_sum.wait_recv()
    for c in (o_fwd, o_own, o_sum):
        c.wait_send()
    mine = ol_v[my_pairs]
    new_p = jnp.exp(ns_v[...] - mcol_v[my_m, :])
    new_o = new_p.astype(BF16).astype(F32) * vf_v[...]
    for b in range(rows):
        for j in range(kv_dev):
            p = b * kv_dev + j
            total = (mine[p] + olr_v[0, p]) + olr_v[2, p]
            for g in range(group):
                h, at = j * group + g, p * 8 + g
                denom = total[group:group + 1, g:g + 1] + new_p[at:at + 1]
                ho_v[pl.ds(b, 1), h * head_dim:(h + 1) * head_dim] = (total[g:g + 1] + new_o[at:at + 1]) / denom
    g_v[...] = ho_v[...].astype(BF16)
    ld_aout.wait()
    project(g_v, aout_v, pa_all)
    cs = gather_tp(pa_all, PA)
    settle(cs)
    att = ((pa_all[0] + pa_all[1]) + pa_all[2]) + pa_all[3]
    hid[...] = (RES_ALPHA * hb[...].astype(F32) + RES_BETA * att).astype(BF16)

    st_own.wait_send()
    st_fwd.wait_send()
    st_send.wait_send()
    for c in own_kv + [ld_x]:
        c.wait()
    for c in near:
        c.wait()
    for c in far[far_state[1]:n_both]:
        c.wait_send()
    for c in far[:n_both]:
        c.wait_recv()

    @pl.when(core == 0)
    def _():
        for c in far[n_both:]:
            c.wait()


def tail_kernel(x_src, token, x_buf, send, recv):
    sp = lax.axis_index("sp")
    peer = flip(sp, 2)
    barrier = pltpu.get_barrier_semaphore()
    pl.semaphore_signal(barrier, inc=1, device_id={"sp": peer}, device_id_type=MESH)
    pl.semaphore_wait(barrier, 1)

    @pl.when(lax.rem(sp, 2) == 1)
    def _():
        cs = []
        for i in range(LATE):
            cs.append(pltpu.make_async_remote_copy(
                x_src.at[i], x_buf.at[i], send.at[i], recv.at[i], device_id={"sp": peer}, device_id_type=MESH))
            cs[-1].start()
        for c in cs:
            c.wait()


def tail_write_kernel(v_in, x_buf, v_out, sem):
    sp = lax.axis_index("sp")
    rows, kv_dev = v_out.shape[:2]
    shard_len = x_buf.shape[1]

    @pl.when(lax.rem(sp, 2) == 1)
    def _():
        cs = []
        for i in range(LATE):
            at = pl.ds(pl.multiple_of(flip(sp, 2) * shard_len, shard_len), shard_len)
            cs.append(pltpu.make_async_copy(x_buf.at[i], v_out.at[rows - 1, kv_dev - LATE + i, at], sem.at[i]))
            cs[-1].start()
        for c in cs:
            c.wait()


def write_kernel(k_buf, v_buf, s_buf, hid_buf, hid, s_out, k_out, v_out, token, sem):
    token[...] = jnp.zeros_like(token)
    cs = []
    for src, dst in ((k_buf, k_out), (v_buf, v_out)):
        for b in range(src.shape[0]):
            for j in range(src.shape[1]):
                cs.append(pltpu.make_async_copy(src.at[b, j], dst.at[b, j], sem.at[len(cs)]))
    cs.append(pltpu.make_async_copy(s_buf, s_out, sem.at[len(cs)]))
    cs.append(pltpu.make_async_copy(hid_buf, hid, sem.at[len(cs)]))
    for c in cs:
        c.start()
    for c in cs:
        c.wait()


def solution(mesh):
    def device_step(tokens, states, k_cache, v_cache, slopes, lin_gain, w_lin_qkv, w_lin_gate, out_gain, w_lin_out, attn_gain, w_attn_in, w_attn_out):
        rows, width = tokens.shape
        seqs, kv_dev, shard_len, head_dim = k_cache.shape
        heads = slopes.shape[0]
        local_w = heads * head_dim
        prompt = 4 * shard_len
        reps = w_attn_in.shape[1] * w_attn_in.shape[2]
        pairs = rows * kv_dev
        group = heads // kv_dev
        cache_shape = (rows, kv_dev, prompt + CACHE_EXTRA, head_dim)
        state_shape = (rows, heads, head_dim, head_dim)
        vm, any_ = pltpu.VMEM, pl.ANY
        w_qkv = jnp.transpose(w_lin_qkv, (1, 0, 2))
        w_in = jnp.transpose(w_attn_in, (0, 2, 1, 3)).reshape(width * reps, head_dim)
        rope = jnp.asarray(rope_table(head_dim, prompt))
        dma = pltpu.SemaphoreType.DMA
        x_shape = (LATE, shard_len, head_dim)
        k_buf, v_buf, s_buf, hid_buf, x_src = pl.pallas_call(
            step_kernel,
            name="step",
            out_shape=(vm(cache_shape, BF16), vm(cache_shape, BF16), vm(state_shape, F32), vm((rows, width), BF16), vm(x_shape, BF16)),
            in_specs=[pl.BlockSpec(memory_space=any_)] * 14,
            out_specs=[pl.BlockSpec(memory_space=vm)] * 5,
            scratch_shapes=[
                vm((rows, width), BF16), vm((1, width), F32), vm((heads, head_dim), F32), vm((1, width), F32), vm((8, head_dim), F32),
                pltpu.SMEM((heads,), F32), vm((3, width, local_w), BF16), vm((width, local_w), BF16), vm((local_w, width), BF16),
                vm((width * reps, head_dim), BF16), vm((local_w, width), BF16),
                vm((2,) + state_shape, F32), vm((2,) + state_shape, F32), vm(state_shape, F32), vm(state_shape, F32),
                vm((rows, width), BF16), vm((128, head_dim), F32), vm((rows, local_w), F32), vm((rows, local_w), BF16),
                vm((128, 128 * reps), BF16), vm((16 * rows, head_dim), F32), vm((16 * rows, head_dim), F32),
                vm((8 * pairs, head_dim), F32), vm((8 * pairs, head_dim), F32), vm((4 * pairs, head_dim), F32), vm((4, 4 * pairs, head_dim), BF16), vm((4 * pairs, 8, head_dim), BF16),
                vm((4 * pairs, 8, shard_len), F32), vm((128, 128), F32), vm((4, 1, 128), F32), vm((128, 128), F32),
                vm((8 * pairs, head_dim), F32), vm((4 * pairs, group + 1, head_dim), F32), vm((pairs, group + 1, head_dim), F32), vm((3, pairs, group + 1, head_dim), F32),
                vm((rows, local_w), F32), vm((4, rows, 128), F32), vm((4, rows, width), F32), vm((4, rows, width), F32),
                vm((4, shard_len, head_dim), BF16),
                dma((NUM_SEMS,)), dma((NUM_SEMS,)), dma((18,)), dma((4,)), pltpu.SemaphoreType.REGULAR((3,)),
            ],
            compiler_params=pltpu.CompilerParams(collective_id=0, has_side_effects=True, vmem_limit_bytes=45 * MIB),
        )(tokens, states, k_cache, v_cache, slopes, lin_gain.reshape(1, -1), w_qkv, w_lin_gate, out_gain.reshape(heads, head_dim), w_lin_out, attn_gain.reshape(1, -1), w_in, w_attn_out, rope)
        bufs = [pltpu.with_memory_space_constraint(a, vm) for a in (k_buf, v_buf, s_buf, hid_buf)]
        hid, s_out, k_out, v_out, token = pl.pallas_call(
            write_kernel,
            name="write",
            out_shape=(jax.ShapeDtypeStruct((rows, width), BF16), jax.ShapeDtypeStruct(state_shape, F32),
                       jax.ShapeDtypeStruct(cache_shape, BF16), jax.ShapeDtypeStruct(cache_shape, BF16), vm((8, 128), F32)),
            in_specs=[pl.BlockSpec(memory_space=vm)] * 4,
            out_specs=[pl.BlockSpec(memory_space=any_)] * 4 + [pl.BlockSpec(memory_space=vm)],
            scratch_shapes=[dma((10,))],
            compiler_params=pltpu.CompilerParams(vmem_limit_bytes=20 * MIB),
        )(*bufs)
        x_buf = pl.pallas_call(
            tail_kernel,
            name="tail",
            out_shape=vm(x_shape, BF16),
            in_specs=[pl.BlockSpec(memory_space=vm), pl.BlockSpec(memory_space=vm)],
            out_specs=pl.BlockSpec(memory_space=vm),
            scratch_shapes=[dma((LATE,)), dma((LATE,))],
            compiler_params=pltpu.CompilerParams(collective_id=1, has_side_effects=True, vmem_limit_bytes=4 * MIB),
        )(pltpu.with_memory_space_constraint(x_src, vm), pltpu.with_memory_space_constraint(token, vm))
        v_out = pl.pallas_call(
            tail_write_kernel,
            name="tail_write",
            out_shape=jax.ShapeDtypeStruct(cache_shape, BF16),
            in_specs=[pl.BlockSpec(memory_space=any_), pl.BlockSpec(memory_space=vm)],
            out_specs=pl.BlockSpec(memory_space=any_),
            scratch_shapes=[dma((LATE,))],
            input_output_aliases={0: 0},
            compiler_params=pltpu.CompilerParams(vmem_limit_bytes=4 * MIB),
        )(v_out, pltpu.with_memory_space_constraint(x_buf, vm))
        return hid, s_out, k_out, v_out

    batch_spec = P(('dp', 'sp'), None)
    head_spec = P(('dp', 'sp'), 'tp', None, None)
    cache_spec = P('dp', 'tp', 'sp', None)
    in_specs = (batch_spec, P('sp', 'dp', 'tp', None, None), cache_spec, cache_spec, P('tp'), P(None), P(None, None, 'tp'), P(None, 'tp'), P('tp'), P('tp', None), P(None), P(None, 'tp', None, None), P('tp', None))
    out_specs = (batch_spec, head_spec, head_spec, head_spec)
    return jax.shard_map(device_step, mesh=mesh, in_specs=in_specs, out_specs=out_specs, check_vma=False)
```

```python
import math

import jax
import jax.numpy as jnp
import numpy as np
from jax import lax
from jax.experimental import pallas as pl
from jax.experimental.pallas import tpu as pltpu
from jax.sharding import PartitionSpec as P

NORM_EPS = 1e-6
ROPE_BASE = 10000000.0
RES_ALPHA = 1.0
RES_BETA = 1.0
CACHE_EXTRA = 16

MESH = pl.DeviceIdType.MESH
F32 = jnp.float32
BF16 = jnp.bfloat16
MIB = 2**20

ST_OWN, ST_FWD, ST_SUM = 0, 1, 2
SQ, PO, PA = 3, 6, 9
QX, MX, OX = 12, 15, 18
KV_NEAR = 21
KV_FAR = 23
NUM_SEMS = KV_FAR + 16
LATE = 2
EARLY = 3


def rope_table(head_dim, position):
    rope_dim = head_dim // 2
    half = rope_dim // 2
    inv_freq = ROPE_BASE ** (-np.arange(0, rope_dim, 2, dtype=np.float64) / rope_dim)
    cos, sin = np.cos(position * inv_freq), np.sin(position * inv_freq)
    table = np.zeros((8, head_dim), np.float32)
    table[0] = np.concatenate([cos, cos, np.ones(head_dim - rope_dim)])
    table[1, :rope_dim] = np.concatenate([-sin, sin])
    return table


def flip(index, mask):
    chip, core = index // 2, index % 2
    if mask & 2:
        chip = 1 - chip
    if mask & 1:
        core = 1 - core
    return chip * 2 + core


def silu(x):
    return x * (1.0 / (1.0 + jnp.exp(-x)))


def step_kernel(
    tokens, states, k_cache, v_cache, slopes, lin_gain, w_qkv, w_gate, out_gain, w_lin_out, attn_gain, w_in, w_attn_out, rope,
    k_buf, v_buf, s_out, hid, x_src,
    tok_v, lg_v, og_v, ag_v, rope_v, slope_s, qkv_v, gate_v, lout_v, in_v, aout_v,
    st_loc, st_rcv, st_sum, st_in, hb, rows_v, o_v, g_v, rep_v, acc_v, proj_v, qf_v, vf_v, qp_v, q_snd, q_all, sc_v, mrow_v, m_all, mcol_v,
    ns_v, ol_v, ol_sum, olr_v, ho_v, sq_all, po_all, pa_all, kst,
    send, recv, lsem, ksem, met,
):
    sp = lax.axis_index("sp")
    tp = lax.axis_index("tp")
    shard_len = k_cache.shape[2]
    kv_dev = k_cache.shape[1]
    head_dim = k_cache.shape[3]
    heads = slopes.shape[0]
    rows = tokens.shape[0]
    width = tokens.shape[1]
    group = heads // kv_dev
    prompt = 4 * shard_len
    local_w = heads * head_dim

    def to_sp(mask):
        return {"sp": flip(sp, mask)}

    def to_tp(off):
        return {"tp": lax.rem(tp + off, 4)}

    core = lax.rem(sp, 2)
    barrier = pltpu.get_barrier_semaphore()
    pl.semaphore_signal(barrier, inc=1, device_id=to_sp(2), device_id_type=MESH)

    @pl.when(core == 0)
    def _():
        for i in (1, 2, 3):
            pl.semaphore_signal(barrier, inc=1, device_id=to_tp(i), device_id_type=MESH)

    def remote(src, dst, i, dev):
        return pltpu.make_async_remote_copy(src, dst, send.at[i], recv.at[i], device_id=dev, device_id_type=MESH)

    def local(src, dst, i):
        return pltpu.make_async_copy(src, dst, lsem.at[i])

    my_rows = pl.ds(pl.multiple_of(sp * shard_len, shard_len), shard_len)
    pieces = [(t, b, j, mask) for t in range(2) for b in range(rows) for j in range(kv_dev) for mask in (2, 3)]
    late = [(1, rows - 1, j, 2) for j in range(kv_dev)[-LATE:]]
    pieces = sorted([p for p in pieces if p not in late], key=lambda p: p[0] > 0 or p[1] > 0) + late
    pieces[1], pieces[2] = pieces[2], pieces[1]
    far = []
    for t, b, j, mask in pieces:
        src, dst = ((k_cache, k_buf), (v_cache, v_buf))[t]
        far.append(remote(src.at[flip(sp, mask) * rows + b, j], dst.at[b, j, my_rows], KV_FAR + len(far), to_sp(mask)))
    n_both = len(far) - len(late)
    cut = shard_len * EARLY // 16
    head = remote(
        v_cache.at[flip(sp, 2) * rows + rows - 1, pl.ds(kv_dev - LATE, LATE), pl.ds(0, cut)],
        v_buf.at[rows - 1, pl.ds(kv_dev - LATE, LATE), pl.ds(pl.multiple_of(sp * shard_len, shard_len), cut)], KV_FAR + n_both, to_sp(2))
    far_state = [0, 0]

    def start_far(n):
        for _ in range(n):
            if far_state[0] < n_both:
                far[far_state[0]].start()
                far_state[0] += 1

    def pump(n):
        for _ in range(n):
            far[far_state[1]].wait_send()
            far_state[1] += 1
            start_far(1)

    @pl.when(core == 1)
    def _():
        pl.semaphore_wait(barrier, 1)
        far[0].start()
        far[1].start()
        pl.semaphore_signal(barrier, inc=1, device_id=to_sp(1), device_id_type=MESH)
        pl.semaphore_wait(met.at[0], 1)

    @pl.when(core == 0)
    def _():
        pl.semaphore_wait(barrier, 5)
        pl.semaphore_signal(met.at[0], inc=1, device_id=to_sp(1), device_id_type=MESH)
        far[0].start()
        for i in (1, 2, 3):
            pl.semaphore_signal(met.at[2], inc=1, device_id=to_tp(i), device_id_type=MESH)

    def meet_tp():
        @pl.when(core == 0)
        def _():
            pl.semaphore_wait(met.at[2], 3)
            pl.semaphore_signal(met.at[1], inc=1, device_id=to_sp(1), device_id_type=MESH)

        @pl.when(core == 1)
        def _():
            pl.semaphore_wait(met.at[1], 1)

    def st_rows(g):
        return pl.ds(g * rows, rows)

    st_own = remote(states.at[0, st_rows(flip(sp, 1))], st_rcv.at[0], ST_OWN, to_sp(1))
    st_fwd = remote(states.at[0, st_rows(flip(sp, 3))], st_rcv.at[1], ST_FWD, to_sp(1))
    st_fwd.start()
    ld_fwd = local(states.at[0, st_rows(flip(sp, 2))], st_loc.at[1], 0)
    ld_slope = local(slopes, slope_s, 1)
    ld_fwd.start()
    ld_slope.start()
    st_own.start()
    ld_own = local(states.at[0, st_rows(sp)], st_loc.at[0], 2)
    ld_tok = local(tokens, tok_v, 3)
    ld_lg = local(lin_gain, lg_v, 4)
    ld_og = local(out_gain, og_v, 5)
    ld_ag = local(attn_gain, ag_v, 6)
    ld_rope = local(rope, rope_v, 7)
    ld_qkv = [local(w_qkv.at[j], qkv_v.at[j], 8 + j) for j in range(3)]
    ld_gate = local(w_gate, gate_v, 11)
    ld_lout = local(w_lin_out, lout_v, 12)
    ld_in = local(w_in, in_v, 13)
    ld_aout = local(w_attn_out, aout_v, 14)
    own_kv = [local(src.at[st_rows(sp)], dst.at[:, :, my_rows], 15 + t) for t, (src, dst) in enumerate(((k_cache, k_buf), (v_cache, v_buf)))]
    near = [remote(src.at[st_rows(flip(sp, 1))], dst.at[:, :, my_rows], KV_NEAR + t, to_sp(1)) for t, (src, dst) in enumerate(((k_cache, k_buf), (v_cache, v_buf)))]
    ld_x = local(v_cache.at[flip(sp, 2) * rows + rows - 1, pl.ds(kv_dev - LATE, LATE), pl.ds(cut, shard_len - cut)], x_src, 17)
    for c in [ld_own, ld_tok, ld_lg, ld_og, ld_ag, ld_rope] + ld_qkv + [ld_gate, ld_lout, ld_in, ld_aout] + near + own_kv + [ld_x]:
        c.start()

    def decay(h, shard):
        off = (shard_len * (3 - shard)).astype(F32)
        return jnp.exp(jnp.full((1, head_dim), -slope_s[h] * off, F32))

    st_fwd.wait_recv()
    ld_slope.wait()
    ld_fwd.wait()
    for h in range(heads):
        w_me, w_ot = decay(h, sp), decay(h, flip(sp, 1))
        for b in range(rows):
            st_sum[b, h] = w_me * st_loc[1, b, h] + w_ot * st_rcv[1, b, h]
    st_send = remote(st_sum, st_in, ST_SUM, to_sp(2))
    st_send.start()

    @pl.when(core == 0)
    def _():
        far[1].start()

    far_state[0] = 2
    start_far(1)

    st_own.wait_recv()
    st_send.wait_recv()
    start_far(1)
    ld_own.wait()
    ld_tok.wait()
    ld_lg.wait()
    x = tok_v[...].astype(F32)
    inv = lax.rsqrt(jnp.mean(x * x, axis=-1, keepdims=True) + NORM_EPS)
    hb[...] = (x * inv * lg_v[...]).astype(BF16)

    def matvec(x_ref, w_ref, k_len, n_len, kb, out_dtype=F32):
        def body(k, acc):
            at = pl.ds(pl.multiple_of(k * kb, kb), kb)
            return acc + jnp.dot(x_ref[:, at], w_ref[at, :], preferred_element_type=F32)
        return lax.fori_loop(0, k_len // kb, body, jnp.zeros((rows, n_len), F32))

    acts = []
    for j in range(3):
        ld_qkv[j].wait()
        acts.append(silu(matvec(hb, qkv_v.at[j], width, local_w, 256)).astype(BF16).astype(F32))
    ld_gate.wait()
    gate = 1.0 / (1.0 + jnp.exp(-matvec(hb, gate_v, width, local_w, 256)))
    rows_v[...] = jnp.zeros_like(rows_v)
    for b in range(rows):
        for h in range(heads):
            cols = slice(h * head_dim, (h + 1) * head_dim)
            rows_v[pl.ds(b * 8 + h, 1), :] = acts[0][b:b + 1, cols]
            rows_v[pl.ds(16 + b * 8 + h, 1), :] = acts[1][b:b + 1, cols]
    cols_t = jnp.transpose(rows_v[...])

    for h in range(heads):
        w_me, w_ot = decay(h, sp), decay(h, flip(sp, 1))
        lam = jnp.exp(jnp.full((1, head_dim), -slope_s[h], F32))
        cols = slice(h * head_dim, (h + 1) * head_dim)
        for b in range(rows):
            moved = w_me * st_loc[0, b, h] + w_ot * st_rcv[0, b, h] + st_in[b, h]
            q_col = cols_t[:, b * 8 + h:b * 8 + h + 1]
            k_col = cols_t[:, 16 + b * 8 + h:16 + b * 8 + h + 1]
            new = lam * moved + k_col * acts[2][b:b + 1, cols]
            s_out[b, h] = new
            o_v[pl.ds(b, 1), cols] = jnp.sum(q_col * new, axis=0, keepdims=True)
    o = o_v[...]

    def gather_tp(ref, base):
        cs = [remote(ref.at[tp], ref.at[tp], base + i - 1, to_tp(i)) for i in (1, 2, 3)]
        for c in cs:
            c.start()
        return cs

    def settle(cs):
        for c in cs:
            c.wait_recv()
        for c in cs:
            c.wait_send()

    sq_all[tp] = jnp.broadcast_to(jnp.sum(o * o, axis=-1, keepdims=True), (rows, 128))
    meet_tp()
    cs = gather_tp(sq_all, SQ)
    pump(1)
    ld_og.wait()
    settle(cs)
    sq = ((sq_all[0] + sq_all[1]) + sq_all[2]) + sq_all[3]
    inv = lax.rsqrt(sq[:, :1] / (4 * local_w) + NORM_EPS)
    out_g = jnp.concatenate([og_v[h:h + 1, :] for h in range(heads)], axis=1)
    g_v[...] = (o * inv * out_g * gate).astype(BF16)

    def project(x_ref, w_ref, dst):
        nb = 512

        def body(n, _):
            at = pl.ds(pl.multiple_of(n * nb, nb), nb)
            dst[tp, :, at] = jnp.dot(x_ref[...], w_ref[:, at], preferred_element_type=F32)
            return 0
        lax.fori_loop(0, width // nb, body, 0)

    ld_lout.wait()
    project(g_v, lout_v, po_all)
    cs = gather_tp(po_all, PO)
    reps = in_v.shape[0] // width
    d_id = lax.broadcasted_iota(jnp.int32, rep_v.shape, 0)
    l_id = lax.broadcasted_iota(jnp.int32, rep_v.shape, 1)
    rep_v[...] = jnp.where((l_id >= d_id * reps) & (l_id < d_id * reps + reps), 1.0, 0.0).astype(BF16)
    settle(cs)
    lin = ((po_all[0] + po_all[1]) + po_all[2]) + po_all[3]
    y = (RES_ALPHA * hb[...].astype(F32) + RES_BETA * lin).astype(BF16).astype(F32)

    ld_ag.wait()
    inv = lax.rsqrt(jnp.mean(y * y, axis=-1, keepdims=True) + NORM_EPS)
    hb[...] = (y * inv * ag_v[...]).astype(BF16)
    ld_in.wait()
    ld_rope.wait()
    lane = lax.broadcasted_iota(jnp.int32, (16, 128 * reps), 1)
    sub = lax.broadcasted_iota(jnp.int32, (16, 128 * reps), 0)
    pick = lax.rem(lane, reps) == sub

    def in_body(d, acc):
        xb = hb[:, pl.ds(pl.multiple_of(d * 128, 128), 128)]
        xr = jnp.dot(xb, rep_v[...], preferred_element_type=F32)
        lhs = jnp.concatenate([jnp.where(pick, xr[b:b + 1], 0.0) for b in range(rows)], axis=0).astype(BF16)
        w = in_v[pl.ds(pl.multiple_of(d * 128 * reps, 128), 128 * reps), :]
        return acc + jnp.dot(lhs, w, preferred_element_type=F32)

    proj = lax.fori_loop(0, width // 128, in_body, jnp.zeros((16 * rows, head_dim), F32)).astype(BF16).astype(F32)
    lane = lax.broadcasted_iota(jnp.int32, proj.shape, 1)
    quarter = head_dim // 4
    partner = jnp.where(lane < quarter, pltpu.roll(proj, head_dim - quarter, 1), pltpu.roll(proj, quarter, 1))
    proj_v[...] = proj
    acc_v[...] = (proj * rope_v[0:1] + partner * rope_v[1:2]).astype(BF16).astype(F32)
    qf_v[...] = jnp.zeros_like(qf_v)
    qp_v[...] = jnp.zeros_like(qp_v)
    ns_v[...] = jnp.zeros_like(ns_v)
    tail_row = lax.broadcasted_iota(jnp.int32, (CACHE_EXTRA, head_dim), 0)
    for b in range(rows):
        for j in range(kv_dev):
            p = b * kv_dev + j
            for g in range(group):
                q_row = acc_v[pl.ds(b * 16 + g * kv_dev + j, 1), :]
                qf_v[pl.ds(p * 8 + g, 1), :] = q_row
                qp_v[pl.ds(p * 4 + g, 1), :] = q_row
            k_new = acc_v[pl.ds(b * 16 + group * kv_dev + j, 1), :]
            v_new = proj_v[pl.ds(b * 16 + (group + 1) * kv_dev + j, 1), :]
            k_buf[b, j, pl.ds(prompt, CACHE_EXTRA), :] = jnp.where(tail_row == 0, k_new, 0.0).astype(BF16)
            v_buf[b, j, pl.ds(prompt, CACHE_EXTRA), :] = jnp.where(tail_row == 0, v_new, 0.0).astype(BF16)
            vf_v[pl.ds(p * 8, 8), :] = jnp.broadcast_to(v_new, (8, head_dim))
            ns_v[pl.ds(p * 8, 8), :] = jnp.broadcast_to(k_new, (8, head_dim))
    qf = qf_v[...]
    pairs = rows * kv_dev
    my_pairs = pl.ds(sp * pairs, pairs)
    q_snd[sp] = qp_v[...].astype(BF16)
    cs = [remote(q_snd.at[sp], q_snd.at[sp], QX + i - 1, to_sp(i)) for i in (1, 2)]
    for c in cs:
        c.start()
    pump(2)
    scale = head_dim ** -0.5
    ns_v[...] = jnp.broadcast_to(jnp.sum(qf * ns_v[...], axis=-1, keepdims=True) * scale, ns_v.shape)

    n_pairs = 4 * pairs
    slots = kst.shape[0]

    def fetch(cache, i):
        slot = lax.rem(i, slots)
        return pltpu.make_async_copy(cache.at[i // kv_dev, lax.rem(i, kv_dev)], kst.at[slot], ksem.at[slot])

    def stream(cache, first, body):
        def step(i, _):
            fetch(cache, i).wait()
            body(i, kst[lax.rem(i, slots)])

            @pl.when(i + slots < n_pairs)
            def _():
                fetch(cache, i + slots).start()
            return 0
        lax.fori_loop(0, n_pairs, step, 0)

    for i in range(slots):
        fetch(k_cache, jnp.int32(i)).start()
    cs[1].wait_recv()
    hand_on = remote(q_snd.at[flip(sp, 2)], q_snd.at[flip(sp, 2)], QX + 2, to_sp(1))
    hand_on.start()
    cs[0].wait_recv()
    hand_on.wait_recv()
    for c in cs + [hand_on]:
        c.wait_send()
    pump(1)
    for d in range(4):
        got = q_snd[d].astype(F32)
        for p in range(pairs):
            q_all[d * pairs + p] = jnp.concatenate([got[p * 4:p * 4 + 4], jnp.zeros((4, head_dim), F32)], axis=0).astype(BF16)

    def score_body(i, keys):
        s = lax.dot_general(q_all[i], keys, (((1,), (1,)), ((), ())), preferred_element_type=F32) * scale
        sc_v[i] = s
        mrow_v[pl.ds(pl.multiple_of(i * 8, 8), 8), :] = jnp.broadcast_to(jnp.max(s, axis=-1, keepdims=True), (8, 128))

    stream(k_cache, 0, score_body)
    for i in range(slots):
        fetch(v_cache, jnp.int32(i)).start()
    my_m = pl.ds(pl.multiple_of(sp * pairs * 8, 8), pairs * 8)
    mrow_v[my_m, :] = jnp.maximum(mrow_v[my_m, :], ns_v[...])
    m_all[sp] = jnp.transpose(mrow_v[...])[:1]
    cs = [remote(m_all.at[sp], m_all.at[sp], MX + i - 1, to_sp(i)) for i in (1, 2, 3)]
    for c in cs:
        c.start()
    pump(1)
    settle(cs)
    m = jnp.maximum(jnp.maximum(m_all[0], m_all[1]), jnp.maximum(m_all[2], m_all[3]))
    mcol_v[...] = jnp.transpose(jnp.broadcast_to(m, (128, 128)))
    pump(1)
    lane = lax.broadcasted_iota(jnp.int32, (1, head_dim), 1)

    def out_body(i, values):
        p = jnp.exp(sc_v[i] - mcol_v[pl.ds(pl.multiple_of(i * 8, 8), 8), :][:, :1])
        total = jnp.sum(p, axis=-1, keepdims=True)
        o = jnp.dot(p.astype(BF16), values, preferred_element_type=F32)
        sums = jnp.zeros((1, head_dim), F32)
        for g in range(group):
            sums = jnp.where(lane == g, total[g:g + 1], sums)
        ol_v[i] = jnp.concatenate([o[:group], sums], axis=0)

    stream(v_cache, 0, out_body)
    o_fwd = remote(ol_v.at[pl.ds(flip(sp, 3) * pairs, pairs)], olr_v.at[1], OX, to_sp(1))
    o_own = remote(ol_v.at[pl.ds(flip(sp, 1) * pairs, pairs)], olr_v.at[0], OX + 1, to_sp(1))
    o_fwd.start()
    o_own.start()
    o_fwd.wait_recv()
    ol_sum[...] = ol_v[pl.ds(flip(sp, 2) * pairs, pairs)] + olr_v[1]
    o_sum = remote(ol_sum, olr_v.at[2], OX + 2, to_sp(2))
    o_sum.start()
    start_far(len(far))

    @pl.when(core == 0)
    def _():
        for c in far[n_both:]:
            c.start()

    @pl.when(core == 1)
    def _():
        head.start()

    o_own.wait_recv()
    o_sum.wait_recv()
    for c in (o_fwd, o_own, o_sum):
        c.wait_send()
    mine = ol_v[my_pairs]
    new_p = jnp.exp(ns_v[...] - mcol_v[my_m, :])
    new_o = new_p.astype(BF16).astype(F32) * vf_v[...]
    for b in range(rows):
        for j in range(kv_dev):
            p = b * kv_dev + j
            total = (mine[p] + olr_v[0, p]) + olr_v[2, p]
            for g in range(group):
                h, at = j * group + g, p * 8 + g
                denom = total[group:group + 1, g:g + 1] + new_p[at:at + 1]
                ho_v[pl.ds(b, 1), h * head_dim:(h + 1) * head_dim] = (total[g:g + 1] + new_o[at:at + 1]) / denom
    g_v[...] = ho_v[...].astype(BF16)
    ld_aout.wait()
    project(g_v, aout_v, pa_all)
    cs = gather_tp(pa_all, PA)
    settle(cs)
    att = ((pa_all[0] + pa_all[1]) + pa_all[2]) + pa_all[3]
    hid[...] = (RES_ALPHA * hb[...].astype(F32) + RES_BETA * att).astype(BF16)

    st_own.wait_send()
    st_fwd.wait_send()
    st_send.wait_send()
    for c in own_kv + [ld_x]:
        c.wait()
    for c in near:
        c.wait()
    for c in far[far_state[1]:n_both]:
        c.wait_send()
    for c in far[:n_both]:
        c.wait_recv()

    @pl.when(core == 0)
    def _():
        for c in far[n_both:]:
            c.wait()

    @pl.when(core == 1)
    def _():
        head.wait()


def tail_kernel(x_src, token, x_buf, send, recv):
    sp = lax.axis_index("sp")
    peer = flip(sp, 2)

    @pl.when(lax.rem(sp, 2) == 1)
    def _():
        barrier = pltpu.get_barrier_semaphore()
        pl.semaphore_signal(barrier, inc=1, device_id={"sp": peer}, device_id_type=MESH)
        pl.semaphore_wait(barrier, 1)
        cs = []
        for i in range(LATE):
            cs.append(pltpu.make_async_remote_copy(
                x_src.at[i], x_buf.at[i], send.at[i], recv.at[i], device_id={"sp": peer}, device_id_type=MESH))
            cs[-1].start()
        for c in cs:
            c.wait()


def tail_write_kernel(v_in, x_buf, v_out, sem):
    sp = lax.axis_index("sp")
    rows, kv_dev = v_out.shape[:2]
    shard_len = (v_out.shape[2] - CACHE_EXTRA) // 4
    cut = shard_len - x_buf.shape[1]

    @pl.when(lax.rem(sp, 2) == 1)
    def _():
        cs = []
        for i in range(LATE):
            at = pl.ds(pl.multiple_of(flip(sp, 2) * shard_len + cut, 128), shard_len - cut)
            cs.append(pltpu.make_async_copy(x_buf.at[i], v_out.at[rows - 1, kv_dev - LATE + i, at], sem.at[i]))
            cs[-1].start()
        for c in cs:
            c.wait()


def write_kernel(k_buf, v_buf, s_buf, hid_buf, hid, s_out, k_out, v_out, token, sem):
    token[...] = jnp.zeros_like(token)
    cs = []
    for src, dst in ((k_buf, k_out), (v_buf, v_out)):
        for b in range(src.shape[0]):
            for j in range(src.shape[1]):
                cs.append(pltpu.make_async_copy(src.at[b, j], dst.at[b, j], sem.at[len(cs)]))
    cs.append(pltpu.make_async_copy(s_buf, s_out, sem.at[len(cs)]))
    cs.append(pltpu.make_async_copy(hid_buf, hid, sem.at[len(cs)]))
    for c in cs:
        c.start()
    for c in cs:
        c.wait()


def solution(mesh):
    def device_step(tokens, states, k_cache, v_cache, slopes, lin_gain, w_lin_qkv, w_lin_gate, out_gain, w_lin_out, attn_gain, w_attn_in, w_attn_out):
        rows, width = tokens.shape
        seqs, kv_dev, shard_len, head_dim = k_cache.shape
        heads = slopes.shape[0]
        local_w = heads * head_dim
        prompt = 4 * shard_len
        reps = w_attn_in.shape[1] * w_attn_in.shape[2]
        pairs = rows * kv_dev
        group = heads // kv_dev
        cache_shape = (rows, kv_dev, prompt + CACHE_EXTRA, head_dim)
        state_shape = (rows, heads, head_dim, head_dim)
        vm, any_ = pltpu.VMEM, pl.ANY
        w_qkv = jnp.transpose(w_lin_qkv, (1, 0, 2))
        w_in = jnp.transpose(w_attn_in, (0, 2, 1, 3)).reshape(width * reps, head_dim)
        rope = jnp.asarray(rope_table(head_dim, prompt))
        dma = pltpu.SemaphoreType.DMA
        x_shape = (LATE, shard_len - shard_len * EARLY // 16, head_dim)
        k_buf, v_buf, s_buf, hid_buf, x_src = pl.pallas_call(
            step_kernel,
            name="step",
            out_shape=(vm(cache_shape, BF16), vm(cache_shape, BF16), vm(state_shape, F32), vm((rows, width), BF16), vm(x_shape, BF16)),
            in_specs=[pl.BlockSpec(memory_space=any_)] * 14,
            out_specs=[pl.BlockSpec(memory_space=vm)] * 5,
            scratch_shapes=[
                vm((rows, width), BF16), vm((1, width), F32), vm((heads, head_dim), F32), vm((1, width), F32), vm((8, head_dim), F32),
                pltpu.SMEM((heads,), F32), vm((3, width, local_w), BF16), vm((width, local_w), BF16), vm((local_w, width), BF16),
                vm((width * reps, head_dim), BF16), vm((local_w, width), BF16),
                vm((2,) + state_shape, F32), vm((2,) + state_shape, F32), vm(state_shape, F32), vm(state_shape, F32),
                vm((rows, width), BF16), vm((128, head_dim), F32), vm((rows, local_w), F32), vm((rows, local_w), BF16),
                vm((128, 128 * reps), BF16), vm((16 * rows, head_dim), F32), vm((16 * rows, head_dim), F32),
                vm((8 * pairs, head_dim), F32), vm((8 * pairs, head_dim), F32), vm((4 * pairs, head_dim), F32), vm((4, 4 * pairs, head_dim), BF16), vm((4 * pairs, 8, head_dim), BF16),
                vm((4 * pairs, 8, shard_len), F32), vm((128, 128), F32), vm((4, 1, 128), F32), vm((128, 128), F32),
                vm((8 * pairs, head_dim), F32), vm((4 * pairs, group + 1, head_dim), F32), vm((pairs, group + 1, head_dim), F32), vm((3, pairs, group + 1, head_dim), F32),
                vm((rows, local_w), F32), vm((4, rows, 128), F32), vm((4, rows, width), F32), vm((4, rows, width), F32),
                vm((4, shard_len, head_dim), BF16),
                dma((NUM_SEMS,)), dma((NUM_SEMS,)), dma((18,)), dma((4,)), pltpu.SemaphoreType.REGULAR((3,)),
            ],
            compiler_params=pltpu.CompilerParams(collective_id=0, has_side_effects=True, vmem_limit_bytes=45 * MIB),
        )(tokens, states, k_cache, v_cache, slopes, lin_gain.reshape(1, -1), w_qkv, w_lin_gate, out_gain.reshape(heads, head_dim), w_lin_out, attn_gain.reshape(1, -1), w_in, w_attn_out, rope)
        bufs = [pltpu.with_memory_space_constraint(a, vm) for a in (k_buf, v_buf, s_buf, hid_buf)]
        hid, s_out, k_out, v_out, token = pl.pallas_call(
            write_kernel,
            name="write",
            out_shape=(jax.ShapeDtypeStruct((rows, width), BF16), jax.ShapeDtypeStruct(state_shape, F32),
                       jax.ShapeDtypeStruct(cache_shape, BF16), jax.ShapeDtypeStruct(cache_shape, BF16), vm((8, 128), F32)),
            in_specs=[pl.BlockSpec(memory_space=vm)] * 4,
            out_specs=[pl.BlockSpec(memory_space=any_)] * 4 + [pl.BlockSpec(memory_space=vm)],
            scratch_shapes=[dma((10,))],
            compiler_params=pltpu.CompilerParams(vmem_limit_bytes=20 * MIB),
        )(*bufs)
        x_buf = pl.pallas_call(
            tail_kernel,
            name="tail",
            out_shape=vm(x_shape, BF16),
            in_specs=[pl.BlockSpec(memory_space=vm), pl.BlockSpec(memory_space=vm)],
            out_specs=pl.BlockSpec(memory_space=vm),
            scratch_shapes=[dma((LATE,)), dma((LATE,))],
            compiler_params=pltpu.CompilerParams(collective_id=1, has_side_effects=True, vmem_limit_bytes=4 * MIB),
        )(pltpu.with_memory_space_constraint(x_src, vm), pltpu.with_memory_space_constraint(token, vm))
        v_out = pl.pallas_call(
            tail_write_kernel,
            name="tail_write",
            out_shape=jax.ShapeDtypeStruct(cache_shape, BF16),
            in_specs=[pl.BlockSpec(memory_space=any_), pl.BlockSpec(memory_space=vm)],
            out_specs=pl.BlockSpec(memory_space=any_),
            scratch_shapes=[dma((LATE,))],
            input_output_aliases={0: 0},
            compiler_params=pltpu.CompilerParams(vmem_limit_bytes=4 * MIB),
        )(v_out, pltpu.with_memory_space_constraint(x_buf, vm))
        return hid, s_out, k_out, v_out

    batch_spec = P(('dp', 'sp'), None)
    head_spec = P(('dp', 'sp'), 'tp', None, None)
    cache_spec = P('dp', 'tp', 'sp', None)
    in_specs = (batch_spec, P('sp', 'dp', 'tp', None, None), cache_spec, cache_spec, P('tp'), P(None), P(None, None, 'tp'), P(None, 'tp'), P('tp'), P('tp', None), P(None), P(None, 'tp', None, None), P('tp', None))
    out_specs = (batch_spec, head_spec, head_spec, head_spec)
    return jax.shard_map(device_step, mesh=mesh, in_specs=in_specs, out_specs=out_specs, check_vma=False)
```

```python
import math

import jax
import jax.numpy as jnp
import numpy as np
from jax import lax
from jax.experimental import pallas as pl
from jax.experimental.pallas import tpu as pltpu
from jax.sharding import PartitionSpec as P

NORM_EPS = 1e-6
ROPE_BASE = 10000000.0
RES_ALPHA = 1.0
RES_BETA = 1.0
CACHE_EXTRA = 16

MESH = pl.DeviceIdType.MESH
F32 = jnp.float32
BF16 = jnp.bfloat16
MIB = 2**20

ST_OWN, ST_FWD, ST_SUM = 0, 1, 2
SQ, PO, PA = 3, 6, 9
QX, MX, OX = 12, 15, 18
KV_NEAR = 21
KV_FAR = 23
NUM_SEMS = KV_FAR + 16
LATE = 2
EARLY = 3


def rope_table(head_dim, position):
    rope_dim = head_dim // 2
    half = rope_dim // 2
    inv_freq = ROPE_BASE ** (-np.arange(0, rope_dim, 2, dtype=np.float64) / rope_dim)
    cos, sin = np.cos(position * inv_freq), np.sin(position * inv_freq)
    table = np.zeros((8, head_dim), np.float32)
    table[0] = np.concatenate([cos, cos, np.ones(head_dim - rope_dim)])
    table[1, :rope_dim] = np.concatenate([-sin, sin])
    return table


def flip(index, mask):
    chip, core = index // 2, index % 2
    if mask & 2:
        chip = 1 - chip
    if mask & 1:
        core = 1 - core
    return chip * 2 + core


def silu(x):
    return x * (1.0 / (1.0 + jnp.exp(-x)))


def step_kernel(
    tokens, states, k_cache, v_cache, slopes, lin_gain, w_qkv, w_gate, out_gain, w_lin_out, attn_gain, w_in, w_attn_out, rope,
    k_buf, v_buf, s_out, hid, x_src,
    tok_v, lg_v, og_v, ag_v, rope_v, slope_s, qkv_v, gate_v, lout_v, in_v, aout_v,
    st_loc, st_rcv, st_sum, st_in, hb, rows_v, o_v, g_v, rep_v, acc_v, proj_v, qf_v, vf_v, qp_v, q_snd, q_all, sc_v, mrow_v, m_all, mcol_v,
    ns_v, ol_v, ol_sum, olr_v, ho_v, sq_all, po_all, pa_all, kst,
    send, recv, lsem, ksem, met,
):
    sp = lax.axis_index("sp")
    tp = lax.axis_index("tp")
    shard_len = k_cache.shape[2]
    kv_dev = k_cache.shape[1]
    head_dim = k_cache.shape[3]
    heads = slopes.shape[0]
    rows = tokens.shape[0]
    width = tokens.shape[1]
    group = heads // kv_dev
    prompt = 4 * shard_len
    local_w = heads * head_dim

    def to_sp(mask):
        return {"sp": flip(sp, mask)}

    def to_tp(off):
        return {"tp": lax.rem(tp + off, 4)}

    core = lax.rem(sp, 2)
    barrier = pltpu.get_barrier_semaphore()
    pl.semaphore_signal(barrier, inc=1, device_id=to_sp(2), device_id_type=MESH)

    @pl.when(core == 0)
    def _():
        for i in (1, 2, 3):
            pl.semaphore_signal(barrier, inc=1, device_id=to_tp(i), device_id_type=MESH)

    def remote(src, dst, i, dev):
        return pltpu.make_async_remote_copy(src, dst, send.at[i], recv.at[i], device_id=dev, device_id_type=MESH)

    def local(src, dst, i):
        return pltpu.make_async_copy(src, dst, lsem.at[i])

    my_rows = pl.ds(pl.multiple_of(sp * shard_len, shard_len), shard_len)
    pieces = [(t, b, j, mask) for t in range(2) for b in range(rows) for j in range(kv_dev) for mask in (2, 3)]
    late = [(1, rows - 1, j, 2) for j in range(kv_dev)[-LATE:]]
    pieces = sorted([p for p in pieces if p not in late], key=lambda p: p[0] > 0 or p[1] > 0) + late
    pieces[1], pieces[2] = pieces[2], pieces[1]
    far = []
    for t, b, j, mask in pieces:
        src, dst = ((k_cache, k_buf), (v_cache, v_buf))[t]
        far.append(remote(src.at[flip(sp, mask) * rows + b, j], dst.at[b, j, my_rows], KV_FAR + len(far), to_sp(mask)))
    n_both = len(far) - len(late)
    cut = shard_len * EARLY // 16
    head = remote(
        v_cache.at[flip(sp, 2) * rows + rows - 1, pl.ds(kv_dev - LATE, LATE), pl.ds(0, cut)],
        v_buf.at[rows - 1, pl.ds(kv_dev - LATE, LATE), pl.ds(pl.multiple_of(sp * shard_len, shard_len), cut)], KV_FAR + n_both, to_sp(2))
    far_state = [0, 0]

    def start_far(n):
        for _ in range(n):
            if far_state[0] < n_both:
                far[far_state[0]].start()
                far_state[0] += 1

    def pump(n):
        for _ in range(n):
            far[far_state[1]].wait_send()
            far_state[1] += 1
            start_far(1)

    @pl.when(core == 1)
    def _():
        pl.semaphore_wait(barrier, 1)
        far[0].start()
        far[1].start()
        pl.semaphore_signal(barrier, inc=1, device_id=to_sp(1), device_id_type=MESH)
        pl.semaphore_wait(met.at[0], 1)

    @pl.when(core == 0)
    def _():
        pl.semaphore_wait(barrier, 5)
        pl.semaphore_signal(met.at[0], inc=1, device_id=to_sp(1), device_id_type=MESH)
        far[0].start()
        for i in (1, 2, 3):
            pl.semaphore_signal(met.at[2], inc=1, device_id=to_tp(i), device_id_type=MESH)

    def meet_tp():
        @pl.when(core == 0)
        def _():
            pl.semaphore_wait(met.at[2], 3)
            pl.semaphore_signal(met.at[1], inc=1, device_id=to_sp(1), device_id_type=MESH)

        @pl.when(core == 1)
        def _():
            pl.semaphore_wait(met.at[1], 1)

    def st_rows(g):
        return pl.ds(g * rows, rows)

    st_own = remote(states.at[0, st_rows(flip(sp, 1))], st_rcv.at[0], ST_OWN, to_sp(1))
    st_fwd = remote(states.at[0, st_rows(flip(sp, 3))], st_rcv.at[1], ST_FWD, to_sp(1))
    st_fwd.start()
    ld_fwd = local(states.at[0, st_rows(flip(sp, 2))], st_loc.at[1], 0)
    ld_slope = local(slopes, slope_s, 1)
    ld_fwd.start()
    ld_slope.start()
    st_own.start()
    ld_own = local(states.at[0, st_rows(sp)], st_loc.at[0], 2)
    ld_tok = local(tokens, tok_v, 3)
    ld_lg = local(lin_gain, lg_v, 4)
    ld_og = local(out_gain, og_v, 5)
    ld_ag = local(attn_gain, ag_v, 6)
    ld_rope = local(rope, rope_v, 7)
    ld_qkv = [local(w_qkv.at[j], qkv_v.at[j], 8 + j) for j in range(3)]
    ld_gate = local(w_gate, gate_v, 11)
    ld_lout = local(w_lin_out, lout_v, 12)
    ld_in = local(w_in, in_v, 13)
    ld_aout = local(w_attn_out, aout_v, 14)
    own_kv = [local(src.at[st_rows(sp)], dst.at[:, :, my_rows], 15 + t) for t, (src, dst) in enumerate(((k_cache, k_buf), (v_cache, v_buf)))]
    near = [remote(src.at[st_rows(flip(sp, 1))], dst.at[:, :, my_rows], KV_NEAR + t, to_sp(1)) for t, (src, dst) in enumerate(((k_cache, k_buf), (v_cache, v_buf)))]
    ld_x = local(v_cache.at[flip(sp, 2) * rows + rows - 1, pl.ds(kv_dev - LATE, LATE), pl.ds(cut, shard_len - cut)], x_src, 17)
    for c in [ld_own, ld_tok, ld_lg, ld_og, ld_ag, ld_rope] + ld_qkv + [ld_gate, ld_lout, ld_in, ld_aout] + near + own_kv + [ld_x]:
        c.start()

    def decay(h, shard):
        off = (shard_len * (3 - shard)).astype(F32)
        return jnp.exp(jnp.full((1, head_dim), -slope_s[h] * off, F32))

    st_fwd.wait_recv()
    ld_slope.wait()
    ld_fwd.wait()
    for h in range(heads):
        w_me, w_ot = decay(h, sp), decay(h, flip(sp, 1))
        for b in range(rows):
            st_sum[b, h] = w_me * st_loc[1, b, h] + w_ot * st_rcv[1, b, h]
    st_send = remote(st_sum, st_in, ST_SUM, to_sp(2))
    st_send.start()

    @pl.when(core == 0)
    def _():
        far[1].start()

    far_state[0] = 2
    start_far(1)

    st_own.wait_recv()
    st_send.wait_recv()
    start_far(1)
    ld_own.wait()
    ld_tok.wait()
    ld_lg.wait()
    x = tok_v[...].astype(F32)
    inv = lax.rsqrt(jnp.mean(x * x, axis=-1, keepdims=True) + NORM_EPS)
    hb[...] = (x * inv * lg_v[...]).astype(BF16)

    def matvec(x_ref, w_ref, k_len, n_len, kb, out_dtype=F32):
        def body(k, acc):
            at = pl.ds(pl.multiple_of(k * kb, kb), kb)
            return acc + jnp.dot(x_ref[:, at], w_ref[at, :], preferred_element_type=F32)
        return lax.fori_loop(0, k_len // kb, body, jnp.zeros((rows, n_len), F32))

    acts = []
    for j in range(3):
        ld_qkv[j].wait()
        acts.append(silu(matvec(hb, qkv_v.at[j], width, local_w, 256)).astype(BF16).astype(F32))
    ld_gate.wait()
    gate = 1.0 / (1.0 + jnp.exp(-matvec(hb, gate_v, width, local_w, 256)))
    rows_v[...] = jnp.zeros_like(rows_v)
    for b in range(rows):
        for h in range(heads):
            cols = slice(h * head_dim, (h + 1) * head_dim)
            rows_v[pl.ds(b * 8 + h, 1), :] = acts[0][b:b + 1, cols]
            rows_v[pl.ds(16 + b * 8 + h, 1), :] = acts[1][b:b + 1, cols]
    cols_t = jnp.transpose(rows_v[...])

    for h in range(heads):
        w_me, w_ot = decay(h, sp), decay(h, flip(sp, 1))
        lam = jnp.exp(jnp.full((1, head_dim), -slope_s[h], F32))
        cols = slice(h * head_dim, (h + 1) * head_dim)
        for b in range(rows):
            moved = w_me * st_loc[0, b, h] + w_ot * st_rcv[0, b, h] + st_in[b, h]
            q_col = cols_t[:, b * 8 + h:b * 8 + h + 1]
            k_col = cols_t[:, 16 + b * 8 + h:16 + b * 8 + h + 1]
            new = lam * moved + k_col * acts[2][b:b + 1, cols]
            s_out[b, h] = new
            o_v[pl.ds(b, 1), cols] = jnp.sum(q_col * new, axis=0, keepdims=True)
    o = o_v[...]

    def gather_tp(ref, base):
        cs = [remote(ref.at[tp], ref.at[tp], base + i - 1, to_tp(i)) for i in (1, 2, 3)]
        for c in cs:
            c.start()
        return cs

    def settle(cs):
        for c in cs:
            c.wait_recv()
        for c in cs:
            c.wait_send()

    sq_all[tp] = jnp.broadcast_to(jnp.sum(o * o, axis=-1, keepdims=True), (rows, 128))
    meet_tp()
    cs = gather_tp(sq_all, SQ)
    pump(1)
    ld_og.wait()
    settle(cs)
    sq = ((sq_all[0] + sq_all[1]) + sq_all[2]) + sq_all[3]
    inv = lax.rsqrt(sq[:, :1] / (4 * local_w) + NORM_EPS)
    out_g = jnp.concatenate([og_v[h:h + 1, :] for h in range(heads)], axis=1)
    g_v[...] = (o * inv * out_g * gate).astype(BF16)

    def project(x_ref, w_ref, dst):
        nb = 512

        def body(n, _):
            at = pl.ds(pl.multiple_of(n * nb, nb), nb)
            dst[tp, :, at] = jnp.dot(x_ref[...], w_ref[:, at], preferred_element_type=F32)
            return 0
        lax.fori_loop(0, width // nb, body, 0)

    ld_lout.wait()
    project(g_v, lout_v, po_all)
    cs = gather_tp(po_all, PO)
    reps = in_v.shape[0] // width
    d_id = lax.broadcasted_iota(jnp.int32, rep_v.shape, 0)
    l_id = lax.broadcasted_iota(jnp.int32, rep_v.shape, 1)
    rep_v[...] = jnp.where((l_id >= d_id * reps) & (l_id < d_id * reps + reps), 1.0, 0.0).astype(BF16)
    settle(cs)
    lin = ((po_all[0] + po_all[1]) + po_all[2]) + po_all[3]
    y = (RES_ALPHA * hb[...].astype(F32) + RES_BETA * lin).astype(BF16).astype(F32)

    ld_ag.wait()
    inv = lax.rsqrt(jnp.mean(y * y, axis=-1, keepdims=True) + NORM_EPS)
    hb[...] = (y * inv * ag_v[...]).astype(BF16)
    ld_in.wait()
    ld_rope.wait()
    lane = lax.broadcasted_iota(jnp.int32, (16, 128 * reps), 1)
    sub = lax.broadcasted_iota(jnp.int32, (16, 128 * reps), 0)
    pick = lax.rem(lane, reps) == sub

    def in_body(d, acc):
        xb = hb[:, pl.ds(pl.multiple_of(d * 128, 128), 128)]
        xr = jnp.dot(xb, rep_v[...], preferred_element_type=F32)
        lhs = jnp.concatenate([jnp.where(pick, xr[b:b + 1], 0.0) for b in range(rows)], axis=0).astype(BF16)
        w = in_v[pl.ds(pl.multiple_of(d * 128 * reps, 128), 128 * reps), :]
        return acc + jnp.dot(lhs, w, preferred_element_type=F32)

    proj = lax.fori_loop(0, width // 128, in_body, jnp.zeros((16 * rows, head_dim), F32)).astype(BF16).astype(F32)
    lane = lax.broadcasted_iota(jnp.int32, proj.shape, 1)
    quarter = head_dim // 4
    partner = jnp.where(lane < quarter, pltpu.roll(proj, head_dim - quarter, 1), pltpu.roll(proj, quarter, 1))
    proj_v[...] = proj
    acc_v[...] = (proj * rope_v[0:1] + partner * rope_v[1:2]).astype(BF16).astype(F32)
    qf_v[...] = jnp.zeros_like(qf_v)
    ns_v[...] = jnp.zeros_like(ns_v)
    tail_row = lax.broadcasted_iota(jnp.int32, (CACHE_EXTRA, head_dim), 0)
    for b in range(rows):
        for j in range(kv_dev):
            p = b * kv_dev + j
            for g in range(group):
                q_row = acc_v[pl.ds(b * 16 + g * kv_dev + j, 1), :]
                qf_v[pl.ds(p * 8 + g, 1), :] = q_row
                qp_v[pl.ds(p * group + g, 1), :] = q_row
            k_new = acc_v[pl.ds(b * 16 + group * kv_dev + j, 1), :]
            v_new = proj_v[pl.ds(b * 16 + (group + 1) * kv_dev + j, 1), :]
            k_buf[b, j, pl.ds(prompt, CACHE_EXTRA), :] = jnp.where(tail_row == 0, k_new, 0.0).astype(BF16)
            v_buf[b, j, pl.ds(prompt, CACHE_EXTRA), :] = jnp.where(tail_row == 0, v_new, 0.0).astype(BF16)
            vf_v[pl.ds(p * 8, 8), :] = jnp.broadcast_to(v_new, (8, head_dim))
            ns_v[pl.ds(p * 8, 8), :] = jnp.broadcast_to(k_new, (8, head_dim))
    qf = qf_v[...]
    pairs = rows * kv_dev
    my_pairs = pl.ds(sp * pairs, pairs)
    q_snd[sp] = qp_v[...].astype(BF16)
    cs = [remote(q_snd.at[sp], q_snd.at[sp], QX + i - 1, to_sp(i)) for i in (1, 2)]
    for c in cs:
        c.start()
    pump(2)
    scale = head_dim ** -0.5
    ns_v[...] = jnp.broadcast_to(jnp.sum(qf * ns_v[...], axis=-1, keepdims=True) * scale, ns_v.shape)

    n_pairs = 4 * pairs
    slots = kst.shape[0]

    def fetch(cache, i):
        slot = lax.rem(i, slots)
        return pltpu.make_async_copy(cache.at[i // kv_dev, lax.rem(i, kv_dev)], kst.at[slot], ksem.at[slot])

    def stream(cache, first, body):
        def step(i, _):
            fetch(cache, i).wait()
            body(i, kst[lax.rem(i, slots)])

            @pl.when(i + slots < n_pairs)
            def _():
                fetch(cache, i + slots).start()
            return 0
        lax.fori_loop(0, n_pairs, step, 0)

    for i in range(slots):
        fetch(k_cache, jnp.int32(i)).start()
    cs[1].wait_recv()
    hand_on = remote(q_snd.at[flip(sp, 2)], q_snd.at[flip(sp, 2)], QX + 2, to_sp(1))
    hand_on.start()
    cs[0].wait_recv()
    hand_on.wait_recv()
    for c in cs + [hand_on]:
        c.wait_send()
    pump(1)
    for d in range(4):
        got = q_snd[d].astype(F32)
        for p in range(pairs):
            q_all[d * pairs + p] = jnp.concatenate([got[p * group:(p + 1) * group], jnp.zeros((8 - group, head_dim), F32)], axis=0).astype(BF16)

    def score_body(i, keys):
        s = lax.dot_general(q_all[i], keys, (((1,), (1,)), ((), ())), preferred_element_type=F32) * scale
        sc_v[i] = s
        mrow_v[pl.ds(pl.multiple_of(i * 8, 8), 8), :] = jnp.broadcast_to(jnp.max(s, axis=-1, keepdims=True), (8, 128))

    stream(k_cache, 0, score_body)
    for i in range(slots):
        fetch(v_cache, jnp.int32(i)).start()
    my_m = pl.ds(pl.multiple_of(sp * pairs * 8, 8), pairs * 8)
    mrow_v[my_m, :] = jnp.maximum(mrow_v[my_m, :], ns_v[...])
    m_all[sp] = jnp.transpose(mrow_v[...])[:1]
    cs = [remote(m_all.at[sp], m_all.at[sp], MX + i - 1, to_sp(i)) for i in (1, 2, 3)]
    for c in cs:
        c.start()
    pump(1)
    settle(cs)
    m = jnp.maximum(jnp.maximum(m_all[0], m_all[1]), jnp.maximum(m_all[2], m_all[3]))
    mcol_v[...] = jnp.transpose(jnp.broadcast_to(m, (128, 128)))
    pump(1)
    lane = lax.broadcasted_iota(jnp.int32, (1, head_dim), 1)

    def out_body(i, values):
        p = jnp.exp(sc_v[i] - mcol_v[pl.ds(pl.multiple_of(i * 8, 8), 8), :][:, :1])
        total = jnp.sum(p, axis=-1, keepdims=True)
        o = jnp.dot(p.astype(BF16), values, preferred_element_type=F32)
        sums = jnp.zeros((1, head_dim), F32)
        for g in range(group):
            sums = jnp.where(lane == g, total[g:g + 1], sums)
        ol_v[i] = jnp.concatenate([o[:group], sums], axis=0)

    stream(v_cache, 0, out_body)
    o_fwd = remote(ol_v.at[pl.ds(flip(sp, 3) * pairs, pairs)], olr_v.at[1], OX, to_sp(1))
    o_own = remote(ol_v.at[pl.ds(flip(sp, 1) * pairs, pairs)], olr_v.at[0], OX + 1, to_sp(1))
    o_fwd.start()
    o_own.start()
    o_fwd.wait_recv()
    ol_sum[...] = ol_v[pl.ds(flip(sp, 2) * pairs, pairs)] + olr_v[1]
    o_sum = remote(ol_sum, olr_v.at[2], OX + 2, to_sp(2))
    o_sum.start()
    start_far(len(far))

    @pl.when(core == 0)
    def _():
        for c in far[n_both:]:
            c.start()

    @pl.when(core == 1)
    def _():
        head.start()

    o_own.wait_recv()
    o_sum.wait_recv()
    for c in (o_fwd, o_own, o_sum):
        c.wait_send()
    mine = ol_v[my_pairs]
    new_p = jnp.exp(ns_v[...] - mcol_v[my_m, :])
    new_o = new_p.astype(BF16).astype(F32) * vf_v[...]
    for b in range(rows):
        for j in range(kv_dev):
            p = b * kv_dev + j
            total = (mine[p] + olr_v[0, p]) + olr_v[2, p]
            for g in range(group):
                h, at = j * group + g, p * 8 + g
                denom = total[group:group + 1, g:g + 1] + new_p[at:at + 1]
                ho_v[pl.ds(b, 1), h * head_dim:(h + 1) * head_dim] = (total[g:g + 1] + new_o[at:at + 1]) / denom
    g_v[...] = ho_v[...].astype(BF16)
    ld_aout.wait()
    project(g_v, aout_v, pa_all)
    cs = gather_tp(pa_all, PA)
    settle(cs)
    att = ((pa_all[0] + pa_all[1]) + pa_all[2]) + pa_all[3]
    hid[...] = (RES_ALPHA * hb[...].astype(F32) + RES_BETA * att).astype(BF16)

    st_own.wait_send()
    st_fwd.wait_send()
    st_send.wait_send()
    for c in own_kv + [ld_x]:
        c.wait()
    for c in near:
        c.wait()
    for c in far[far_state[1]:n_both]:
        c.wait_send()
    for c in far[:n_both]:
        c.wait_recv()

    @pl.when(core == 0)
    def _():
        for c in far[n_both:]:
            c.wait()

    @pl.when(core == 1)
    def _():
        head.wait()


def tail_kernel(x_src, token, x_buf, send, recv):
    sp = lax.axis_index("sp")
    peer = flip(sp, 2)

    @pl.when(lax.rem(sp, 2) == 1)
    def _():
        barrier = pltpu.get_barrier_semaphore()
        pl.semaphore_signal(barrier, inc=1, device_id={"sp": peer}, device_id_type=MESH)
        pl.semaphore_wait(barrier, 1)
        copy = pltpu.make_async_remote_copy(
            x_src, x_buf, send.at[0], recv.at[0], device_id={"sp": peer}, device_id_type=MESH)
        copy.start()
        copy.wait()


def tail_write_kernel(v_in, x_buf, v_out, sem):
    sp = lax.axis_index("sp")
    rows, kv_dev = v_out.shape[:2]
    shard_len = (v_out.shape[2] - CACHE_EXTRA) // 4
    cut = shard_len - x_buf.shape[1]

    @pl.when(lax.rem(sp, 2) == 1)
    def _():
        at = pl.ds(pl.multiple_of(flip(sp, 2) * shard_len + cut, 128), shard_len - cut)
        copy = pltpu.make_async_copy(x_buf, v_out.at[rows - 1, pl.ds(kv_dev - LATE, LATE), at], sem.at[0])
        copy.start()
        copy.wait()


def write_kernel(k_buf, v_buf, s_buf, hid_buf, hid, s_out, k_out, v_out, token, sem):
    token[...] = jnp.zeros_like(token)
    cs = []
    for src, dst in ((k_buf, k_out), (v_buf, v_out)):
        for b in range(src.shape[0]):
            for j in range(src.shape[1]):
                cs.append(pltpu.make_async_copy(src.at[b, j], dst.at[b, j], sem.at[len(cs)]))
    cs.append(pltpu.make_async_copy(s_buf, s_out, sem.at[len(cs)]))
    cs.append(pltpu.make_async_copy(hid_buf, hid, sem.at[len(cs)]))
    for c in cs:
        c.start()
    for c in cs:
        c.wait()


def solution(mesh):
    def device_step(tokens, states, k_cache, v_cache, slopes, lin_gain, w_lin_qkv, w_lin_gate, out_gain, w_lin_out, attn_gain, w_attn_in, w_attn_out):
        rows, width = tokens.shape
        seqs, kv_dev, shard_len, head_dim = k_cache.shape
        heads = slopes.shape[0]
        local_w = heads * head_dim
        prompt = 4 * shard_len
        reps = w_attn_in.shape[1] * w_attn_in.shape[2]
        pairs = rows * kv_dev
        group = heads // kv_dev
        cache_shape = (rows, kv_dev, prompt + CACHE_EXTRA, head_dim)
        state_shape = (rows, heads, head_dim, head_dim)
        vm, any_ = pltpu.VMEM, pl.ANY
        w_qkv = jnp.transpose(w_lin_qkv, (1, 0, 2))
        w_in = jnp.transpose(w_attn_in, (0, 2, 1, 3)).reshape(width * reps, head_dim)
        rope = jnp.asarray(rope_table(head_dim, prompt))
        dma = pltpu.SemaphoreType.DMA
        x_shape = (LATE, shard_len - shard_len * EARLY // 16, head_dim)
        k_buf, v_buf, s_buf, hid_buf, x_src = pl.pallas_call(
            step_kernel,
            name="step",
            out_shape=(vm(cache_shape, BF16), vm(cache_shape, BF16), vm(state_shape, F32), vm((rows, width), BF16), vm(x_shape, BF16)),
            in_specs=[pl.BlockSpec(memory_space=any_)] * 14,
            out_specs=[pl.BlockSpec(memory_space=vm)] * 5,
            scratch_shapes=[
                vm((rows, width), BF16), vm((1, width), F32), vm((heads, head_dim), F32), vm((1, width), F32), vm((8, head_dim), F32),
                pltpu.SMEM((heads,), F32), vm((3, width, local_w), BF16), vm((width, local_w), BF16), vm((local_w, width), BF16),
                vm((width * reps, head_dim), BF16), vm((local_w, width), BF16),
                vm((2,) + state_shape, F32), vm((2,) + state_shape, F32), vm(state_shape, F32), vm(state_shape, F32),
                vm((rows, width), BF16), vm((128, head_dim), F32), vm((rows, local_w), F32), vm((rows, local_w), BF16),
                vm((128, 128 * reps), BF16), vm((16 * rows, head_dim), F32), vm((16 * rows, head_dim), F32),
                vm((8 * pairs, head_dim), F32), vm((8 * pairs, head_dim), F32), vm((group * pairs, head_dim), F32), vm((4, group * pairs, head_dim), BF16), vm((4 * pairs, 8, head_dim), BF16),
                vm((4 * pairs, 8, shard_len), F32), vm((128, 128), F32), vm((4, 1, 128), F32), vm((128, 128), F32),
                vm((8 * pairs, head_dim), F32), vm((4 * pairs, group + 1, head_dim), F32), vm((pairs, group + 1, head_dim), F32), vm((3, pairs, group + 1, head_dim), F32),
                vm((rows, local_w), F32), vm((4, rows, 128), F32), vm((4, rows, width), F32), vm((4, rows, width), F32),
                vm((4, shard_len, head_dim), BF16),
                dma((NUM_SEMS,)), dma((NUM_SEMS,)), dma((18,)), dma((4,)), pltpu.SemaphoreType.REGULAR((3,)),
            ],
            compiler_params=pltpu.CompilerParams(collective_id=0, has_side_effects=True, vmem_limit_bytes=45 * MIB),
        )(tokens, states, k_cache, v_cache, slopes, lin_gain.reshape(1, -1), w_qkv, w_lin_gate, out_gain.reshape(heads, head_dim), w_lin_out, attn_gain.reshape(1, -1), w_in, w_attn_out, rope)
        bufs = [pltpu.with_memory_space_constraint(a, vm) for a in (k_buf, v_buf, s_buf, hid_buf)]
        hid, s_out, k_out, v_out, token = pl.pallas_call(
            write_kernel,
            name="write",
            out_shape=(jax.ShapeDtypeStruct((rows, width), BF16), jax.ShapeDtypeStruct(state_shape, F32),
                       jax.ShapeDtypeStruct(cache_shape, BF16), jax.ShapeDtypeStruct(cache_shape, BF16), vm((8, 128), F32)),
            in_specs=[pl.BlockSpec(memory_space=vm)] * 4,
            out_specs=[pl.BlockSpec(memory_space=any_)] * 4 + [pl.BlockSpec(memory_space=vm)],
            scratch_shapes=[dma((10,))],
            compiler_params=pltpu.CompilerParams(vmem_limit_bytes=20 * MIB),
        )(*bufs)
        x_buf = pl.pallas_call(
            tail_kernel,
            name="tail",
            out_shape=vm(x_shape, BF16),
            in_specs=[pl.BlockSpec(memory_space=vm), pl.BlockSpec(memory_space=vm)],
            out_specs=pl.BlockSpec(memory_space=vm),
            scratch_shapes=[dma((LATE,)), dma((LATE,))],
            compiler_params=pltpu.CompilerParams(collective_id=1, has_side_effects=True, vmem_limit_bytes=4 * MIB),
        )(pltpu.with_memory_space_constraint(x_src, vm), pltpu.with_memory_space_constraint(token, vm))
        v_out = pl.pallas_call(
            tail_write_kernel,
            name="tail_write",
            out_shape=jax.ShapeDtypeStruct(cache_shape, BF16),
            in_specs=[pl.BlockSpec(memory_space=any_), pl.BlockSpec(memory_space=vm)],
            out_specs=pl.BlockSpec(memory_space=any_),
            scratch_shapes=[dma((LATE,))],
            input_output_aliases={0: 0},
            compiler_params=pltpu.CompilerParams(vmem_limit_bytes=4 * MIB),
        )(v_out, pltpu.with_memory_space_constraint(x_buf, vm))
        return hid, s_out, k_out, v_out

    batch_spec = P(('dp', 'sp'), None)
    head_spec = P(('dp', 'sp'), 'tp', None, None)
    cache_spec = P('dp', 'tp', 'sp', None)
    in_specs = (batch_spec, P('sp', 'dp', 'tp', None, None), cache_spec, cache_spec, P('tp'), P(None), P(None, None, 'tp'), P(None, 'tp'), P('tp'), P('tp', None), P(None), P(None, 'tp', None, None), P('tp', None))
    out_specs = (batch_spec, head_spec, head_spec, head_spec)
    return jax.shard_map(device_step, mesh=mesh, in_specs=in_specs, out_specs=out_specs, check_vma=False)
```
